8 devices in a mesh: parts: 1 (over z), col: 2 (over y), row: 2 (over x), sub: 2 (over core).
Axes of the slice: x: 2, y: 2, z: 1, core: 2. Of those that a mesh axis runs over, the one named last changes fastest.
Arguments:
- edge_dist: float32 [8, 128, 1024], P(('parts', 'row', 'sub'), None, 'col')
Outputs:
- output: float32 [8, 128, 1024], P(('parts', 'row', 'sub'), None, 'col')
All inputs are finite; a program needn't handle non-finite values.
Results may differ from the reference program's by a relative error of at most 0.001.
Values sent between devices are 32-bit elements.
A program may use at most 1 GiB of HBM per device.

```python
import jax
import jax.numpy as jnp
from jax import lax

VERTICES = 1024
BLOCK = 128
ROW_DEVS = 4
COL_DEVS = 2
CHORDS = 2

ROUNDS = VERTICES // BLOCK
NO_EDGE = 2 ** 16


def to_stored(full_dist):
    by_rows = full_dist.reshape(ROUNDS // ROW_DEVS, ROW_DEVS, BLOCK, VERTICES).transpose(1, 0, 2, 3)
    by_rows = by_rows.reshape(ROUNDS, BLOCK, ROUNDS // COL_DEVS, COL_DEVS, BLOCK).transpose(0, 1, 3, 2, 4)
    return by_rows.reshape(ROUNDS, BLOCK, VERTICES)


def from_stored(stored):
    by_cols = stored.reshape(ROUNDS, BLOCK, COL_DEVS, ROUNDS // COL_DEVS, BLOCK).transpose(0, 1, 3, 2, 4)
    by_cols = by_cols.reshape(ROW_DEVS, ROUNDS // ROW_DEVS, BLOCK, VERTICES).transpose(1, 0, 2, 3)
    return by_cols.reshape(VERTICES, VERTICES)


def setup_inputs(seed: int = 0, part: int = 0) -> dict:
    base_key = jax.random.fold_in(jax.random.key(seed), part)
    key_cycle, key_dst, key_wt = jax.random.split(base_key, 3)
    vertex_ids = jnp.arange(VERTICES)
    cycle_wt = jax.random.randint(key_cycle, (VERTICES,), 8, 17).astype(jnp.float32) / 8.0
    chord_dst = jax.random.randint(key_dst, (VERTICES, CHORDS), 0, VERTICES)
    chord_wt = jax.random.randint(key_wt, (VERTICES, CHORDS), 1, 17).astype(jnp.float32) / 8.0
    full_dist = jnp.full((VERTICES, VERTICES), NO_EDGE, dtype=jnp.float32)
    full_dist = full_dist.at[vertex_ids, (vertex_ids + 1) % VERTICES].min(cycle_wt)
    full_dist = full_dist.at[vertex_ids[:, None], chord_dst].min(chord_wt)
    full_dist = full_dist.at[vertex_ids, vertex_ids].set(0.0)
    return {'edge_dist': to_stored(full_dist)}


def close_block(block_in):
    def pivot_step(pivot_idx, current):
        col_vec = lax.dynamic_slice_in_dim(current, pivot_idx, 1, axis=1)
        row_vec = lax.dynamic_slice_in_dim(current, pivot_idx, 1, axis=0)
        return jnp.minimum(current, col_vec + row_vec)
    return lax.fori_loop(0, block_in.shape[0], pivot_step, block_in)


def min_plus(left_mat, right_mat):
    num_rows = left_mat.shape[0]
    row_groups = left_mat.reshape(num_rows // 8, 8, left_mat.shape[1])
    result = lax.map(lambda row_group: jnp.min(row_group[:, :, None] + right_mat[None, :, :], axis=1), row_groups)
    return result.reshape(num_rows, right_mat.shape[1])


def reference(edge_dist):
    def one_round(current, round_idx):
        offset = round_idx * BLOCK
        diag_blk = close_block(lax.dynamic_slice(current, (offset, offset), (BLOCK, BLOCK)))
        row_pan = min_plus(diag_blk, lax.dynamic_slice_in_dim(current, offset, BLOCK, axis=0))
        col_pan = min_plus(lax.dynamic_slice_in_dim(current, offset, BLOCK, axis=1), diag_blk)
        return jnp.minimum(current, min_plus(col_pan, row_pan)), None
    full_dist = lax.scan(one_round, from_stored(edge_dist), jnp.arange(ROUNDS))[0]
    return to_stored(full_dist)
```

```python
import functools

import jax
import jax.numpy as jnp
from jax import lax
from jax.experimental import pallas as pl
from jax.experimental.pallas import tpu as pltpu
from jax.sharding import PartitionSpec as P

MESH = pl.DeviceIdType.MESH
BLK = 128
ROUNDS = 8
ROW_PEERS = ((0, 1), (1, 1), (1, 0))
ALL_PEERS = ((1, 0, 1), (1, 1, 1), (0, 0, 1), (0, 1, 1), (1, 0, 0), (0, 1, 0), (1, 1, 0))


def lanes(tiles, idx):
    flat = tiles.reshape(-1, 128)
    idx = jnp.broadcast_to(idx[None], (flat.shape[0] // 8, 8, 128)).reshape(-1, 128)
    return jnp.take_along_axis(flat, idx, axis=1, mode='promise_in_bounds').reshape(tiles.shape)


def kernel(in_ref, out_ref, mat, rowp, colp, dst, cb, brep, brepd, cpr,
           row_send, row_recv, col_send, col_recv, dia_send, dia_recv):
    row, sub, col = lax.axis_index('row'), lax.axis_index('sub'), lax.axis_index('col')
    my_row = row * 2 + sub
    lane = lax.broadcasted_iota(jnp.int32, (8, 128), 1)
    in_grp = lane & 15
    grp_base = lane - in_grp

    def peer(d_col, d_row, d_sub):
        return {'col': (col + d_col) % 2, 'row': (row + d_row) % 2, 'sub': (sub + d_sub) % 2}

    barrier = pltpu.get_barrier_semaphore()
    for offs in ALL_PEERS:
        pl.semaphore_signal(barrier, inc=1, device_id=peer(*offs), device_id_type=MESH)

    def swap_chunks(tiles):
        for bit in (1, 2, 4):
            mask = (lane & (16 * bit)) == 0
            pairs = tiles.reshape(8 // (2 * bit), 2, bit, 8, 128)
            lo, hi = pairs[:, 0].reshape(-1, 128), pairs[:, 1].reshape(-1, 128)
            lo_up = pltpu.roll(lo, 128 - 16 * bit, 1)
            hi_up = pltpu.roll(hi, 16 * bit, 1)
            lo, hi, lo_up, hi_up = (v.reshape(8 // (2 * bit), bit, 8, 128) for v in (lo, hi, lo_up, hi_up))
            tiles = jnp.stack([jnp.where(mask, lo, hi_up), jnp.where(mask, lo_up, hi)], axis=1).reshape(8, 8, 128)
        return tiles

    def row_copy(rnd, x, i):
        d_row, d_sub = ROW_PEERS[i]
        return pltpu.make_async_remote_copy(
            src_ref=rowp.at[rnd, x], dst_ref=rowp.at[rnd, x],
            send_sem=row_send.at[rnd, x, i], recv_sem=row_recv.at[rnd, x],
            device_id=peer(0, d_row, d_sub), device_id_type=MESH)

    def col_copy(rnd, a):
        return pltpu.make_async_remote_copy(
            src_ref=colp.at[rnd, a], dst_ref=colp.at[rnd, a],
            send_sem=col_send.at[rnd, a], recv_sem=col_recv.at[rnd, a],
            device_id=peer(1, 0, 0), device_id_type=MESH)

    def dia_copy(rnd, i):
        return pltpu.make_async_remote_copy(
            src_ref=dst.at[rnd], dst_ref=dst.at[rnd],
            send_sem=dia_send.at[rnd, i], recv_sem=dia_recv.at[rnd],
            device_id=peer(*ALL_PEERS[i]), device_id_type=MESH)

    def send_row(rnd, x):
        for i in range(3):
            row_copy(rnd, x, i).start()

    def send_dia(rnd):
        for i in range(7):
            dia_copy(rnd, i).start()

    def close(rnd, x):
        dst[rnd] = rowp[rnd, x]

        def group(g, carry):
            rg, q = g // 8, g % 8
            cg, half = g // 2, (g % 2) * 8
            pivot_tile = dst[rnd, rg, cg]
            ucol = [lanes(pivot_tile, jnp.full((8, 128), 16 * q + half + p, jnp.int32)) for p in range(8)]
            rows = lanes(dst[rnd, rg], in_grp + 16 * q)
            left = [lanes(dst[rnd, :, cg], grp_base + (half + p)) for p in range(8)]
            for p in range(8):
                for j in range(p + 1, 8):
                    ucol[j] = jnp.minimum(ucol[j], ucol[p] + ucol[j][p:p + 1, :])
                rows = jnp.minimum(rows, ucol[p][None] + rows[:, p:p + 1, :])
            acc = dst[rnd]
            for p in range(8):
                acc = jnp.minimum(acc, left[p][:, None] + rows[:, p:p + 1, :][None])
            dst[rnd] = acc
            return carry
        lax.fori_loop(0, 16, group, 0)

    def make_brep(src, out):
        def one(i, carry):
            out[i] = lanes(src[i // 8], in_grp + 16 * (i % 8))
            return carry
        lax.fori_loop(0, 16, one, 0, unroll=True)

    def product(acc, left, right):
        def pivot(k, acc):
            return jnp.minimum(acc, left(k)[:, None] + right[k // 8, :, pl.ds(k % 8, 1), :][None])
        return lax.fori_loop(0, BLK, pivot, acc, unroll=True)

    def close_and_send(rnd, x):
        close(rnd, x)
        send_dia(rnd)

    slot_r = jnp.where(my_row == 0, 0, ROUNDS)
    slot_c = jnp.where(col == 0, 0, ROUNDS)
    for a in range(2):
        for x in range(4):
            for r in range(2):
                tiles = swap_chunks(in_ref[a, 64 * r:64 * r + 64, BLK * x:BLK * x + BLK].reshape(8, 8, 128))
                mat[a, x, r] = tiles
                if a == 0:
                    rowp[slot_r, x, r] = tiles
                if x == 0:
                    colp[slot_c, a, r] = tiles

    pl.semaphore_wait(barrier, 7)

    @pl.when((my_row == 0) & (col == 0))
    def _():
        close_and_send(0, 0)

    @pl.when(my_row == 0)
    def _():
        for x in range(4):
            send_row(0, x)

    @pl.when(col == 0)
    def _():
        for a in range(2):
            col_copy(0, a).start()

    def one_round(k, carry):
        n = k + 1
        more = n < ROUNDS
        own_row = (my_row == n % 4) & more
        own_col = (col == n % 2) & more
        a1 = jnp.minimum(n // 4, 1)
        x1 = jnp.minimum((n + jnp.where(col == n % 2, 0, 1)) // 2, 3)

        @pl.when((my_row != k % 4) | (col != k % 2))
        def _():
            dia_copy(k, 0).wait_recv()

        def wait_row(x):
            @pl.when(my_row != k % 4)
            def _():
                row_copy(k, x, 0).wait_recv()

        make_brep(dst.at[k], brepd)
        wait_row(x1)
        make_brep(rowp.at[k, x1], brep.at[x1])

        def head(h, carry):
            a = jnp.where(h == 0, a1, 1 - a1)

            @pl.when(col != k % 2)
            def _():
                col_copy(k, a).wait_recv()

            pan = colp.at[k, a]
            cpr[...] = product(pan[...], lambda p: lanes(pan[:, p // 16], grp_base + p % 16), brepd)
            tab = cb.at[a]

            def fly(p):
                avs = lanes(cpr[:, p // 16], grp_base + p % 16)
                tab[p] = avs
                return avs
            acc = product(mat[a, x1], fly, brep.at[x1])
            mat[a, x1] = acc
            send_it = own_row & (h == 0)
            rowp[jnp.where(send_it, n, ROUNDS), x1] = acc
            colp[jnp.where(own_col, n, ROUNDS), a] = acc

            @pl.when(send_it)
            def _():
                send_row(n, x1)

            @pl.when(own_col)
            def _():
                col_copy(n, a).start()

            @pl.when(send_it & own_col)
            def _():
                close_and_send(n, x1)
            return carry
        lax.fori_loop(0, 2, head, 0)

        def tail(t, carry):
            h = t // 3
            a = jnp.where(h == 0, a1, 1 - a1)
            x = (x1 + 1 + t % 3) % 4

            @pl.when(h == 0)
            def _():
                wait_row(x)
                make_brep(rowp.at[k, x], brep.at[x])

            tab = cb.at[a]
            acc = product(mat[a, x], lambda p: tab[p], brep.at[x])
            mat[a, x] = acc
            send_it = own_row & (h == 0)
            rowp[jnp.where(send_it, n, ROUNDS), x] = acc

            @pl.when(send_it)
            def _():
                send_row(n, x)
            return carry
        lax.fori_loop(0, 6, tail, 0)
        return carry
    lax.fori_loop(0, ROUNDS, one_round, 0)

    for a in range(2):
        for x in range(4):
            for r in range(2):
                tiles = swap_chunks(mat[a, x, r])
                out_ref[a, 64 * r:64 * r + 64, BLK * x:BLK * x + BLK] = tiles.reshape(64, 128)

    def drain(k, carry):
        @pl.when(my_row == k % 4)
        def _():
            for x in range(4):
                for i in range(3):
                    row_copy(k, x, i).wait_send()

        @pl.when(col == k % 2)
        def _():
            for a in range(2):
                col_copy(k, a).wait_send()

        @pl.when((my_row == k % 4) & (col == k % 2))
        def _():
            for i in range(7):
                dia_copy(k, i).wait_send()
        return carry
    lax.fori_loop(0, ROUNDS, drain, 0)


def solution(mesh):
    spec = P(('parts', 'row', 'sub'), None, 'col')
    tile = (8, 128)
    dma = pltpu.SemaphoreType.DMA

    def local_run(local_dist):
        return pl.pallas_call(
            kernel,
            out_shape=jax.ShapeDtypeStruct(local_dist.shape, local_dist.dtype),
            in_specs=[pl.BlockSpec(memory_space=pltpu.VMEM)],
            out_specs=pl.BlockSpec(memory_space=pltpu.VMEM),
            scratch_shapes=[
                pltpu.VMEM((2, 4, 2, 8) + tile, jnp.float32),
                pltpu.VMEM((ROUNDS + 1, 4, 2, 8) + tile, jnp.float32),
                pltpu.VMEM((ROUNDS + 1, 2, 2, 8) + tile, jnp.float32),
                pltpu.VMEM((ROUNDS, 2, 8) + tile, jnp.float32),
                pltpu.VMEM((2, BLK, 2) + tile, jnp.float32),
                pltpu.VMEM((4, 16, 8) + tile, jnp.float32),
                pltpu.VMEM((16, 8) + tile, jnp.float32),
                pltpu.VMEM((2, 8) + tile, jnp.float32),
                dma((ROUNDS, 4, 3)), dma((ROUNDS, 4)),
                dma((ROUNDS, 2)), dma((ROUNDS, 2)),
                dma((ROUNDS, 7)), dma((ROUNDS,)),
            ],
            compiler_params=pltpu.CompilerParams(collective_id=0, has_side_effects=True),
            name='apsp',
        )(local_dist)

    return jax.shard_map(local_run, mesh=mesh, in_specs=(spec,), out_specs=spec, check_vma=False)
```

```python
import functools

import jax
import jax.numpy as jnp
from jax import lax
from jax.experimental import pallas as pl
from jax.experimental.pallas import tpu as pltpu
from jax.sharding import PartitionSpec as P

MESH = pl.DeviceIdType.MESH
BLK = 128
ROUNDS = 8
ROW_PEERS = ((0, 1), (1, 1), (1, 0))
ALL_PEERS = ((1, 0, 1), (1, 1, 1), (0, 0, 1), (0, 1, 1), (1, 0, 0), (0, 1, 0), (1, 1, 0))


def lanes(tiles, idx):
    flat = tiles.reshape(-1, 128)
    idx = jnp.broadcast_to(idx[None], (flat.shape[0] // 8, 8, 128)).reshape(-1, 128)
    return jnp.take_along_axis(flat, idx, axis=1, mode='promise_in_bounds').reshape(tiles.shape)


def kernel(in_ref, out_ref, mat, rowp, colp, dst, cb, brep, brepd, cpr,

           row_send, row_recv, col_send, col_recv, dia_send, dia_fwd, dia_recv):
    row, sub, col = lax.axis_index('row'), lax.axis_index('sub'), lax.axis_index('col')
    my_row = row * 2 + sub
    lane = lax.broadcasted_iota(jnp.int32, (8, 128), 1)
    in_grp = lane & 15
    grp_base = lane - in_grp

    def peer(d_col, d_row, d_sub):
        return {'col': (col + d_col) % 2, 'row': (row + d_row) % 2, 'sub': (sub + d_sub) % 2}

    barrier = pltpu.get_barrier_semaphore()
    for offs in ALL_PEERS:
        pl.semaphore_signal(barrier, inc=1, device_id=peer(*offs), device_id_type=MESH)

    def swap_chunks(tiles):
        for bit in (1, 2, 4):
            mask = (lane & (16 * bit)) == 0
            pairs = tiles.reshape(8 // (2 * bit), 2, bit, 8, 128)
            lo, hi = pairs[:, 0].reshape(-1, 128), pairs[:, 1].reshape(-1, 128)
            lo_up = pltpu.roll(lo, 128 - 16 * bit, 1)
            hi_up = pltpu.roll(hi, 16 * bit, 1)
            lo, hi, lo_up, hi_up = (v.reshape(8 // (2 * bit), bit, 8, 128) for v in (lo, hi, lo_up, hi_up))
            tiles = jnp.stack([jnp.where(mask, lo, hi_up), jnp.where(mask, lo_up, hi)], axis=1).reshape(8, 8, 128)
        return tiles

    def row_copy(rnd, x, i):
        d_row, d_sub = ROW_PEERS[i]
        return pltpu.make_async_remote_copy(
            src_ref=rowp.at[rnd, x], dst_ref=rowp.at[rnd, x],
            send_sem=row_send.at[rnd, x, i], recv_sem=row_recv.at[rnd, x],
            device_id=peer(0, d_row, d_sub), device_id_type=MESH)

    def col_copy(rnd, a):
        return pltpu.make_async_remote_copy(
            src_ref=colp.at[rnd, a], dst_ref=colp.at[rnd, a],
            send_sem=col_send.at[rnd, a], recv_sem=col_recv.at[rnd, a],
            device_id=peer(1, 0, 0), device_id_type=MESH)

    def dia_copy(rnd, i):
        turn = rnd % 2
        offs = ((1, turn, 1), (1, 1 - turn, 1), (0, 1, 1), (0, 0, 1))[i]
        return pltpu.make_async_remote_copy(
            src_ref=dst.at[rnd], dst_ref=dst.at[rnd],
            send_sem=dia_send.at[rnd, i], recv_sem=dia_recv.at[rnd],
            device_id=peer(*offs), device_id_type=MESH)

    def dia_pass(rnd):
        return pltpu.make_async_remote_copy(
            src_ref=dst.at[rnd], dst_ref=dst.at[rnd],
            send_sem=dia_fwd.at[rnd], recv_sem=dia_recv.at[rnd],
            device_id=peer(0, 0, 1), device_id_type=MESH)

    def passes(rnd):
        return (sub != rnd % 2) & ((col != rnd % 2) | (row != (rnd % 4) // 2))

    def send_row(rnd, x):
        for i in range(3):
            row_copy(rnd, x, i).start()

    def send_dia(rnd):
        for i in range(4):
            dia_copy(rnd, i).start()

    def close(rnd, a, x):
        dst[rnd] = mat[a, x]

        def group(g, carry):
            rg, q = g // 8, g % 8
            cg, half = g // 2, (g % 2) * 8
            pivot_tile = dst[rnd, rg, cg]
            ucol = [lanes(pivot_tile, jnp.full((8, 128), 16 * q + half + p, jnp.int32)) for p in range(8)]
            rows = lanes(dst[rnd, rg], in_grp + 16 * q)
            left = [lanes(dst[rnd, :, cg], grp_base + (half + p)) for p in range(8)]
            for p in range(8):
                for j in range(p + 1, 8):
                    ucol[j] = jnp.minimum(ucol[j], ucol[p] + ucol[j][p:p + 1, :])
                rows = jnp.minimum(rows, ucol[p][None] + rows[:, p:p + 1, :])
            acc = dst[rnd]
            for p in range(8):
                acc = jnp.minimum(acc, left[p][:, None] + rows[:, p:p + 1, :][None])
            dst[rnd] = acc
            return carry
        lax.fori_loop(0, 16, group, 0)

    def make_brep(src, out):
        def one(i, carry):
            out[i] = lanes(src[i // 8], in_grp + 16 * (i % 8))
            return carry
        lax.fori_loop(0, 16, one, 0, unroll=True)

    def product(acc, left, right):
        def pivot(k, acc):
            return jnp.minimum(acc, left(k)[:, None] + right[k // 8, :, pl.ds(k % 8, 1), :][None])
        return lax.fori_loop(0, BLK, pivot, acc, unroll=True)

    def close_and_send(rnd, a, x):
        close(rnd, a, x)
        send_dia(rnd)

    slot_r = jnp.where(my_row == 0, 0, ROUNDS)
    slot_c = jnp.where(col == 0, 0, ROUNDS)
    for a in range(2):
        for x in range(4):
            for r in range(2):
                tiles = swap_chunks(in_ref[a, 64 * r:64 * r + 64, BLK * x:BLK * x + BLK].reshape(8, 8, 128))
                mat[a, x, r] = tiles
                if a == 0:
                    rowp[slot_r, x, r] = tiles
                if x == 0:
                    colp[slot_c, a, r] = tiles

    pl.semaphore_wait(barrier, 7)

    @pl.when((my_row == 0) & (col == 0))
    def _():
        close_and_send(0, 0, 0)

    @pl.when(my_row == 0)
    def _():
        for x in range(4):
            if x == 0:
                @pl.when(col != 0)
                def _():
                    send_row(0, 0)
            else:
                send_row(0, x)

    @pl.when(col == 0)
    def _():
        @pl.when(my_row != 0)
        def _():
            col_copy(0, 0).start()
        col_copy(0, 1).start()

    def one_round(k, carry):
        n = k + 1
        more = n < ROUNDS
        own_row = (my_row == n % 4) & more
        own_col = (col == n % 2) & more
        a1 = jnp.minimum(n // 4, 1)
        x1 = ((n + jnp.where(col == n % 2, 0, 1)) // 2) % 4
        xk = k // 2
        is_row, is_col = my_row == k % 4, col == k % 2

        @pl.when(~is_row | ~is_col)
        def _():
            dia_copy(k, 0).wait_recv()

        @pl.when(passes(k))
        def _():
            dia_pass(k).start()

        def wait_row(x):
            @pl.when(~is_row)
            def _():
                row_copy(k, x, 0).wait_recv()

        make_brep(dst.at[k], brepd)
        wait_row(x1)
        make_brep(rowp.at[k, x1], brep.at[x1])

        def head(h, carry):
            a = jnp.where(h == 0, a1, 1 - a1)

            on_diag = is_row & (a == k // 4)
            send_it = own_row & (h == 0)

            @pl.when(~is_col & ~on_diag)
            def _():
                col_copy(k, a).wait_recv()

            @pl.when(on_diag)
            def _():
                cpr[...] = dst[k]

            @pl.when(~on_diag)
            def _():
                pan = colp.at[k, a]
                cpr[...] = product(pan[...], lambda p: lanes(pan[:, p // 16], grp_base + p % 16), brepd)

            @pl.when(is_col)
            def _():
                mat[a, xk] = cpr[...]

            @pl.when(is_col & send_it)
            def _():
                rowp[n, xk] = cpr[...]
                send_row(n, xk)

            tab = cb.at[a]

            def fly(p):
                avs = lanes(cpr[:, p // 16], grp_base + p % 16)
                tab[p] = avs
                return avs
            acc = product(mat[a, x1], fly, brep.at[x1])
            mat[a, x1] = acc
            rowp[jnp.where(send_it, n, ROUNDS), x1] = acc
            colp[jnp.where(own_col, n, ROUNDS), a] = acc

            @pl.when(send_it & ~own_col)
            def _():
                send_row(n, x1)

            @pl.when(own_col & ~send_it)
            def _():
                col_copy(n, a).start()

            @pl.when(send_it & own_col)
            def _():
                close_and_send(n, a, x1)
            return carry
        lax.fori_loop(0, 2, head, 0)

        def tail(t, carry):
            h = t // 3
            a = jnp.where(h == 0, a1, 1 - a1)
            x = (x1 + 1 + t % 3) % 4

            @pl.when((col != k % 2) | (t % 3 != 2))
            def _():
                @pl.when(h == 0)
                def _():
                    wait_row(x)
                    make_brep(rowp.at[k, x], brep.at[x])

                tab = cb.at[a]
                acc = product(mat[a, x], lambda p: tab[p], brep.at[x])
                mat[a, x] = acc
                send_it = own_row & (h == 0)
                rowp[jnp.where(send_it, n, ROUNDS), x] = acc

                @pl.when(send_it)
                def _():
                    send_row(n, x)
            return carry
        lax.fori_loop(0, 6, tail, 0)
        return carry
    lax.fori_loop(0, ROUNDS, one_round, 0)

    for a in range(2):
        for x in range(4):
            for r in range(2):
                tiles = swap_chunks(mat[a, x, r])
                out_ref[a, 64 * r:64 * r + 64, BLK * x:BLK * x + BLK] = tiles.reshape(64, 128)

    def drain(k, carry):
        is_row, is_col = my_row == k % 4, col == k % 2
        for x in range(4):
            @pl.when(is_row & (~is_col | (x != k // 2)))
            def _():
                for i in range(3):
                    row_copy(k, x, i).wait_send()
        for a in range(2):
            @pl.when(is_col & (~is_row | (a != k // 4)))
            def _():
                col_copy(k, a).wait_send()

        @pl.when(is_row & is_col)
        def _():
            for i in range(4):
                dia_copy(k, i).wait_send()

        @pl.when(passes(k))
        def _():
            dia_pass(k).wait_send()
        return carry
    lax.fori_loop(0, ROUNDS, drain, 0)


def solution(mesh):
    spec = P(('parts', 'row', 'sub'), None, 'col')
    tile = (8, 128)
    dma = pltpu.SemaphoreType.DMA

    def local_run(local_dist):
        return pl.pallas_call(
            kernel,
            out_shape=jax.ShapeDtypeStruct(local_dist.shape, local_dist.dtype),
            in_specs=[pl.BlockSpec(memory_space=pltpu.VMEM)],
            out_specs=pl.BlockSpec(memory_space=pltpu.VMEM),
            scratch_shapes=[
                pltpu.VMEM((2, 4, 2, 8) + tile, jnp.float32),
                pltpu.VMEM((ROUNDS + 1, 4, 2, 8) + tile, jnp.float32),
                pltpu.VMEM((ROUNDS + 1, 2, 2, 8) + tile, jnp.float32),
                pltpu.VMEM((ROUNDS, 2, 8) + tile, jnp.float32),
                pltpu.VMEM((2, BLK, 2) + tile, jnp.float32),
                pltpu.VMEM((4, 16, 8) + tile, jnp.float32),
                pltpu.VMEM((16, 8) + tile, jnp.float32),
                pltpu.VMEM((2, 8) + tile, jnp.float32),
                dma((ROUNDS, 4, 3)), dma((ROUNDS, 4)),
                dma((ROUNDS, 2)), dma((ROUNDS, 2)),
                dma((ROUNDS, 4)), dma((ROUNDS,)), dma((ROUNDS,)),
            ],
            compiler_params=pltpu.CompilerParams(collective_id=0, has_side_effects=True),
            name='apsp',
        )(local_dist)

    return jax.shard_map(local_run, mesh=mesh, in_specs=(spec,), out_specs=spec, check_vma=False)
```

```python
import functools

import jax
import jax.numpy as jnp
from jax import lax
from jax.experimental import pallas as pl
from jax.experimental.pallas import tpu as pltpu
from jax.sharding import PartitionSpec as P

MESH = pl.DeviceIdType.MESH
BLK = 128
ROUNDS = 8
HEAD_STEP, TAIL_STEP = 128, 64
ROW_PEERS = ((0, 1), (1, 1), (1, 0))
ALL_PEERS = ((1, 0, 1), (1, 1, 1), (0, 0, 1), (0, 1, 1), (1, 0, 0), (0, 1, 0), (1, 1, 0))


def lanes(tiles, idx):
    flat = tiles.reshape(-1, 128)
    idx = jnp.broadcast_to(idx[None], (flat.shape[0] // 8, 8, 128)).reshape(-1, 128)
    return jnp.take_along_axis(flat, idx, axis=1, mode='promise_in_bounds').reshape(tiles.shape)


def kernel(in_ref, out_ref, mat, rowp, colp, dst, cb, brep, brepd, cpr,

           row_send, row_recv, col_send, col_recv, dia_send, dia_fwd, dia_recv):
    row, sub, col = lax.axis_index('row'), lax.axis_index('sub'), lax.axis_index('col')
    my_row = row * 2 + sub
    lane = lax.broadcasted_iota(jnp.int32, (8, 128), 1)
    in_grp = lane & 15
    grp_base = lane - in_grp

    def peer(d_col, d_row, d_sub):
        return {'col': (col + d_col) % 2, 'row': (row + d_row) % 2, 'sub': (sub + d_sub) % 2}

    barrier = pltpu.get_barrier_semaphore()
    for offs in ALL_PEERS:
        pl.semaphore_signal(barrier, inc=1, device_id=peer(*offs), device_id_type=MESH)

    def swap_chunks(tiles):
        for bit in (1, 2, 4):
            mask = (lane & (16 * bit)) == 0
            pairs = tiles.reshape(8 // (2 * bit), 2, bit, 8, 128)
            lo, hi = pairs[:, 0].reshape(-1, 128), pairs[:, 1].reshape(-1, 128)
            lo_up = pltpu.roll(lo, 128 - 16 * bit, 1)
            hi_up = pltpu.roll(hi, 16 * bit, 1)
            lo, hi, lo_up, hi_up = (v.reshape(8 // (2 * bit), bit, 8, 128) for v in (lo, hi, lo_up, hi_up))
            tiles = jnp.stack([jnp.where(mask, lo, hi_up), jnp.where(mask, lo_up, hi)], axis=1).reshape(8, 8, 128)
        return tiles

    def row_copy(rnd, x, i):
        d_row, d_sub = ROW_PEERS[i]
        return pltpu.make_async_remote_copy(
            src_ref=rowp.at[rnd, x], dst_ref=rowp.at[rnd, x],
            send_sem=row_send.at[rnd, x, i], recv_sem=row_recv.at[rnd, x],
            device_id=peer(0, d_row, d_sub), device_id_type=MESH)

    def col_copy(rnd, a):
        return pltpu.make_async_remote_copy(
            src_ref=colp.at[rnd, a], dst_ref=colp.at[rnd, a],
            send_sem=col_send.at[rnd, a], recv_sem=col_recv.at[rnd, a],
            device_id=peer(1, 0, 0), device_id_type=MESH)

    def dia_copy(rnd, i):
        turn = rnd % 2
        offs = ((1, turn, 1), (1, 1 - turn, 1), (0, 1, 1), (0, 0, 1))[i]
        return pltpu.make_async_remote_copy(
            src_ref=dst.at[rnd], dst_ref=dst.at[rnd],
            send_sem=dia_send.at[rnd, i], recv_sem=dia_recv.at[rnd],
            device_id=peer(*offs), device_id_type=MESH)

    def dia_pass(rnd):
        return pltpu.make_async_remote_copy(
            src_ref=dst.at[rnd], dst_ref=dst.at[rnd],
            send_sem=dia_fwd.at[rnd], recv_sem=dia_recv.at[rnd],
            device_id=peer(0, 0, 1), device_id_type=MESH)

    def passes(rnd):
        return (sub != rnd % 2) & ((col != rnd % 2) | (row != (rnd % 4) // 2))

    def send_row(rnd, x):
        for i in range(3):
            row_copy(rnd, x, i).start()

    def send_dia(rnd):
        for i in range(4):
            dia_copy(rnd, i).start()

    def close(rnd, a, x):
        dst[rnd] = mat[a, x]

        def group(g, carry):
            rg, q = g // 8, g % 8
            cg, half = g // 2, (g % 2) * 8
            pivot_tile = dst[rnd, rg, cg]
            ucol = [lanes(pivot_tile, jnp.full((8, 128), 16 * q + half + p, jnp.int32)) for p in range(8)]
            rows = lanes(dst[rnd, rg], in_grp + 16 * q)
            left = [lanes(dst[rnd, :, cg], grp_base + (half + p)) for p in range(8)]
            for p in range(8):
                for j in range(p + 1, 8):
                    ucol[j] = jnp.minimum(ucol[j], ucol[p] + ucol[j][p:p + 1, :])
                rows = jnp.minimum(rows, ucol[p][None] + rows[:, p:p + 1, :])
            acc = dst[rnd]
            for p in range(8):
                acc = jnp.minimum(acc, left[p][:, None] + rows[:, p:p + 1, :][None])
            dst[rnd] = acc
            return carry
        lax.fori_loop(0, 16, group, 0)

    def make_brep(src, out):
        def one(i, carry):
            out[i] = lanes(src[i // 8], in_grp + 16 * (i % 8))
            return carry
        lax.fori_loop(0, 16, one, 0, unroll=True)

    def product(acc, left, right, step):
        def chunk(i, acc):
            def pivot(u, acc):
                b = right[i * (step // 8) + u // 8, :, pl.ds(u % 8, 1), :]
                return jnp.minimum(acc, left(i * (step // 16) + u // 16, i * step + u, u % 16)[:, None] + b[None])
            return lax.fori_loop(0, step, pivot, acc, unroll=True)
        return lax.fori_loop(0, BLK // step, chunk, acc, unroll=step == BLK)

    def close_and_send(rnd, a, x):
        close(rnd, a, x)
        send_dia(rnd)

    slot_r = jnp.where(my_row == 0, 0, ROUNDS)
    slot_c = jnp.where(col == 0, 0, ROUNDS)
    for a in range(2):
        for x in range(4):
            for r in range(2):
                tiles = swap_chunks(in_ref[a, 64 * r:64 * r + 64, BLK * x:BLK * x + BLK].reshape(8, 8, 128))
                mat[a, x, r] = tiles
                if a == 0:
                    rowp[slot_r, x, r] = tiles
                if x == 0:
                    colp[slot_c, a, r] = tiles

    pl.semaphore_wait(barrier, 7)

    @pl.when((my_row == 0) & (col == 0))
    def _():
        close_and_send(0, 0, 0)

    @pl.when(my_row == 0)
    def _():
        for x in range(4):
            if x == 0:
                @pl.when(col != 0)
                def _():
                    send_row(0, 0)
            else:
                send_row(0, x)

    @pl.when(col == 0)
    def _():
        @pl.when(my_row != 0)
        def _():
            col_copy(0, 0).start()
        col_copy(0, 1).start()

    def one_round(k, carry):
        n = k + 1
        more = n < ROUNDS
        own_row = (my_row == n % 4) & more
        own_col = (col == n % 2) & more
        a1 = jnp.minimum(n // 4, 1)
        x1 = ((n + jnp.where(col == n % 2, 0, 1)) // 2) % 4
        xk = k // 2
        is_row, is_col = my_row == k % 4, col == k % 2

        @pl.when(~is_row | ~is_col)
        def _():
            dia_copy(k, 0).wait_recv()

        @pl.when(passes(k))
        def _():
            dia_pass(k).start()

        def wait_row(x):
            @pl.when(~is_row)
            def _():
                row_copy(k, x, 0).wait_recv()

        make_brep(dst.at[k], brepd)
        wait_row(x1)
        make_brep(rowp.at[k, x1], brep.at[x1])

        def head(h, carry):
            a = jnp.where(h == 0, a1, 1 - a1)

            on_diag = is_row & (a == k // 4)
            send_it = own_row & (h == 0)

            @pl.when(~is_col & ~on_diag)
            def _():
                col_copy(k, a).wait_recv()

            @pl.when(on_diag)
            def _():
                cpr[...] = dst[k]

            @pl.when(~on_diag)
            def _():
                pan = colp.at[k, a]
                cpr[...] = product(pan[...], lambda c, p, l: lanes(pan[:, c], grp_base + l), brepd, HEAD_STEP)

            @pl.when(is_col)
            def _():
                mat[a, xk] = cpr[...]

            @pl.when(is_col & send_it)
            def _():
                rowp[n, xk] = cpr[...]
                send_row(n, xk)

            tab = cb.at[a]

            def fly(c, p, l):
                avs = lanes(cpr[:, c], grp_base + l)
                tab[p] = avs
                return avs
            acc = product(mat[a, x1], fly, brep.at[x1], HEAD_STEP)
            mat[a, x1] = acc
            rowp[jnp.where(send_it, n, ROUNDS), x1] = acc
            colp[jnp.where(own_col, n, ROUNDS), a] = acc

            @pl.when(send_it & ~own_col)
            def _():
                send_row(n, x1)

            @pl.when(own_col & ~send_it)
            def _():
                col_copy(n, a).start()

            @pl.when(send_it & own_col)
            def _():
                close_and_send(n, a, x1)
            return carry
        lax.fori_loop(0, 2, head, 0)

        def tail(t, carry):
            h = t // 3
            a = jnp.where(h == 0, a1, 1 - a1)
            x = (x1 + 1 + t % 3) % 4

            @pl.when((col != k % 2) | (t % 3 != 2))
            def _():
                @pl.when(h == 0)
                def _():
                    wait_row(x)
                    make_brep(rowp.at[k, x], brep.at[x])

                tab = cb.at[a]
                acc = product(mat[a, x], lambda c, p, l: tab[p], brep.at[x], TAIL_STEP)
                mat[a, x] = acc
                send_it = own_row & (h == 0)
                rowp[jnp.where(send_it, n, ROUNDS), x] = acc

                @pl.when(send_it)
                def _():
                    send_row(n, x)
            return carry
        lax.fori_loop(0, 6, tail, 0)
        return carry
    lax.fori_loop(0, ROUNDS, one_round, 0)

    for a in range(2):
        for x in range(4):
            for r in range(2):
                tiles = swap_chunks(mat[a, x, r])
                out_ref[a, 64 * r:64 * r + 64, BLK * x:BLK * x + BLK] = tiles.reshape(64, 128)

    def drain(k, carry):
        is_row, is_col = my_row == k % 4, col == k % 2
        for x in range(4):
            @pl.when(is_row & (~is_col | (x != k // 2)))
            def _():
                for i in range(3):
                    row_copy(k, x, i).wait_send()
        for a in range(2):
            @pl.when(is_col & (~is_row | (a != k // 4)))
            def _():
                col_copy(k, a).wait_send()

        @pl.when(is_row & is_col)
        def _():
            for i in range(4):
                dia_copy(k, i).wait_send()

        @pl.when(passes(k))
        def _():
            dia_pass(k).wait_send()
        return carry
    lax.fori_loop(0, ROUNDS, drain, 0)


def solution(mesh):
    spec = P(('parts', 'row', 'sub'), None, 'col')
    tile = (8, 128)
    dma = pltpu.SemaphoreType.DMA

    def local_run(local_dist):
        return pl.pallas_call(
            kernel,
            out_shape=jax.ShapeDtypeStruct(local_dist.shape, local_dist.dtype),
            in_specs=[pl.BlockSpec(memory_space=pltpu.VMEM)],
            out_specs=pl.BlockSpec(memory_space=pltpu.VMEM),
            scratch_shapes=[
                pltpu.VMEM((2, 4, 2, 8) + tile, jnp.float32),
                pltpu.VMEM((ROUNDS + 1, 4, 2, 8) + tile, jnp.float32),
                pltpu.VMEM((ROUNDS + 1, 2, 2, 8) + tile, jnp.float32),
                pltpu.VMEM((ROUNDS, 2, 8) + tile, jnp.float32),
                pltpu.VMEM((2, BLK, 2) + tile, jnp.float32),
                pltpu.VMEM((4, 16, 8) + tile, jnp.float32),
                pltpu.VMEM((16, 8) + tile, jnp.float32),
                pltpu.VMEM((2, 8) + tile, jnp.float32),
                dma((ROUNDS, 4, 3)), dma((ROUNDS, 4)),
                dma((ROUNDS, 2)), dma((ROUNDS, 2)),
                dma((ROUNDS, 4)), dma((ROUNDS,)), dma((ROUNDS,)),
            ],
            compiler_params=pltpu.CompilerParams(collective_id=0, has_side_effects=True),
            name='apsp',
        )(local_dist)

    return jax.shard_map(local_run, mesh=mesh, in_specs=(spec,), out_specs=spec, check_vma=False)
```

```python
import functools

import jax
import jax.numpy as jnp
from jax import lax
from jax.experimental import pallas as pl
from jax.experimental.pallas import tpu as pltpu
from jax.sharding import PartitionSpec as P

MESH = pl.DeviceIdType.MESH
BLK = 128
ROUNDS = 8
HEAD_STEP, TAIL_STEP = 64, 64
ROW_PEERS = ((0, 1), (1, 1), (1, 0))
ALL_PEERS = ((1, 0, 1), (1, 1, 1), (0, 0, 1), (0, 1, 1), (1, 0, 0), (0, 1, 0), (1, 1, 0))


def lanes(tiles, idx):
    flat = tiles.reshape(-1, 128)
    idx = jnp.broadcast_to(idx[None], (flat.shape[0] // 8, 8, 128)).reshape(-1, 128)
    return jnp.take_along_axis(flat, idx, axis=1, mode='promise_in_bounds').reshape(tiles.shape)


def kernel(in_ref, out_ref, mat, rowp, colp, dst, cb, brep, brepd, cpr,

           row_send, row_recv, col_send, col_recv, dia_send, dia_fwd, dia_recv):
    row, sub, col = lax.axis_index('row'), lax.axis_index('sub'), lax.axis_index('col')
    my_row = row * 2 + sub
    lane = lax.broadcasted_iota(jnp.int32, (8, 128), 1)
    in_grp = lane & 15
    grp_base = lane - in_grp

    def peer(d_col, d_row, d_sub):
        return {'col': (col + d_col) % 2, 'row': (row + d_row) % 2, 'sub': (sub + d_sub) % 2}

    barrier = pltpu.get_barrier_semaphore()
    for offs in ALL_PEERS:
        pl.semaphore_signal(barrier, inc=1, device_id=peer(*offs), device_id_type=MESH)

    def swap_chunks(tiles):
        for bit in (1, 2, 4):
            mask = (lane & (16 * bit)) == 0
            pairs = tiles.reshape(8 // (2 * bit), 2, bit, 8, 128)
            lo, hi = pairs[:, 0].reshape(-1, 128), pairs[:, 1].reshape(-1, 128)
            lo_up = pltpu.roll(lo, 128 - 16 * bit, 1)
            hi_up = pltpu.roll(hi, 16 * bit, 1)
            lo, hi, lo_up, hi_up = (v.reshape(8 // (2 * bit), bit, 8, 128) for v in (lo, hi, lo_up, hi_up))
            tiles = jnp.stack([jnp.where(mask, lo, hi_up), jnp.where(mask, lo_up, hi)], axis=1).reshape(8, 8, 128)
        return tiles

    def row_copy(rnd, x, i):
        d_row, d_sub = ROW_PEERS[i]
        return pltpu.make_async_remote_copy(
            src_ref=rowp.at[rnd, x], dst_ref=rowp.at[rnd, x],
            send_sem=row_send.at[rnd, x, i], recv_sem=row_recv.at[rnd, x],
            device_id=peer(0, d_row, d_sub), device_id_type=MESH)

    def col_copy(rnd, a):
        return pltpu.make_async_remote_copy(
            src_ref=colp.at[rnd, a], dst_ref=colp.at[rnd, a],
            send_sem=col_send.at[rnd, a], recv_sem=col_recv.at[rnd, a],
            device_id=peer(1, 0, 0), device_id_type=MESH)

    def dia_copy(rnd, i):
        turn = rnd % 2
        offs = ((1, turn, 1), (1, 1 - turn, 1), (0, 1, 1), (0, 0, 1))[i]
        return pltpu.make_async_remote_copy(
            src_ref=dst.at[rnd], dst_ref=dst.at[rnd],
            send_sem=dia_send.at[rnd, i], recv_sem=dia_recv.at[rnd],
            device_id=peer(*offs), device_id_type=MESH)

    def dia_pass(rnd):
        return pltpu.make_async_remote_copy(
            src_ref=dst.at[rnd], dst_ref=dst.at[rnd],
            send_sem=dia_fwd.at[rnd], recv_sem=dia_recv.at[rnd],
            device_id=peer(0, 0, 1), device_id_type=MESH)

    def passes(rnd):
        return (sub != rnd % 2) & ((col != rnd % 2) | (row != (rnd % 4) // 2))

    def send_row(rnd, x):
        for i in range(3):
            row_copy(rnd, x, i).start()

    def send_dia(rnd):
        for i in range(4):
            dia_copy(rnd, i).start()

    def close(rnd, a, x):
        dst[rnd] = mat[a, x]

        def group(g, carry):
            rg, q = g // 8, g % 8
            cg, half = g // 2, (g % 2) * 8
            pivot_tile = dst[rnd, rg, cg]
            ucol = [lanes(pivot_tile, jnp.full((8, 128), 16 * q + half + p, jnp.int32)) for p in range(8)]
            rows = lanes(dst[rnd, rg], in_grp + 16 * q)
            left = [lanes(dst[rnd, :, cg], grp_base + (half + p)) for p in range(8)]
            for p in range(8):
                for j in range(p + 1, 8):
                    ucol[j] = jnp.minimum(ucol[j], ucol[p] + ucol[j][p:p + 1, :])
                rows = jnp.minimum(rows, ucol[p][None] + rows[:, p:p + 1, :])
            acc = dst[rnd]
            for p in range(8):
                acc = jnp.minimum(acc, left[p][:, None] + rows[:, p:p + 1, :][None])
            dst[rnd] = acc
            return carry
        lax.fori_loop(0, 16, group, 0)

    def make_brep(src, out):
        def one(i, carry):
            out[i] = lanes(src[i // 8], in_grp + 16 * (i % 8))
            return carry
        lax.fori_loop(0, 16, one, 0, unroll=True)

    def product(acc, left, right, step):
        def chunk(i, acc):
            def pivot(u, acc):
                b = right[i * (step // 8) + u // 8, :, pl.ds(u % 8, 1), :]
                return jnp.minimum(acc, left(i * (step // 16) + u // 16, i * step + u, u % 16)[:, None] + b[None])
            return lax.fori_loop(0, step, pivot, acc, unroll=True)
        return lax.fori_loop(0, BLK // step, chunk, acc, unroll=step == BLK)

    def close_and_send(rnd, a, x):
        close(rnd, a, x)
        send_dia(rnd)

    slot_r = jnp.where(my_row == 0, 0, ROUNDS)
    slot_c = jnp.where(col == 0, 0, ROUNDS)
    for a in range(2):
        for x in range(4):
            for r in range(2):
                tiles = swap_chunks(in_ref[a, 64 * r:64 * r + 64, BLK * x:BLK * x + BLK].reshape(8, 8, 128))
                mat[a, x, r] = tiles
                if a == 0:
                    rowp[slot_r, x, r] = tiles
                if x == 0:
                    colp[slot_c, a, r] = tiles

    pl.semaphore_wait(barrier, 7)

    @pl.when((my_row == 0) & (col == 0))
    def _():
        close_and_send(0, 0, 0)

    @pl.when(my_row == 0)
    def _():
        for x in range(4):
            if x == 0:
                @pl.when(col != 0)
                def _():
                    send_row(0, 0)
            else:
                send_row(0, x)

    @pl.when(col == 0)
    def _():
        @pl.when(my_row != 0)
        def _():
            col_copy(0, 0).start()
        col_copy(0, 1).start()

    def one_round(k, carry):
        n = k + 1
        more = n < ROUNDS
        own_row = (my_row == n % 4) & more
        own_col = (col == n % 2) & more
        a1 = jnp.minimum(n // 4, 1)
        x1 = ((n + jnp.where(col == n % 2, 0, 1)) // 2) % 4
        xk = k // 2
        is_row, is_col = my_row == k % 4, col == k % 2

        @pl.when(~is_row | ~is_col)
        def _():
            dia_copy(k, 0).wait_recv()

        @pl.when(passes(k))
        def _():
            dia_pass(k).start()

        def wait_row(x):
            @pl.when(~is_row)
            def _():
                row_copy(k, x, 0).wait_recv()

        make_brep(dst.at[k], brepd)
        wait_row(x1)
        make_brep(rowp.at[k, x1], brep.at[x1])

        def head(h, carry):
            a = jnp.where(h == 0, a1, 1 - a1)

            on_diag = is_row & (a == k // 4)
            send_it = own_row & (h == 0)

            @pl.when(~is_col & ~on_diag)
            def _():
                col_copy(k, a).wait_recv()

            @pl.when(on_diag)
            def _():
                cpr[...] = dst[k]

            @pl.when(~on_diag)
            def _():
                pan = colp.at[k, a]
                cpr[...] = product(pan[...], lambda c, p, l: lanes(pan[:, c], grp_base + l), brepd, HEAD_STEP)

            @pl.when(is_col)
            def _():
                mat[a, xk] = cpr[...]

            @pl.when(is_col & send_it)
            def _():
                rowp[n, xk] = cpr[...]
                send_row(n, xk)

            tab = cb.at[a]

            def fly(c, p, l):
                avs = lanes(cpr[:, c], grp_base + l)
                tab[p] = avs
                return avs
            acc = product(mat[a, x1], fly, brep.at[x1], HEAD_STEP)
            mat[a, x1] = acc
            rowp[jnp.where(send_it, n, ROUNDS), x1] = acc
            colp[jnp.where(own_col, n, ROUNDS), a] = acc

            @pl.when(send_it & ~own_col)
            def _():
                send_row(n, x1)

            @pl.when(own_col & ~send_it)
            def _():
                col_copy(n, a).start()

            @pl.when(send_it & own_col)
            def _():
                close_and_send(n, a, x1)
            return carry
        lax.fori_loop(0, 2, head, 0)

        def tail(t, carry):
            h = t // 3
            a = jnp.where(h == 0, a1, 1 - a1)
            x = (x1 + 1 + t % 3) % 4

            @pl.when((col != k % 2) | (t % 3 != 2))
            def _():
                @pl.when(h == 0)
                def _():
                    wait_row(x)
                    make_brep(rowp.at[k, x], brep.at[x])

                tab = cb.at[a]
                acc = product(mat[a, x], lambda c, p, l: tab[p], brep.at[x], TAIL_STEP)
                mat[a, x] = acc
                send_it = own_row & (h == 0)
                rowp[jnp.where(send_it, n, ROUNDS), x] = acc

                @pl.when(send_it)
                def _():
                    send_row(n, x)
            return carry
        lax.fori_loop(0, 6, tail, 0)
        return carry
    lax.fori_loop(0, ROUNDS, one_round, 0)

    for a in range(2):
        for x in range(4):
            for r in range(2):
                tiles = swap_chunks(mat[a, x, r])
                out_ref[a, 64 * r:64 * r + 64, BLK * x:BLK * x + BLK] = tiles.reshape(64, 128)

    def drain(k, carry):
        is_row, is_col = my_row == k % 4, col == k % 2
        for x in range(4):
            @pl.when(is_row & (~is_col | (x != k // 2)))
            def _():
                for i in range(3):
                    row_copy(k, x, i).wait_send()
        for a in range(2):
            @pl.when(is_col & (~is_row | (a != k // 4)))
            def _():
                col_copy(k, a).wait_send()

        @pl.when(is_row & is_col)
        def _():
            for i in range(4):
                dia_copy(k, i).wait_send()

        @pl.when(passes(k))
        def _():
            dia_pass(k).wait_send()
        return carry
    lax.fori_loop(0, ROUNDS, drain, 0)


def solution(mesh):
    spec = P(('parts', 'row', 'sub'), None, 'col')
    tile = (8, 128)
    dma = pltpu.SemaphoreType.DMA

    def local_run(local_dist):
        return pl.pallas_call(
            kernel,
            out_shape=jax.ShapeDtypeStruct(local_dist.shape, local_dist.dtype),
            in_specs=[pl.BlockSpec(memory_space=pltpu.VMEM)],
            out_specs=pl.BlockSpec(memory_space=pltpu.VMEM),
            scratch_shapes=[
                pltpu.VMEM((2, 4, 2, 8) + tile, jnp.float32),
                pltpu.VMEM((ROUNDS + 1, 4, 2, 8) + tile, jnp.float32),
                pltpu.VMEM((ROUNDS + 1, 2, 2, 8) + tile, jnp.float32),
                pltpu.VMEM((ROUNDS, 2, 8) + tile, jnp.float32),
                pltpu.VMEM((2, BLK, 2) + tile, jnp.float32),
                pltpu.VMEM((4, 16, 8) + tile, jnp.float32),
                pltpu.VMEM((16, 8) + tile, jnp.float32),
                pltpu.VMEM((2, 8) + tile, jnp.float32),
                dma((ROUNDS, 4, 3)), dma((ROUNDS, 4)),
                dma((ROUNDS, 2)), dma((ROUNDS, 2)),
                dma((ROUNDS, 4)), dma((ROUNDS,)), dma((ROUNDS,)),
            ],
            compiler_params=pltpu.CompilerParams(collective_id=0, has_side_effects=True),
            name='apsp',
        )(local_dist)

    return jax.shard_map(local_run, mesh=mesh, in_specs=(spec,), out_specs=spec, check_vma=False)
```

```python
import functools

import jax
import jax.numpy as jnp
from jax import lax
from jax.experimental import pallas as pl
from jax.experimental.pallas import tpu as pltpu
from jax.sharding import PartitionSpec as P

MESH = pl.DeviceIdType.MESH
BLK = 128
ROUNDS = 8
HEAD_STEP, TAIL_STEP = 128, 64
ROW_PEERS = ((0, 1), (1, 1), (1, 0))
ALL_PEERS = ((1, 0, 1), (1, 1, 1), (0, 0, 1), (0, 1, 1), (1, 0, 0), (0, 1, 0), (1, 1, 0))


def lanes(tiles, idx):
    flat = tiles.reshape(-1, 128)
    idx = jnp.broadcast_to(idx, tiles.shape).reshape(-1, 128)
    return jnp.take_along_axis(flat, idx, axis=1, mode='promise_in_bounds').reshape(tiles.shape)


def kernel(in_ref, out_ref, mat, rowp, colp, dst, cb, brep, brepd, cpr,

           row_send, row_recv, col_send, col_recv, dia_send, dia_fwd, dia_recv):
    row, sub, col = lax.axis_index('row'), lax.axis_index('sub'), lax.axis_index('col')
    my_row = row * 2 + sub
    lane = lax.broadcasted_iota(jnp.int32, (8, 128), 1)
    in_grp = lane & 15
    grp_base = lane - in_grp
    nth_pivot = lax.broadcasted_iota(jnp.int32, (8, 8, 128), 0)

    def peer(d_col, d_row, d_sub):
        return {'col': (col + d_col) % 2, 'row': (row + d_row) % 2, 'sub': (sub + d_sub) % 2}

    barrier = pltpu.get_barrier_semaphore()
    for offs in ALL_PEERS:
        pl.semaphore_signal(barrier, inc=1, device_id=peer(*offs), device_id_type=MESH)

    def swap_chunks(tiles):
        for bit in (1, 2, 4):
            mask = (lane & (16 * bit)) == 0
            pairs = tiles.reshape(8 // (2 * bit), 2, bit, 8, 128)
            lo, hi = pairs[:, 0].reshape(-1, 128), pairs[:, 1].reshape(-1, 128)
            lo_up = pltpu.roll(lo, 128 - 16 * bit, 1)
            hi_up = pltpu.roll(hi, 16 * bit, 1)
            lo, hi, lo_up, hi_up = (v.reshape(8 // (2 * bit), bit, 8, 128) for v in (lo, hi, lo_up, hi_up))
            tiles = jnp.stack([jnp.where(mask, lo, hi_up), jnp.where(mask, lo_up, hi)], axis=1).reshape(8, 8, 128)
        return tiles

    def row_copy(rnd, x, i):
        d_row, d_sub = ROW_PEERS[i]
        return pltpu.make_async_remote_copy(
            src_ref=rowp.at[rnd, x], dst_ref=rowp.at[rnd, x],
            send_sem=row_send.at[rnd, x, i], recv_sem=row_recv.at[rnd, x],
            device_id=peer(0, d_row, d_sub), device_id_type=MESH)

    def col_copy(rnd, a):
        return pltpu.make_async_remote_copy(
            src_ref=colp.at[rnd, a], dst_ref=colp.at[rnd, a],
            send_sem=col_send.at[rnd, a], recv_sem=col_recv.at[rnd, a],
            device_id=peer(1, 0, 0), device_id_type=MESH)

    def dia_copy(rnd, i):
        turn = rnd % 2
        offs = ((1, turn, 1), (1, 1 - turn, 1), (0, 1, 1), (0, 0, 1))[i]
        return pltpu.make_async_remote_copy(
            src_ref=dst.at[rnd], dst_ref=dst.at[rnd],
            send_sem=dia_send.at[rnd, i], recv_sem=dia_recv.at[rnd],
            device_id=peer(*offs), device_id_type=MESH)

    def dia_pass(rnd):
        return pltpu.make_async_remote_copy(
            src_ref=dst.at[rnd], dst_ref=dst.at[rnd],
            send_sem=dia_fwd.at[rnd], recv_sem=dia_recv.at[rnd],
            device_id=peer(0, 0, 1), device_id_type=MESH)

    def passes(rnd):
        return (sub != rnd % 2) & ((col != rnd % 2) | (row != (rnd % 4) // 2))

    def send_row(rnd, x):
        for i in range(3):
            row_copy(rnd, x, i).start()

    def send_dia(rnd):
        for i in range(4):
            dia_copy(rnd, i).start()

    def close(rnd, a, x):
        dst[rnd] = mat[a, x]

        def group(g, carry):
            rg, cg = lax.div(g, 8), lax.div(g, 2)
            q, half = lax.rem(g, 8), lax.rem(g, 2) * 8
            ucol = lanes(jnp.broadcast_to(dst[rnd, rg, cg][None], (8, 8, 128)), nth_pivot + (16 * q + half))
            rows = lanes(dst[rnd, rg], in_grp[None] + 16 * q)
            left = lanes(jnp.broadcast_to(dst[rnd, :, cg][None], (8, 2, 8, 128)),
                         (nth_pivot + (grp_base + half)[None])[:, None])
            for p in range(8):
                rows = jnp.minimum(rows, ucol[0][None] + rows[:, p:p + 1, :])
                if p < 7:
                    ucol = jnp.minimum(ucol[1:], ucol[0][None] + ucol[1:, p:p + 1, :])
            block = dst[rnd]
            for p in range(8):
                block = jnp.minimum(block, left[p][:, None] + rows[:, p:p + 1, :][None])
            dst[rnd] = block
            return carry

        def groups(i, carry):
            return lax.fori_loop(0, 4, lambda u, c: group(i * 4 + u, c), carry, unroll=True)
        lax.fori_loop(0, 4, groups, 0)

    def make_brep(src, out):
        def one(i, carry):
            out[i] = lanes(src[lax.div(i, 8)], in_grp + 16 * lax.rem(i, 8))
            return carry
        lax.fori_loop(0, 16, one, 0, unroll=True)

    def product(acc, left, right, step):
        def chunk(i, acc):
            def pivot(u, acc):
                b = right[i * (step // 8) + lax.div(u, 8), :, pl.ds(lax.rem(u, 8), 1), :]
                return jnp.minimum(acc, left(i * (step // 16) + lax.div(u, 16), i * step + u, lax.rem(u, 16))[:, None] + b[None])
            return lax.fori_loop(0, step, pivot, acc, unroll=True)
        return lax.fori_loop(0, BLK // step, chunk, acc, unroll=step == BLK)

    def close_and_send(rnd, a, x):
        close(rnd, a, x)
        send_dia(rnd)

    slot_r = jnp.where(my_row == 0, 0, ROUNDS)
    slot_c = jnp.where(col == 0, 0, ROUNDS)
    for a in range(2):
        for x in range(4):
            for r in range(2):
                tiles = swap_chunks(in_ref[a, 64 * r:64 * r + 64, BLK * x:BLK * x + BLK].reshape(8, 8, 128))
                mat[a, x, r] = tiles
                if a == 0:
                    rowp[slot_r, x, r] = tiles
                if x == 0:
                    colp[slot_c, a, r] = tiles

    pl.semaphore_wait(barrier, 7)

    @pl.when((my_row == 0) & (col == 0))
    def _():
        close_and_send(0, 0, 0)

    @pl.when(my_row == 0)
    def _():
        for x in range(4):
            if x == 0:
                @pl.when(col != 0)
                def _():
                    send_row(0, 0)
            else:
                send_row(0, x)

    @pl.when(col == 0)
    def _():
        @pl.when(my_row != 0)
        def _():
            col_copy(0, 0).start()
        col_copy(0, 1).start()

    def one_round(k, carry):
        n = k + 1
        more = n < ROUNDS
        own_row = (my_row == n % 4) & more
        own_col = (col == n % 2) & more
        a1 = jnp.minimum(n // 4, 1)
        x1 = ((n + jnp.where(col == n % 2, 0, 1)) // 2) % 4
        xk = k // 2
        is_row, is_col = my_row == k % 4, col == k % 2

        @pl.when(~is_row | ~is_col)
        def _():
            dia_copy(k, 0).wait_recv()

        @pl.when(passes(k))
        def _():
            dia_pass(k).start()

        def wait_row(x):
            @pl.when(~is_row)
            def _():
                row_copy(k, x, 0).wait_recv()

        make_brep(dst.at[k], brepd)
        wait_row(x1)
        make_brep(rowp.at[k, x1], brep.at[x1])

        def head(h, carry):
            a = jnp.where(h == 0, a1, 1 - a1)

            on_diag = is_row & (a == k // 4)
            send_it = own_row & (h == 0)

            @pl.when(~is_col & ~on_diag)
            def _():
                col_copy(k, a).wait_recv()

            @pl.when(on_diag)
            def _():
                cpr[...] = dst[k]

            @pl.when(~on_diag)
            def _():
                pan = colp.at[k, a]
                cpr[...] = product(pan[...], lambda c, p, l: lanes(pan[:, c], grp_base + l), brepd, HEAD_STEP)

            @pl.when(is_col)
            def _():
                mat[a, xk] = cpr[...]

            @pl.when(is_col & send_it)
            def _():
                rowp[n, xk] = cpr[...]
                send_row(n, xk)

            tab = cb.at[a]

            def fly(c, p, l):
                avs = lanes(cpr[:, c], grp_base + l)
                tab[p] = avs
                return avs
            acc = product(mat[a, x1], fly, brep.at[x1], HEAD_STEP)
            mat[a, x1] = acc
            rowp[jnp.where(send_it, n, ROUNDS), x1] = acc
            colp[jnp.where(own_col, n, ROUNDS), a] = acc

            @pl.when(send_it & ~own_col)
            def _():
                send_row(n, x1)

            @pl.when(own_col & ~send_it)
            def _():
                col_copy(n, a).start()

            @pl.when(send_it & own_col)
            def _():
                close_and_send(n, a, x1)
            return carry
        lax.fori_loop(0, 2, head, 0)

        def tail(t, carry):
            h = t // 3
            a = jnp.where(h == 0, a1, 1 - a1)
            x = (x1 + 1 + t % 3) % 4

            @pl.when((col != k % 2) | (t % 3 != 2))
            def _():
                @pl.when(h == 0)
                def _():
                    wait_row(x)
                    make_brep(rowp.at[k, x], brep.at[x])

                tab = cb.at[a]
                acc = product(mat[a, x], lambda c, p, l: tab[p], brep.at[x], TAIL_STEP)
                mat[a, x] = acc
                send_it = own_row & (h == 0)
                rowp[jnp.where(send_it, n, ROUNDS), x] = acc

                @pl.when(send_it)
                def _():
                    send_row(n, x)
            return carry
        lax.fori_loop(0, 6, tail, 0)
        return carry
    lax.fori_loop(0, ROUNDS, one_round, 0)

    for a in range(2):
        for x in range(4):
            for r in range(2):
                tiles = swap_chunks(mat[a, x, r])
                out_ref[a, 64 * r:64 * r + 64, BLK * x:BLK * x + BLK] = tiles.reshape(64, 128)

    def drain(k, carry):
        is_row, is_col = my_row == k % 4, col == k % 2
        for x in range(4):
            @pl.when(is_row & (~is_col | (x != k // 2)))
            def _():
                for i in range(3):
                    row_copy(k, x, i).wait_send()
        for a in range(2):
            @pl.when(is_col & (~is_row | (a != k // 4)))
            def _():
                col_copy(k, a).wait_send()

        @pl.when(is_row & is_col)
        def _():
            for i in range(4):
                dia_copy(k, i).wait_send()

        @pl.when(passes(k))
        def _():
            dia_pass(k).wait_send()
        return carry
    lax.fori_loop(0, ROUNDS, drain, 0)


def solution(mesh):
    spec = P(('parts', 'row', 'sub'), None, 'col')
    tile = (8, 128)
    dma = pltpu.SemaphoreType.DMA

    def local_run(local_dist):
        return pl.pallas_call(
            kernel,
            out_shape=jax.ShapeDtypeStruct(local_dist.shape, local_dist.dtype),
            in_specs=[pl.BlockSpec(memory_space=pltpu.VMEM)],
            out_specs=pl.BlockSpec(memory_space=pltpu.VMEM),
            scratch_shapes=[
                pltpu.VMEM((2, 4, 2, 8) + tile, jnp.float32),
                pltpu.VMEM((ROUNDS + 1, 4, 2, 8) + tile, jnp.float32),
                pltpu.VMEM((ROUNDS + 1, 2, 2, 8) + tile, jnp.float32),
                pltpu.VMEM((ROUNDS, 2, 8) + tile, jnp.float32),
                pltpu.VMEM((2, BLK, 2) + tile, jnp.float32),
                pltpu.VMEM((4, 16, 8) + tile, jnp.float32),
                pltpu.VMEM((16, 8) + tile, jnp.float32),
                pltpu.VMEM((2, 8) + tile, jnp.float32),
                dma((ROUNDS, 4, 3)), dma((ROUNDS, 4)),
                dma((ROUNDS, 2)), dma((ROUNDS, 2)),
                dma((ROUNDS, 4)), dma((ROUNDS,)), dma((ROUNDS,)),
            ],
            compiler_params=pltpu.CompilerParams(collective_id=0, has_side_effects=True),
            name='apsp',
        )(local_dist)

    return jax.shard_map(local_run, mesh=mesh, in_specs=(spec,), out_specs=spec, check_vma=False)
```

```python
import functools

import jax
import jax.numpy as jnp
from jax import lax
from jax.experimental import pallas as pl
from jax.experimental.pallas import tpu as pltpu
from jax.sharding import PartitionSpec as P

MESH = pl.DeviceIdType.MESH
BLK = 128
ROUNDS = 8
ROW_PEERS = ((0, 1), (1, 1), (1, 0))
ALL_PEERS = ((1, 0, 1), (1, 1, 1), (0, 0, 1), (0, 1, 1), (1, 0, 0), (0, 1, 0), (1, 1, 0))


def lanes(tiles, idx):
    flat = tiles.reshape(-1, 128)
    idx = jnp.broadcast_to(idx, tiles.shape).reshape(-1, 128)
    return jnp.take_along_axis(flat, idx, axis=1, mode='promise_in_bounds').reshape(tiles.shape)


def kernel(in_ref, out_ref, mat, rowp, colp, dst, cb, brep, brepd, cpr,

           row_send, row_recv, col_send, col_recv, dia_send, dia_fwd, dia_recv):
    row, sub, col = lax.axis_index('row'), lax.axis_index('sub'), lax.axis_index('col')
    my_row = row * 2 + sub
    lane = lax.broadcasted_iota(jnp.int32, (8, 128), 1)
    in_grp = lane & 15
    grp_base = lane - in_grp
    nth_pivot = lax.broadcasted_iota(jnp.int32, (8, 8, 128), 0)

    def peer(d_col, d_row, d_sub):
        return {'col': (col + d_col) % 2, 'row': (row + d_row) % 2, 'sub': (sub + d_sub) % 2}

    barrier = pltpu.get_barrier_semaphore()
    for offs in ALL_PEERS:
        pl.semaphore_signal(barrier, inc=1, device_id=peer(*offs), device_id_type=MESH)

    def swap_chunks(tiles):
        for bit in (1, 2, 4):
            mask = (lane & (16 * bit)) == 0
            pairs = tiles.reshape(8 // (2 * bit), 2, bit, 8, 128)
            lo, hi = pairs[:, 0].reshape(-1, 128), pairs[:, 1].reshape(-1, 128)
            lo_up = pltpu.roll(lo, 128 - 16 * bit, 1)
            hi_up = pltpu.roll(hi, 16 * bit, 1)
            lo, hi, lo_up, hi_up = (v.reshape(8 // (2 * bit), bit, 8, 128) for v in (lo, hi, lo_up, hi_up))
            tiles = jnp.stack([jnp.where(mask, lo, hi_up), jnp.where(mask, lo_up, hi)], axis=1).reshape(8, 8, 128)
        return tiles

    def row_copy(rnd, x, i):
        d_row, d_sub = ROW_PEERS[i]
        return pltpu.make_async_remote_copy(
            src_ref=rowp.at[rnd, x], dst_ref=rowp.at[rnd, x],
            send_sem=row_send.at[rnd, x, i], recv_sem=row_recv.at[rnd, x],
            device_id=peer(0, d_row, d_sub), device_id_type=MESH)

    def col_copy(rnd, a):
        return pltpu.make_async_remote_copy(
            src_ref=colp.at[rnd, a], dst_ref=colp.at[rnd, a],
            send_sem=col_send.at[rnd, a], recv_sem=col_recv.at[rnd, a],
            device_id=peer(1, 0, 0), device_id_type=MESH)

    def dia_copy(rnd, i):
        turn = rnd % 2
        offs = ((1, turn, 1), (1, 1 - turn, 1), (0, 1, 1), (0, 0, 1))[i]
        return pltpu.make_async_remote_copy(
            src_ref=dst.at[rnd], dst_ref=dst.at[rnd],
            send_sem=dia_send.at[rnd, i], recv_sem=dia_recv.at[rnd],
            device_id=peer(*offs), device_id_type=MESH)

    def dia_pass(rnd):
        return pltpu.make_async_remote_copy(
            src_ref=dst.at[rnd], dst_ref=dst.at[rnd],
            send_sem=dia_fwd.at[rnd], recv_sem=dia_recv.at[rnd],
            device_id=peer(0, 0, 1), device_id_type=MESH)

    def passes(rnd):
        return (sub != rnd % 2) & ((col != rnd % 2) | (row != (rnd % 4) // 2))

    def send_row(rnd, x):
        for i in range(3):
            row_copy(rnd, x, i).start()

    def send_dia(rnd):
        for i in range(4):
            dia_copy(rnd, i).start()

    def close(rnd, a, x):
        dst[rnd] = mat[a, x]

        def group(g, carry):
            rg, cg = lax.div(g, 8), lax.div(g, 2)
            q, half = lax.rem(g, 8), lax.rem(g, 2) * 8
            ucol = lanes(jnp.broadcast_to(dst[rnd, rg, cg][None], (8, 8, 128)), nth_pivot + (16 * q + half))
            rows = lanes(dst[rnd, rg], in_grp[None] + 16 * q)
            left = lanes(jnp.broadcast_to(dst[rnd, :, cg][None], (8, 2, 8, 128)),
                         (nth_pivot + (grp_base + half)[None])[:, None])
            for p in range(8):
                rows = jnp.minimum(rows, ucol[0][None] + rows[:, p:p + 1, :])
                if p < 7:
                    ucol = jnp.minimum(ucol[1:], ucol[0][None] + ucol[1:, p:p + 1, :])
            block = dst[rnd]
            for p in range(8):
                block = jnp.minimum(block, left[p][:, None] + rows[:, p:p + 1, :][None])
            dst[rnd] = block
            return carry

        def groups(i, carry):
            return lax.fori_loop(0, 4, lambda u, c: group(i * 4 + u, c), carry, unroll=True)
        lax.fori_loop(0, 4, groups, 0)

    def spread(src, out):
        def build(g):
            out[g] = lanes(src[lax.div(g, 8)], (in_grp + 16 * lax.rem(g, 8))[None])
        return build

    def product(acc, left, right, step, build=None):
        def chunk(i, acc):
            def group(u, acc):
                g = i * step + u
                if build is not None:
                    build(g)
                for s in range(8):
                    acc = jnp.minimum(acc, left(g, s)[:, None] + right[g, :, s:s + 1, :][None])
                return acc
            return lax.fori_loop(0, step, group, acc, unroll=True)
        if step == 16:
            return chunk(0, acc)
        return lax.fori_loop(0, 16 // step, chunk, acc)

    def from_panel(ref):
        def left(g, s):
            return lanes(ref(lax.div(g, 2)), grp_base + (lax.rem(g, 2) * 8 + s))
        return left

    def saving(left, save):
        def both(g, s):
            cols = left(g, s)
            save(8 * g + s, cols)
            return cols
        return both

    def close_and_send(rnd, a, x):
        close(rnd, a, x)
        send_dia(rnd)

    slot_r = jnp.where(my_row == 0, 0, ROUNDS)
    slot_c = jnp.where(col == 0, 0, ROUNDS)
    for a in range(2):
        for x in range(4):
            for r in range(2):
                tiles = swap_chunks(in_ref[a, 64 * r:64 * r + 64, BLK * x:BLK * x + BLK].reshape(8, 8, 128))
                mat[a, x, r] = tiles
                if a == 0:
                    rowp[slot_r, x, r] = tiles
                if x == 0:
                    colp[slot_c, a, r] = tiles

    pl.semaphore_wait(barrier, 7)

    @pl.when((my_row == 0) & (col == 0))
    def _():
        close_and_send(0, 0, 0)

    @pl.when(my_row == 0)
    def _():
        for x in range(4):
            if x == 0:
                @pl.when(col != 0)
                def _():
                    send_row(0, 0)
            else:
                send_row(0, x)

    @pl.when(col == 0)
    def _():
        @pl.when(my_row != 0)
        def _():
            col_copy(0, 0).start()
        col_copy(0, 1).start()

    def one_round(k, carry):
        n = k + 1
        more = n < ROUNDS
        own_row = (my_row == n % 4) & more
        own_col = (col == n % 2) & more
        a1 = jnp.minimum(n // 4, 1)
        x1 = ((n + jnp.where(col == n % 2, 0, 1)) // 2) % 4
        xk = k // 2
        is_row, is_col = my_row == k % 4, col == k % 2

        @pl.when(~is_row | ~is_col)
        def _():
            dia_copy(k, 0).wait_recv()

        @pl.when(passes(k))
        def _():
            dia_pass(k).start()

        def wait_row(x):
            @pl.when(~is_row)
            def _():
                row_copy(k, x, 0).wait_recv()

        spread_dia = spread(dst.at[k], brepd)

        def spread_row(x):
            return spread(rowp.at[k, x], brep.at[x])

        def wait_col(a):
            @pl.when((col != k % 2) & ((my_row != k % 4) | (a != k // 4)))
            def _():
                col_copy(k, a).wait_recv()

        def one_panel(a, build):
            pan = colp.at[k, a]
            cpr[a] = product(pan[...], from_panel(lambda c: pan[:, c]), brepd, 8, build)

        def head(h, carry):
            a = jnp.where(h == 0, a1, 1 - a1)
            wait_col(a)

            @pl.when(h == 0)
            def _():
                one_panel(a, spread_dia)

            @pl.when(h == 1)
            def _():
                one_panel(a, None)

            @pl.when(is_col)
            def _():
                mat[a, xk] = cpr[a]

            @pl.when(is_col & (h == 0))
            def _():
                rowp[n, xk] = cpr[a]
                send_row(n, xk)

            tab = cb.at[:, a]

            def keep(p, cols):
                tab[p] = cols

            def fly(build):
                mat[a, x1] = product(mat[a, x1], saving(from_panel(lambda c: cpr[a, :, c]), keep), brep.at[x1], 8, build)

            @pl.when(h == 0)
            def _():
                wait_row(x1)
                fly(spread_row(x1))

            @pl.when(h == 1)
            def _():
                fly(None)

            @pl.when((h == 0) & (col != n % 2))
            def _():
                rowp[n, x1] = mat[a, x1]
                send_row(n, x1)

            @pl.when((h == 1) & (col == n % 2))
            def _():
                colp[n, a] = mat[a, x1]
                col_copy(n, a).start()

            @pl.when((h == 0) & (col == n % 2))
            def _():
                close_and_send(n, a, x1)
            return carry

        def tail(t, carry):
            h = t // 3
            a = jnp.where(h == 0, a1, 1 - a1)
            x = (x1 + 1 + t % 3) % 4

            @pl.when((col != k % 2) | (t % 3 != 2))
            def _():
                tab = cb.at[:, a]

                @pl.when(h == 0)
                def _():
                    wait_row(x)
                    acc = product(mat[a, x], lambda g, s: tab[8 * g + s], brep.at[x], 8, spread_row(x))
                    mat[a, x] = acc
                    rowp[n, x] = acc
                    send_row(n, x)

                @pl.when(h == 1)
                def _():
                    mat[a, x] = product(mat[a, x], lambda g, s: tab[8 * g + s], brep.at[x], 8)
            return carry

        @pl.when(own_row)
        def _():
            lax.fori_loop(0, 2, head, 0)
            lax.fori_loop(0, 6, tail, 0)

        def four(tiles):
            return tiles.reshape((4,) + tiles.shape[2:])

        def two(tiles):
            return tiles.reshape((2, 2) + tiles.shape[1:])

        @pl.when(~own_row)
        def _():
            @pl.when(is_row)
            def _():
                wait_col(1 - k // 4)
                one_panel(1 - k // 4, spread_dia)
                cpr[k // 4] = dst[k]

            @pl.when(~is_row)
            def _():
                wait_col(0)
                wait_col(1)
                pan = colp.at[k]
                cpr[...] = two(product(four(pan[...]), from_panel(lambda c: four(pan[:, :, c])), brepd, 16, spread_dia))

            @pl.when(is_col)
            def _():
                mat[:, xk] = cpr[...]
            wait_row(x1)

            def keep(p, cols):
                cb[p] = two(cols)
            acc = two(product(four(mat[:, x1]), saving(from_panel(lambda c: four(cpr[:, :, c])), keep), brep.at[x1],
                              16, spread_row(x1)))
            mat[:, x1] = acc

            @pl.when(own_col)
            def _():
                colp[n] = acc
                for a in range(2):
                    col_copy(n, a).start()

            def joint(t, carry):
                x = (x1 + 1 + t) % 4

                @pl.when((col != k % 2) | (t != 2))
                def _():
                    wait_row(x)
                    mat[:, x] = two(product(four(mat[:, x]), lambda g, s: four(cb[8 * g + s]), brep.at[x],
                                            16, spread_row(x)))
                return carry
            lax.fori_loop(0, 3, joint, 0)
        return carry
    lax.fori_loop(0, ROUNDS, one_round, 0)

    for a in range(2):
        for x in range(4):
            for r in range(2):
                tiles = swap_chunks(mat[a, x, r])
                out_ref[a, 64 * r:64 * r + 64, BLK * x:BLK * x + BLK] = tiles.reshape(64, 128)

    def drain(k, carry):
        is_row, is_col = my_row == k % 4, col == k % 2
        for x in range(4):
            @pl.when(is_row & (~is_col | (x != k // 2)))
            def _():
                for i in range(3):
                    row_copy(k, x, i).wait_send()
        for a in range(2):
            @pl.when(is_col & (~is_row | (a != k // 4)))
            def _():
                col_copy(k, a).wait_send()

        @pl.when(is_row & is_col)
        def _():
            for i in range(4):
                dia_copy(k, i).wait_send()

        @pl.when(passes(k))
        def _():
            dia_pass(k).wait_send()
        return carry
    lax.fori_loop(0, ROUNDS, drain, 0)


def solution(mesh):
    spec = P(('parts', 'row', 'sub'), None, 'col')
    tile = (8, 128)
    dma = pltpu.SemaphoreType.DMA

    def local_run(local_dist):
        return pl.pallas_call(
            kernel,
            out_shape=jax.ShapeDtypeStruct(local_dist.shape, local_dist.dtype),
            in_specs=[pl.BlockSpec(memory_space=pltpu.VMEM)],
            out_specs=pl.BlockSpec(memory_space=pltpu.VMEM),
            scratch_shapes=[
                pltpu.VMEM((2, 4, 2, 8) + tile, jnp.float32),
                pltpu.VMEM((ROUNDS + 1, 4, 2, 8) + tile, jnp.float32),
                pltpu.VMEM((ROUNDS + 1, 2, 2, 8) + tile, jnp.float32),
                pltpu.VMEM((ROUNDS, 2, 8) + tile, jnp.float32),
                pltpu.VMEM((BLK, 2, 2) + tile, jnp.float32),
                pltpu.VMEM((4, 16, 8) + tile, jnp.float32),
                pltpu.VMEM((16, 8) + tile, jnp.float32),
                pltpu.VMEM((2, 2, 8) + tile, jnp.float32),
                dma((ROUNDS, 4, 3)), dma((ROUNDS, 4)),
                dma((ROUNDS, 2)), dma((ROUNDS, 2)),
                dma((ROUNDS, 4)), dma((ROUNDS,)), dma((ROUNDS,)),
            ],
            compiler_params=pltpu.CompilerParams(collective_id=0, has_side_effects=True),
            name='apsp',
        )(local_dist)

    return jax.shard_map(local_run, mesh=mesh, in_specs=(spec,), out_specs=spec, check_vma=False)
```

```python
import functools

import jax
import jax.numpy as jnp
from jax import lax
from jax.experimental import pallas as pl
from jax.experimental.pallas import tpu as pltpu
from jax.sharding import PartitionSpec as P

MESH = pl.DeviceIdType.MESH
BLK = 128
ROUNDS = 8
HEAD_STEP, TAIL_STEP = 128, 64
ROW_PEERS = ((0, 1), (1, 1), (1, 0))
ALL_PEERS = ((1, 0, 1), (1, 1, 1), (0, 0, 1), (0, 1, 1), (1, 0, 0), (0, 1, 0), (1, 1, 0))


def lanes(tiles, idx):
    flat = tiles.reshape(-1, 128)
    idx = jnp.broadcast_to(idx, tiles.shape).reshape(-1, 128)
    return jnp.take_along_axis(flat, idx, axis=1, mode='promise_in_bounds').reshape(tiles.shape)


def kernel(in_ref, out_ref, mat, rowp, colp, dst, cb, brep, brepd, cpr,

           row_send, row_recv, col_send, col_recv, dia_send, dia_fwd, dia_recv):
    row, sub, col = lax.axis_index('row'), lax.axis_index('sub'), lax.axis_index('col')
    my_row = row * 2 + sub
    lane = lax.broadcasted_iota(jnp.int32, (8, 128), 1)
    in_grp = lane & 15
    grp_base = lane - in_grp
    nth_pivot = lax.broadcasted_iota(jnp.int32, (8, 8, 128), 0)

    def peer(d_col, d_row, d_sub):
        return {'col': (col + d_col) % 2, 'row': (row + d_row) % 2, 'sub': (sub + d_sub) % 2}

    barrier = pltpu.get_barrier_semaphore()
    for offs in ALL_PEERS:
        pl.semaphore_signal(barrier, inc=1, device_id=peer(*offs), device_id_type=MESH)

    def swap_chunks(tiles):
        for bit in (1, 2, 4):
            mask = (lane & (16 * bit)) == 0
            pairs = tiles.reshape(8 // (2 * bit), 2, bit, 8, 128)
            lo, hi = pairs[:, 0].reshape(-1, 128), pairs[:, 1].reshape(-1, 128)
            lo_up = pltpu.roll(lo, 128 - 16 * bit, 1)
            hi_up = pltpu.roll(hi, 16 * bit, 1)
            lo, hi, lo_up, hi_up = (v.reshape(8 // (2 * bit), bit, 8, 128) for v in (lo, hi, lo_up, hi_up))
            tiles = jnp.stack([jnp.where(mask, lo, hi_up), jnp.where(mask, lo_up, hi)], axis=1).reshape(8, 8, 128)
        return tiles

    def row_copy(rnd, x, i):
        d_row, d_sub = ROW_PEERS[i]
        return pltpu.make_async_remote_copy(
            src_ref=rowp.at[rnd, x], dst_ref=rowp.at[rnd, x],
            send_sem=row_send.at[rnd, x, i], recv_sem=row_recv.at[rnd, x],
            device_id=peer(0, d_row, d_sub), device_id_type=MESH)

    def col_copy(rnd, a):
        return pltpu.make_async_remote_copy(
            src_ref=colp.at[rnd, a], dst_ref=colp.at[rnd, a],
            send_sem=col_send.at[rnd, a], recv_sem=col_recv.at[rnd, a],
            device_id=peer(1, 0, 0), device_id_type=MESH)

    def dia_copy(rnd, i):
        turn = rnd % 2
        offs = ((1, turn, 1), (1, 1 - turn, 1), (0, 1, 1), (0, 0, 1))[i]
        return pltpu.make_async_remote_copy(
            src_ref=dst.at[rnd], dst_ref=dst.at[rnd],
            send_sem=dia_send.at[rnd, i], recv_sem=dia_recv.at[rnd],
            device_id=peer(*offs), device_id_type=MESH)

    def dia_pass(rnd):
        return pltpu.make_async_remote_copy(
            src_ref=dst.at[rnd], dst_ref=dst.at[rnd],
            send_sem=dia_fwd.at[rnd], recv_sem=dia_recv.at[rnd],
            device_id=peer(0, 0, 1), device_id_type=MESH)

    def passes(rnd):
        return (sub != rnd % 2) & ((col != rnd % 2) | (row != (rnd % 4) // 2))

    def send_row(rnd, x):
        for i in range(3):
            row_copy(rnd, x, i).start()

    def send_dia(rnd):
        for i in range(4):
            dia_copy(rnd, i).start()

    def close(rnd, a, x):
        dst[rnd] = mat[a, x]

        def group(g, carry):
            rg, cg = lax.div(g, 8), lax.div(g, 2)
            q, half = lax.rem(g, 8), lax.rem(g, 2) * 8
            ucol = lanes(jnp.broadcast_to(dst[rnd, rg, cg][None], (8, 8, 128)), nth_pivot + (16 * q + half))
            rows = lanes(dst[rnd, rg], in_grp[None] + 16 * q)
            left = lanes(jnp.broadcast_to(dst[rnd, :, cg][None], (8, 2, 8, 128)),
                         (nth_pivot + (grp_base + half)[None])[:, None])
            for p in range(8):
                rows = jnp.minimum(rows, ucol[0][None] + rows[:, p:p + 1, :])
                if p < 7:
                    ucol = jnp.minimum(ucol[1:], ucol[0][None] + ucol[1:, p:p + 1, :])
            block = dst[rnd]
            for p in range(8):
                block = jnp.minimum(block, left[p][:, None] + rows[:, p:p + 1, :][None])
            dst[rnd] = block
            return carry

        def groups(i, carry):
            return lax.fori_loop(0, 4, lambda u, c: group(i * 4 + u, c), carry, unroll=True)
        lax.fori_loop(0, 4, groups, 0)

    def make_brep(src, out):
        def one(i, carry):
            out[i] = lanes(src[lax.div(i, 8)], in_grp + 16 * lax.rem(i, 8))
            return carry
        lax.fori_loop(0, 16, one, 0, unroll=True)

    def product(acc, left, right, step):
        def chunk(i, acc):
            def pivot(u, acc):
                b = right[i * (step // 8) + lax.div(u, 8), :, pl.ds(lax.rem(u, 8), 1), :]
                return jnp.minimum(acc, left(i * (step // 16) + lax.div(u, 16), i * step + u, lax.rem(u, 16))[:, None] + b[None])
            return lax.fori_loop(0, step, pivot, acc, unroll=True)
        return lax.fori_loop(0, BLK // step, chunk, acc, unroll=step == BLK)

    def close_and_send(rnd, a, x):
        close(rnd, a, x)
        send_dia(rnd)

    slot_r = jnp.where(my_row == 0, 0, ROUNDS)
    slot_c = jnp.where(col == 0, 0, ROUNDS)
    def unpack(a, x):
        for r in range(2):
            tiles = swap_chunks(in_ref[a, 64 * r:64 * r + 64, BLK * x:BLK * x + BLK].reshape(8, 8, 128))
            mat[a, x, r] = tiles
            if a == 0:
                rowp[slot_r, x, r] = tiles
            if x == 0:
                colp[slot_c, a, r] = tiles

    unpack(0, 0)

    @pl.when((my_row == 0) & (col == 0))
    def _():
        close(0, 0, 0)
        pl.semaphore_wait(barrier, 7)
        send_dia(0)
    for a in range(2):
        for x in range(4):
            if a + x:
                unpack(a, x)

    @pl.when((my_row != 0) | (col != 0))
    def _():
        pl.semaphore_wait(barrier, 7)

    @pl.when(my_row == 0)
    def _():
        for x in (1, 2, 3):
            send_row(0, x)

        @pl.when(col != 0)
        def _():
            send_row(0, 0)

    @pl.when(col == 0)
    def _():
        @pl.when(my_row != 0)
        def _():
            col_copy(0, 0).start()
        col_copy(0, 1).start()

    def one_round(k, carry):
        n = k + 1
        more = n < ROUNDS
        own_row = (my_row == n % 4) & more
        own_col = (col == n % 2) & more
        a1 = jnp.minimum(n // 4, 1)
        x1 = ((n + jnp.where(col == n % 2, 0, 1)) // 2) % 4
        xk = k // 2
        is_row, is_col = my_row == k % 4, col == k % 2

        def first_rows():
            @pl.when(~is_row)
            def _():
                row_copy(k, x1, 0).wait_recv()
            make_brep(rowp.at[k, x1], brep.at[x1])

        @pl.when(~is_col)
        def _():
            first_rows()

        @pl.when(~is_row | ~is_col)
        def _():
            dia_copy(k, 0).wait_recv()

        @pl.when(passes(k))
        def _():
            dia_pass(k).start()

        def wait_row(x):
            @pl.when(~is_row)
            def _():
                row_copy(k, x, 0).wait_recv()

        make_brep(dst.at[k], brepd)

        def head(h, carry):
            a = jnp.where(h == 0, a1, 1 - a1)

            on_diag = is_row & (a == k // 4)
            send_it = own_row & (h == 0)

            @pl.when(~is_col & ~on_diag)
            def _():
                col_copy(k, a).wait_recv()

            @pl.when(on_diag)
            def _():
                cpr[...] = dst[k]

            @pl.when(~on_diag)
            def _():
                pan = colp.at[k, a]
                cpr[...] = product(pan[...], lambda c, p, l: lanes(pan[:, c], grp_base + l), brepd, HEAD_STEP)

            @pl.when(is_col)
            def _():
                mat[a, xk] = cpr[...]

                @pl.when(h == 0)
                def _():
                    first_rows()

            @pl.when(is_col & send_it)
            def _():
                rowp[n, xk] = cpr[...]
                send_row(n, xk)

            tab = cb.at[a]

            def fly(c, p, l):
                avs = lanes(cpr[:, c], grp_base + l)
                tab[p] = avs
                return avs
            acc = product(mat[a, x1], fly, brep.at[x1], HEAD_STEP)
            mat[a, x1] = acc
            rowp[jnp.where(send_it, n, ROUNDS), x1] = acc
            colp[jnp.where(own_col, n, ROUNDS), a] = acc

            @pl.when(send_it & ~own_col)
            def _():
                send_row(n, x1)

            @pl.when(own_col & ~send_it)
            def _():
                col_copy(n, a).start()

            @pl.when(send_it & own_col)
            def _():
                close_and_send(n, a, x1)
            return carry
        lax.fori_loop(0, 2, head, 0)

        def tail(t, carry):
            h = t // 3
            a = jnp.where(h == 0, a1, 1 - a1)
            x = (x1 + 1 + t % 3) % 4

            @pl.when((col != k % 2) | (t % 3 != 2))
            def _():
                @pl.when(h == 0)
                def _():
                    wait_row(x)
                    make_brep(rowp.at[k, x], brep.at[x])

                tab = cb.at[a]
                acc = product(mat[a, x], lambda c, p, l: tab[p], brep.at[x], TAIL_STEP)
                mat[a, x] = acc
                send_it = own_row & (h == 0)
                rowp[jnp.where(send_it, n, ROUNDS), x] = acc

                @pl.when(send_it)
                def _():
                    send_row(n, x)
            return carry
        lax.fori_loop(0, 6, tail, 0)
        return carry
    lax.fori_loop(0, ROUNDS, one_round, 0)

    for a in range(2):
        for x in range(4):
            for r in range(2):
                tiles = swap_chunks(mat[a, x, r])
                out_ref[a, 64 * r:64 * r + 64, BLK * x:BLK * x + BLK] = tiles.reshape(64, 128)

    def drain(k, carry):
        is_row, is_col = my_row == k % 4, col == k % 2
        for x in range(4):
            @pl.when(is_row & (~is_col | (x != k // 2)))
            def _():
                for i in range(3):
                    row_copy(k, x, i).wait_send()
        for a in range(2):
            @pl.when(is_col & (~is_row | (a != k // 4)))
            def _():
                col_copy(k, a).wait_send()

        @pl.when(is_row & is_col)
        def _():
            for i in range(4):
                dia_copy(k, i).wait_send()

        @pl.when(passes(k))
        def _():
            dia_pass(k).wait_send()
        return carry
    lax.fori_loop(0, ROUNDS, drain, 0)


def solution(mesh):
    spec = P(('parts', 'row', 'sub'), None, 'col')
    tile = (8, 128)
    dma = pltpu.SemaphoreType.DMA

    def local_run(local_dist):
        return pl.pallas_call(
            kernel,
            out_shape=jax.ShapeDtypeStruct(local_dist.shape, local_dist.dtype),
            in_specs=[pl.BlockSpec(memory_space=pltpu.VMEM)],
            out_specs=pl.BlockSpec(memory_space=pltpu.VMEM),
            scratch_shapes=[
                pltpu.VMEM((2, 4, 2, 8) + tile, jnp.float32),
                pltpu.VMEM((ROUNDS + 1, 4, 2, 8) + tile, jnp.float32),
                pltpu.VMEM((ROUNDS + 1, 2, 2, 8) + tile, jnp.float32),
                pltpu.VMEM((ROUNDS, 2, 8) + tile, jnp.float32),
                pltpu.VMEM((2, BLK, 2) + tile, jnp.float32),
                pltpu.VMEM((4, 16, 8) + tile, jnp.float32),
                pltpu.VMEM((16, 8) + tile, jnp.float32),
                pltpu.VMEM((2, 8) + tile, jnp.float32),
                dma((ROUNDS, 4, 3)), dma((ROUNDS, 4)),
                dma((ROUNDS, 2)), dma((ROUNDS, 2)),
                dma((ROUNDS, 4)), dma((ROUNDS,)), dma((ROUNDS,)),
            ],
            compiler_params=pltpu.CompilerParams(collective_id=0, has_side_effects=True),
            name='apsp',
        )(local_dist)

    return jax.shard_map(local_run, mesh=mesh, in_specs=(spec,), out_specs=spec, check_vma=False)
```

```python
import functools

import jax
import jax.numpy as jnp
from jax import lax
from jax.experimental import pallas as pl
from jax.experimental.pallas import tpu as pltpu
from jax.sharding import PartitionSpec as P

MESH = pl.DeviceIdType.MESH
BLK = 128
ROUNDS = 8
HEAD_STEP, TAIL_STEP = 128, 64
ROW_PEERS = ((0, 1), (1, 1), (1, 0))
ALL_PEERS = ((1, 0, 1), (1, 1, 1), (0, 0, 1), (0, 1, 1), (1, 0, 0), (0, 1, 0), (1, 1, 0))


def lanes(tiles, idx):
    flat = tiles.reshape(-1, 128)
    idx = jnp.broadcast_to(idx, tiles.shape).reshape(-1, 128)
    return jnp.take_along_axis(flat, idx, axis=1, mode='promise_in_bounds').reshape(tiles.shape)


def kernel(in_ref, out_ref, mat, rowp, colp, dst, cb, brep, brepd, cpr,

           row_send, row_recv, col_send, col_recv, dia_send, dia_fwd, dia_recv):
    row, sub, col = lax.axis_index('row'), lax.axis_index('sub'), lax.axis_index('col')
    my_row = row * 2 + sub
    lane = lax.broadcasted_iota(jnp.int32, (8, 128), 1)
    in_grp = lane & 15
    grp_base = lane - in_grp
    nth_pivot = lax.broadcasted_iota(jnp.int32, (8, 8, 128), 0)

    def peer(d_col, d_row, d_sub):
        return {'col': (col + d_col) % 2, 'row': (row + d_row) % 2, 'sub': (sub + d_sub) % 2}

    barrier = pltpu.get_barrier_semaphore()
    for offs in ALL_PEERS:
        pl.semaphore_signal(barrier, inc=1, device_id=peer(*offs), device_id_type=MESH)

    def swap_chunks(tiles):
        for bit in (1, 2, 4):
            mask = (lane & (16 * bit)) == 0
            pairs = tiles.reshape(8 // (2 * bit), 2, bit, 8, 128)
            lo, hi = pairs[:, 0].reshape(-1, 128), pairs[:, 1].reshape(-1, 128)
            lo_up = pltpu.roll(lo, 128 - 16 * bit, 1)
            hi_up = pltpu.roll(hi, 16 * bit, 1)
            lo, hi, lo_up, hi_up = (v.reshape(8 // (2 * bit), bit, 8, 128) for v in (lo, hi, lo_up, hi_up))
            tiles = jnp.stack([jnp.where(mask, lo, hi_up), jnp.where(mask, lo_up, hi)], axis=1).reshape(8, 8, 128)
        return tiles

    def row_copy(rnd, x, i):
        d_row, d_sub = ROW_PEERS[i]
        return pltpu.make_async_remote_copy(
            src_ref=rowp.at[rnd, x], dst_ref=rowp.at[rnd, x],
            send_sem=row_send.at[rnd, x, i], recv_sem=row_recv.at[rnd, x],
            device_id=peer(0, d_row, d_sub), device_id_type=MESH)

    def col_copy(rnd, a):
        return pltpu.make_async_remote_copy(
            src_ref=colp.at[rnd, a], dst_ref=colp.at[rnd, a],
            send_sem=col_send.at[rnd, a], recv_sem=col_recv.at[rnd, a],
            device_id=peer(1, 0, 0), device_id_type=MESH)

    def dia_copy(rnd, i, r):
        turn = rnd % 2
        offs = ((1, turn, 1), (1, 1 - turn, 1), (0, 1, 1), (0, 0, 1))[i]
        return pltpu.make_async_remote_copy(
            src_ref=dst.at[rnd, r], dst_ref=dst.at[rnd, r],
            send_sem=dia_send.at[rnd, i, r], recv_sem=dia_recv.at[rnd, r],
            device_id=peer(*offs), device_id_type=MESH)

    def dia_pass(rnd, r):
        return pltpu.make_async_remote_copy(
            src_ref=dst.at[rnd, r], dst_ref=dst.at[rnd, r],
            send_sem=dia_fwd.at[rnd, r], recv_sem=dia_recv.at[rnd, r],
            device_id=peer(0, 0, 1), device_id_type=MESH)

    def passes(rnd):
        return (sub != rnd % 2) & ((col != rnd % 2) | (row != (rnd % 4) // 2))

    def send_row(rnd, x):
        for i in range(3):
            row_copy(rnd, x, i).start()

    def send_dia(rnd):
        for i in range(4):
            for r in range(2):
                dia_copy(rnd, i, r).start()

    def close(rnd, a, x):
        dst[rnd] = mat[a, x]

        def group(g, carry):
            rg, cg = lax.div(g, 8), lax.div(g, 2)
            q, half = lax.rem(g, 8), lax.rem(g, 2) * 8
            ucol = lanes(jnp.broadcast_to(dst[rnd, rg, cg][None], (8, 8, 128)), nth_pivot + (16 * q + half))
            rows = lanes(dst[rnd, rg], in_grp[None] + 16 * q)
            left = lanes(jnp.broadcast_to(dst[rnd, :, cg][None], (8, 2, 8, 128)),
                         (nth_pivot + (grp_base + half)[None])[:, None])
            for p in range(8):
                rows = jnp.minimum(rows, ucol[0][None] + rows[:, p:p + 1, :])
                if p < 7:
                    ucol = jnp.minimum(ucol[1:], ucol[0][None] + ucol[1:, p:p + 1, :])
            block = dst[rnd]
            for p in range(8):
                block = jnp.minimum(block, left[p][:, None] + rows[:, p:p + 1, :][None])
            dst[rnd] = block
            return carry

        def groups(i, carry):
            return lax.fori_loop(0, 4, lambda u, c: group(i * 4 + u, c), carry, unroll=True)
        lax.fori_loop(0, 4, groups, 0)

    def make_brep(src, out):
        def one(i, carry):
            out[i] = lanes(src[lax.div(i, 8)], in_grp + 16 * lax.rem(i, 8))
            return carry
        lax.fori_loop(0, 16, one, 0, unroll=True)

    def part(i, acc, left, right, step):
        def pivot(u, acc):
            b = right[i * (step // 8) + lax.div(u, 8), :, pl.ds(lax.rem(u, 8), 1), :]
            return jnp.minimum(acc, left(i * (step // 16) + lax.div(u, 16), i * step + u, lax.rem(u, 16))[:, None] + b[None])
        return lax.fori_loop(0, step, pivot, acc, unroll=True)

    def product(acc, left, right, step):
        return lax.fori_loop(0, BLK // step, lambda i, acc: part(i, acc, left, right, step), acc, unroll=step == BLK)

    def close_and_send(rnd, a, x):
        close(rnd, a, x)
        send_dia(rnd)

    slot_r = jnp.where(my_row == 0, 0, ROUNDS)
    slot_c = jnp.where(col == 0, 0, ROUNDS)
    def unpack(a, x):
        for r in range(2):
            tiles = swap_chunks(in_ref[a, 64 * r:64 * r + 64, BLK * x:BLK * x + BLK].reshape(8, 8, 128))
            mat[a, x, r] = tiles
            if a == 0:
                rowp[slot_r, x, r] = tiles
            if x == 0:
                colp[slot_c, a, r] = tiles

    unpack(0, 0)

    @pl.when((my_row == 0) & (col == 0))
    def _():
        close(0, 0, 0)
        pl.semaphore_wait(barrier, 7)
        send_dia(0)
    for a in range(2):
        for x in range(4):
            if a + x:
                unpack(a, x)

    @pl.when((my_row != 0) | (col != 0))
    def _():
        pl.semaphore_wait(barrier, 7)

    @pl.when(my_row == 0)
    def _():
        for x in (1, 2, 3):
            send_row(0, x)

        @pl.when(col != 0)
        def _():
            send_row(0, 0)

    @pl.when(col == 0)
    def _():
        @pl.when(my_row != 0)
        def _():
            col_copy(0, 0).start()
        col_copy(0, 1).start()

    def drain(k):
        is_row, is_col = my_row == k % 4, col == k % 2
        for x in range(4):
            @pl.when(is_row & (~is_col | (x != k // 2)))
            def _():
                for i in range(3):
                    row_copy(k, x, i).wait_send()
        for a in range(2):
            @pl.when(is_col & (~is_row | (a != k // 4)))
            def _():
                col_copy(k, a).wait_send()

        @pl.when(is_row & is_col)
        def _():
            for i in range(4):
                for r in range(2):
                    dia_copy(k, i, r).wait_send()

        @pl.when(passes(k))
        def _():
            for r in range(2):
                dia_pass(k, r).wait_send()

    def one_round(k, carry):
        n = k + 1
        more = n < ROUNDS
        own_row = (my_row == n % 4) & more
        own_col = (col == n % 2) & more
        a1 = jnp.minimum(n // 4, 1)
        x1 = ((n + jnp.where(col == n % 2, 0, 1)) // 2) % 4
        xk = k // 2
        is_row, is_col = my_row == k % 4, col == k % 2

        def first_rows():
            @pl.when(~is_row)
            def _():
                row_copy(k, x1, 0).wait_recv()
            make_brep(rowp.at[k, x1], brep.at[x1])

        @pl.when(~is_col)
        def _():
            first_rows()

        @pl.when(k > 0)
        def _():
            drain(k - 1)

        def closed_half(r):
            @pl.when(~is_row | ~is_col)
            def _():
                dia_copy(k, 0, r).wait_recv()

            @pl.when(passes(k))
            def _():
                dia_pass(k, r).start()

            def one(q, carry):
                brepd[8 * r + q] = lanes(dst[k, r], in_grp + 16 * q)
                return carry
            lax.fori_loop(0, 8, one, 0, unroll=True)

        def wait_row(x):
            @pl.when(~is_row)
            def _():
                row_copy(k, x, 0).wait_recv()


        def head(h, carry):
            a = jnp.where(h == 0, a1, 1 - a1)

            on_diag = is_row & (a == k // 4)
            send_it = own_row & (h == 0)

            @pl.when(~is_col & ~on_diag)
            def _():
                col_copy(k, a).wait_recv()

            pan = colp.at[k, a]

            def left(c, p, l):
                return lanes(pan[:, c], grp_base + l)

            @pl.when(h == 0)
            def _():
                @pl.when(~on_diag)
                def _():
                    cpr[...] = pan[...]

                def by_half(r, carry):
                    closed_half(r)

                    @pl.when(~on_diag)
                    def _():
                        cpr[...] = part(r, cpr[...], left, brepd, BLK // 2)
                    return carry
                lax.fori_loop(0, 2, by_half, 0)

            @pl.when(on_diag)
            def _():
                cpr[...] = dst[k]

            @pl.when(~on_diag & (h == 1))
            def _():
                cpr[...] = product(pan[...], left, brepd, HEAD_STEP)

            @pl.when(is_col)
            def _():
                mat[a, xk] = cpr[...]

                @pl.when(h == 0)
                def _():
                    first_rows()

            @pl.when(is_col & send_it)
            def _():
                rowp[n, xk] = cpr[...]
                send_row(n, xk)

            tab = cb.at[a]

            def fly(c, p, l):
                avs = lanes(cpr[:, c], grp_base + l)
                tab[p] = avs
                return avs
            acc = product(mat[a, x1], fly, brep.at[x1], HEAD_STEP)
            mat[a, x1] = acc
            rowp[jnp.where(send_it, n, ROUNDS), x1] = acc
            colp[jnp.where(own_col, n, ROUNDS), a] = acc

            @pl.when(send_it & ~own_col)
            def _():
                send_row(n, x1)

            @pl.when(own_col & ~send_it)
            def _():
                col_copy(n, a).start()

            @pl.when(send_it & own_col)
            def _():
                close_and_send(n, a, x1)
            return carry
        lax.fori_loop(0, 2, head, 0)

        def tail(t, carry):
            h = t // 3
            a = jnp.where(h == 0, a1, 1 - a1)
            x = (x1 + 1 + t % 3) % 4

            @pl.when((col != k % 2) | (t % 3 != 2))
            def _():
                @pl.when(h == 0)
                def _():
                    wait_row(x)
                    make_brep(rowp.at[k, x], brep.at[x])

                tab = cb.at[a]
                acc = product(mat[a, x], lambda c, p, l: tab[p], brep.at[x], TAIL_STEP)
                mat[a, x] = acc
                send_it = own_row & (h == 0)
                rowp[jnp.where(send_it, n, ROUNDS), x] = acc

                @pl.when(send_it)
                def _():
                    send_row(n, x)
            return carry
        lax.fori_loop(0, 6, tail, 0)
        return carry
    lax.fori_loop(0, ROUNDS, one_round, 0)

    for a in range(2):
        for x in range(4):
            for r in range(2):
                tiles = swap_chunks(mat[a, x, r])
                out_ref[a, 64 * r:64 * r + 64, BLK * x:BLK * x + BLK] = tiles.reshape(64, 128)

    drain(ROUNDS - 1)


def solution(mesh):
    spec = P(('parts', 'row', 'sub'), None, 'col')
    tile = (8, 128)
    dma = pltpu.SemaphoreType.DMA

    def local_run(local_dist):
        return pl.pallas_call(
            kernel,
            out_shape=jax.ShapeDtypeStruct(local_dist.shape, local_dist.dtype),
            in_specs=[pl.BlockSpec(memory_space=pltpu.VMEM)],
            out_specs=pl.BlockSpec(memory_space=pltpu.VMEM),
            scratch_shapes=[
                pltpu.VMEM((2, 4, 2, 8) + tile, jnp.float32),
                pltpu.VMEM((ROUNDS + 1, 4, 2, 8) + tile, jnp.float32),
                pltpu.VMEM((ROUNDS + 1, 2, 2, 8) + tile, jnp.float32),
                pltpu.VMEM((ROUNDS, 2, 8) + tile, jnp.float32),
                pltpu.VMEM((2, BLK, 2) + tile, jnp.float32),
                pltpu.VMEM((4, 16, 8) + tile, jnp.float32),
                pltpu.VMEM((16, 8) + tile, jnp.float32),
                pltpu.VMEM((2, 8) + tile, jnp.float32),
                dma((ROUNDS, 4, 3)), dma((ROUNDS, 4)),
                dma((ROUNDS, 2)), dma((ROUNDS, 2)),
                dma((ROUNDS, 4, 2)), dma((ROUNDS, 2)), dma((ROUNDS, 2)),
            ],
            compiler_params=pltpu.CompilerParams(collective_id=0, has_side_effects=True),
            name='apsp',
        )(local_dist)

    return jax.shard_map(local_run, mesh=mesh, in_specs=(spec,), out_specs=spec, check_vma=False)
```

```python
import functools

import jax
import jax.numpy as jnp
from jax import lax
from jax.experimental import pallas as pl
from jax.experimental.pallas import tpu as pltpu
from jax.sharding import PartitionSpec as P

MESH = pl.DeviceIdType.MESH
BLK = 128
ROUNDS = 8
HEAD_STEP, TAIL_STEP = 128, 64
ROW_PEERS = ((0, 1), (1, 1), (1, 0))
ALL_PEERS = ((1, 0, 1), (1, 1, 1), (0, 0, 1), (0, 1, 1), (1, 0, 0), (0, 1, 0), (1, 1, 0))


def lanes(tiles, idx):
    flat = tiles.reshape(-1, 128)
    idx = jnp.broadcast_to(idx, tiles.shape).reshape(-1, 128)
    return jnp.take_along_axis(flat, idx, axis=1, mode='promise_in_bounds').reshape(tiles.shape)


def kernel(in_ref, out_ref, mat, rowp, colp, dst, cb, brep, brepd, cpr,

           row_send, row_recv, col_send, col_recv, dia_send, dia_fwd, dia_recv):
    row, sub, col = lax.axis_index('row'), lax.axis_index('sub'), lax.axis_index('col')
    my_row = row * 2 + sub
    lane = lax.broadcasted_iota(jnp.int32, (8, 128), 1)
    in_grp = lane & 15
    grp_base = lane - in_grp
    nth_pivot = lax.broadcasted_iota(jnp.int32, (8, 8, 128), 0)

    def peer(d_col, d_row, d_sub):
        return {'col': (col + d_col) % 2, 'row': (row + d_row) % 2, 'sub': (sub + d_sub) % 2}

    barrier = pltpu.get_barrier_semaphore()
    for offs in ALL_PEERS:
        pl.semaphore_signal(barrier, inc=1, device_id=peer(*offs), device_id_type=MESH)

    def swap_chunks(tiles):
        for bit in (1, 2, 4):
            mask = (lane & (16 * bit)) == 0
            pairs = tiles.reshape(8 // (2 * bit), 2, bit, 8, 128)
            lo, hi = pairs[:, 0].reshape(-1, 128), pairs[:, 1].reshape(-1, 128)
            lo_up = pltpu.roll(lo, 128 - 16 * bit, 1)
            hi_up = pltpu.roll(hi, 16 * bit, 1)
            lo, hi, lo_up, hi_up = (v.reshape(8 // (2 * bit), bit, 8, 128) for v in (lo, hi, lo_up, hi_up))
            tiles = jnp.stack([jnp.where(mask, lo, hi_up), jnp.where(mask, lo_up, hi)], axis=1).reshape(8, 8, 128)
        return tiles

    def row_copy(rnd, x, i):
        d_row, d_sub = ROW_PEERS[i]
        return pltpu.make_async_remote_copy(
            src_ref=rowp.at[rnd, x], dst_ref=rowp.at[rnd, x],
            send_sem=row_send.at[rnd, x, i], recv_sem=row_recv.at[rnd, x],
            device_id=peer(0, d_row, d_sub), device_id_type=MESH)

    def col_copy(rnd, a):
        return pltpu.make_async_remote_copy(
            src_ref=colp.at[rnd, a], dst_ref=colp.at[rnd, a],
            send_sem=col_send.at[rnd, a], recv_sem=col_recv.at[rnd, a],
            device_id=peer(1, 0, 0), device_id_type=MESH)

    def dia_copy(rnd, i):
        turn = rnd % 2
        offs = ((1, turn, 1), (1, 1 - turn, 1), (0, 1, 1), (0, 0, 1))[i]
        return pltpu.make_async_remote_copy(
            src_ref=dst.at[rnd], dst_ref=dst.at[rnd],
            send_sem=dia_send.at[rnd, i], recv_sem=dia_recv.at[rnd],
            device_id=peer(*offs), device_id_type=MESH)

    def dia_pass(rnd):
        return pltpu.make_async_remote_copy(
            src_ref=dst.at[rnd], dst_ref=dst.at[rnd],
            send_sem=dia_fwd.at[rnd], recv_sem=dia_recv.at[rnd],
            device_id=peer(0, 0, 1), device_id_type=MESH)

    def passes(rnd):
        return (sub != rnd % 2) & ((col != rnd % 2) | (row != (rnd % 4) // 2))

    def send_row(rnd, x):
        for i in range(3):
            row_copy(rnd, x, i).start()

    def send_dia(rnd):
        for i in range(4):
            dia_copy(rnd, i).start()

    def close(rnd, a, x):
        dst[rnd] = mat[a, x]

        def group(g, carry):
            rg, cg = lax.div(g, 8), lax.div(g, 2)
            q, half = lax.rem(g, 8), lax.rem(g, 2) * 8
            ucol = lanes(jnp.broadcast_to(dst[rnd, rg, cg][None], (8, 8, 128)), nth_pivot + (16 * q + half))
            rows = lanes(dst[rnd, rg], in_grp[None] + 16 * q)
            left = lanes(jnp.broadcast_to(dst[rnd, :, cg][None], (8, 2, 8, 128)),
                         (nth_pivot + (grp_base + half)[None])[:, None])
            for p in range(8):
                rows = jnp.minimum(rows, ucol[0][None] + rows[:, p:p + 1, :])
                if p < 7:
                    ucol = jnp.minimum(ucol[1:], ucol[0][None] + ucol[1:, p:p + 1, :])
            block = dst[rnd]
            for p in range(8):
                block = jnp.minimum(block, left[p][:, None] + rows[:, p:p + 1, :][None])
            dst[rnd] = block
            return carry

        def groups(i, carry):
            return lax.fori_loop(0, 4, lambda u, c: group(i * 4 + u, c), carry, unroll=True)
        lax.fori_loop(0, 4, groups, 0)

    def make_brep(src, out):
        def one(i, carry):
            out[i] = lanes(src[lax.div(i, 8)], in_grp + 16 * lax.rem(i, 8))
            return carry
        lax.fori_loop(0, 16, one, 0, unroll=True)

    def product(acc, left, right, step):
        def chunk(i, acc):
            def pivot(u, acc):
                b = right[i * (step // 8) + lax.div(u, 8), :, pl.ds(lax.rem(u, 8), 1), :]
                return jnp.minimum(acc, left(i * (step // 16) + lax.div(u, 16), i * step + u, lax.rem(u, 16))[:, None] + b[None])
            return lax.fori_loop(0, step, pivot, acc, unroll=True)
        return lax.fori_loop(0, BLK // step, chunk, acc, unroll=step == BLK)

    def close_and_send(rnd, a, x):
        close(rnd, a, x)
        send_dia(rnd)

    slot_r = jnp.where(my_row == 0, 0, ROUNDS)
    slot_c = jnp.where(col == 0, 0, ROUNDS)
    def unpack(a, x):
        for r in range(2):
            tiles = swap_chunks(in_ref[a, 64 * r:64 * r + 64, BLK * x:BLK * x + BLK].reshape(8, 8, 128))
            mat[a, x, r] = tiles
            if a == 0:
                rowp[slot_r, x, r] = tiles
            if x == 0:
                colp[slot_c, a, r] = tiles

    unpack(0, 0)

    @pl.when((my_row == 0) & (col == 0))
    def _():
        close(0, 0, 0)
        pl.semaphore_wait(barrier, 7)
        send_dia(0)
    for a in range(2):
        for x in range(4):
            if a + x:
                unpack(a, x)

    @pl.when((my_row != 0) | (col != 0))
    def _():
        pl.semaphore_wait(barrier, 7)

    @pl.when(my_row == 0)
    def _():
        for x in (1, 2, 3):
            send_row(0, x)

        @pl.when(col != 0)
        def _():
            send_row(0, 0)

    @pl.when(col == 0)
    def _():
        @pl.when(my_row != 0)
        def _():
            col_copy(0, 0).start()
        col_copy(0, 1).start()

    def one_round(k, carry):
        n = k + 1
        more = n < ROUNDS
        own_row = (my_row == n % 4) & more
        own_col = (col == n % 2) & more
        a1 = jnp.minimum(n // 4, 1)
        x1 = ((n + jnp.where(col == n % 2, 0, 1)) // 2) % 4
        xk = k // 2
        is_row, is_col = my_row == k % 4, col == k % 2

        def first_rows():
            @pl.when(~is_row)
            def _():
                row_copy(k, x1, 0).wait_recv()
            make_brep(rowp.at[k, x1], brep.at[x1])

        @pl.when(~is_col)
        def _():
            first_rows()

        @pl.when(~is_row | ~is_col)
        def _():
            dia_copy(k, 0).wait_recv()

        @pl.when(passes(k))
        def _():
            dia_pass(k).start()

        def wait_row(x):
            @pl.when(~is_row)
            def _():
                row_copy(k, x, 0).wait_recv()

        make_brep(dst.at[k], brepd)

        def head(h, carry):
            a = jnp.where(h == 0, a1, 1 - a1)

            on_diag = is_row & (a == k // 4)
            send_it = own_row & (h == 0)

            @pl.when(~is_col & ~on_diag)
            def _():
                col_copy(k, a).wait_recv()

            @pl.when(on_diag)
            def _():
                cpr[...] = dst[k]

            @pl.when(~on_diag)
            def _():
                pan = colp.at[k, a]
                cpr[...] = product(pan[...], lambda c, p, l: lanes(pan[:, c], grp_base + l), brepd, HEAD_STEP)

            @pl.when(is_col)
            def _():
                mat[a, xk] = cpr[...]

                @pl.when(h == 0)
                def _():
                    first_rows()

            @pl.when(is_col & send_it)
            def _():
                rowp[n, xk] = cpr[...]
                send_row(n, xk)

            tab = cb.at[a]

            def fly(c, p, l):
                avs = lanes(cpr[:, c], grp_base + l)
                tab[p] = avs
                return avs
            acc = product(mat[a, x1], fly, brep.at[x1], HEAD_STEP)
            mat[a, x1] = acc
            rowp[jnp.where(send_it, n, ROUNDS), x1] = acc
            colp[jnp.where(own_col, n, ROUNDS), a] = acc

            @pl.when(send_it & ~own_col)
            def _():
                send_row(n, x1)

            @pl.when(own_col & ~send_it)
            def _():
                col_copy(n, a).start()

            @pl.when(send_it & own_col)
            def _():
                close_and_send(n, a, x1)
            return carry

        def tail(phase, t, carry):
            h = t // 3
            a = jnp.where(h == 0, a1, 1 - a1)
            x = (x1 + 1 + t % 3) % 4

            @pl.when(((col != k % 2) | (t % 3 != 2)) & ((own_row & (h == phase)) | (~own_row & (phase == 1))))
            def _():
                @pl.when(h == 0)
                def _():
                    wait_row(x)
                    make_brep(rowp.at[k, x], brep.at[x])

                tab = cb.at[a]
                acc = product(mat[a, x], lambda c, p, l: tab[p], brep.at[x], TAIL_STEP)
                mat[a, x] = acc
                send_it = own_row & (h == 0)
                rowp[jnp.where(send_it, n, ROUNDS), x] = acc

                @pl.when(send_it)
                def _():
                    send_row(n, x)
            return carry
        def in_order(phase, carry):
            head(phase, carry)
            return lax.fori_loop(0, 6, functools.partial(tail, phase), carry)
        lax.fori_loop(0, 2, in_order, 0)
        return carry
    lax.fori_loop(0, ROUNDS, one_round, 0)

    for a in range(2):
        for x in range(4):
            for r in range(2):
                tiles = swap_chunks(mat[a, x, r])
                out_ref[a, 64 * r:64 * r + 64, BLK * x:BLK * x + BLK] = tiles.reshape(64, 128)

    def drain(k, carry):
        is_row, is_col = my_row == k % 4, col == k % 2
        for x in range(4):
            @pl.when(is_row & (~is_col | (x != k // 2)))
            def _():
                for i in range(3):
                    row_copy(k, x, i).wait_send()
        for a in range(2):
            @pl.when(is_col & (~is_row | (a != k // 4)))
            def _():
                col_copy(k, a).wait_send()

        @pl.when(is_row & is_col)
        def _():
            for i in range(4):
                dia_copy(k, i).wait_send()

        @pl.when(passes(k))
        def _():
            dia_pass(k).wait_send()
        return carry
    lax.fori_loop(0, ROUNDS, drain, 0)


def solution(mesh):
    spec = P(('parts', 'row', 'sub'), None, 'col')
    tile = (8, 128)
    dma = pltpu.SemaphoreType.DMA

    def local_run(local_dist):
        return pl.pallas_call(
            kernel,
            out_shape=jax.ShapeDtypeStruct(local_dist.shape, local_dist.dtype),
            in_specs=[pl.BlockSpec(memory_space=pltpu.VMEM)],
            out_specs=pl.BlockSpec(memory_space=pltpu.VMEM),
            scratch_shapes=[
                pltpu.VMEM((2, 4, 2, 8) + tile, jnp.float32),
                pltpu.VMEM((ROUNDS + 1, 4, 2, 8) + tile, jnp.float32),
                pltpu.VMEM((ROUNDS + 1, 2, 2, 8) + tile, jnp.float32),
                pltpu.VMEM((ROUNDS, 2, 8) + tile, jnp.float32),
                pltpu.VMEM((2, BLK, 2) + tile, jnp.float32),
                pltpu.VMEM((4, 16, 8) + tile, jnp.float32),
                pltpu.VMEM((16, 8) + tile, jnp.float32),
                pltpu.VMEM((2, 8) + tile, jnp.float32),
                dma((ROUNDS, 4, 3)), dma((ROUNDS, 4)),
                dma((ROUNDS, 2)), dma((ROUNDS, 2)),
                dma((ROUNDS, 4)), dma((ROUNDS,)), dma((ROUNDS,)),
            ],
            compiler_params=pltpu.CompilerParams(collective_id=0, has_side_effects=True),
            name='apsp',
        )(local_dist)

    return jax.shard_map(local_run, mesh=mesh, in_specs=(spec,), out_specs=spec, check_vma=False)
```

```python
import functools

import jax
import jax.numpy as jnp
from jax import lax
from jax.experimental import pallas as pl
from jax.experimental.pallas import tpu as pltpu
from jax.sharding import PartitionSpec as P

MESH = pl.DeviceIdType.MESH
BLK = 128
ROUNDS = 8
HEAD_STEP, TAIL_STEP = 128, 64
ROW_PEERS = ((0, 1), (1, 1), (1, 0))
ALL_PEERS = ((1, 0, 1), (1, 1, 1), (0, 0, 1), (0, 1, 1), (1, 0, 0), (0, 1, 0), (1, 1, 0))


def lanes(tiles, idx):
    flat = tiles.reshape(-1, 128)
    idx = jnp.broadcast_to(idx, tiles.shape).reshape(-1, 128)
    return jnp.take_along_axis(flat, idx, axis=1, mode='promise_in_bounds').reshape(tiles.shape)


def kernel(in_ref, out_ref, mat, rowp, colp, dst, cb, brep, brepd, cpr,

           row_send, row_recv, col_send, col_recv, dia_send, dia_fwd, dia_recv):
    row, sub, col = lax.axis_index('row'), lax.axis_index('sub'), lax.axis_index('col')
    my_row = row * 2 + sub
    lane = lax.broadcasted_iota(jnp.int32, (8, 128), 1)
    in_grp = lane & 15
    grp_base = lane - in_grp
    nth_pivot = lax.broadcasted_iota(jnp.int32, (8, 8, 128), 0)

    def peer(d_col, d_row, d_sub):
        return {'col': (col + d_col) % 2, 'row': (row + d_row) % 2, 'sub': (sub + d_sub) % 2}

    barrier = pltpu.get_barrier_semaphore()
    for offs in ALL_PEERS:
        pl.semaphore_signal(barrier, inc=1, device_id=peer(*offs), device_id_type=MESH)

    def swap_chunks(tiles):
        for bit in (1, 2, 4):
            mask = (lane & (16 * bit)) == 0
            pairs = tiles.reshape(8 // (2 * bit), 2, bit, 8, 128)
            lo, hi = pairs[:, 0].reshape(-1, 128), pairs[:, 1].reshape(-1, 128)
            lo_up = pltpu.roll(lo, 128 - 16 * bit, 1)
            hi_up = pltpu.roll(hi, 16 * bit, 1)
            lo, hi, lo_up, hi_up = (v.reshape(8 // (2 * bit), bit, 8, 128) for v in (lo, hi, lo_up, hi_up))
            tiles = jnp.stack([jnp.where(mask, lo, hi_up), jnp.where(mask, lo_up, hi)], axis=1).reshape(8, 8, 128)
        return tiles

    def row_copy(rnd, x, i):
        d_row, d_sub = ROW_PEERS[i]
        return pltpu.make_async_remote_copy(
            src_ref=rowp.at[rnd, x], dst_ref=rowp.at[rnd, x],
            send_sem=row_send.at[rnd, x, i], recv_sem=row_recv.at[rnd, x],
            device_id=peer(0, d_row, d_sub), device_id_type=MESH)

    def col_copy(rnd, a):
        return pltpu.make_async_remote_copy(
            src_ref=colp.at[rnd, a], dst_ref=colp.at[rnd, a],
            send_sem=col_send.at[rnd, a], recv_sem=col_recv.at[rnd, a],
            device_id=peer(1, 0, 0), device_id_type=MESH)

    def dia_copy(rnd, i):
        turn = rnd % 2
        offs = ((1, turn, 1), (1, 1 - turn, 1), (0, 1, 1), (0, 0, 1))[i]
        return pltpu.make_async_remote_copy(
            src_ref=dst.at[rnd], dst_ref=dst.at[rnd],
            send_sem=dia_send.at[rnd, i], recv_sem=dia_recv.at[rnd],
            device_id=peer(*offs), device_id_type=MESH)

    def dia_pass(rnd):
        return pltpu.make_async_remote_copy(
            src_ref=dst.at[rnd], dst_ref=dst.at[rnd],
            send_sem=dia_fwd.at[rnd], recv_sem=dia_recv.at[rnd],
            device_id=peer(0, 0, 1), device_id_type=MESH)

    def passes(rnd):
        return (sub != rnd % 2) & ((col != rnd % 2) | (row != (rnd % 4) // 2))

    def send_row(rnd, x):
        for i in range(3):
            row_copy(rnd, x, i).start()

    def send_dia(rnd):
        for i in range(4):
            dia_copy(rnd, i).start()

    def close(rnd, a, x):
        dst[rnd] = mat[a, x]

        def group(g, carry):
            rg, cg = lax.div(g, 8), lax.div(g, 2)
            q, half = lax.rem(g, 8), lax.rem(g, 2) * 8
            ucol = lanes(jnp.broadcast_to(dst[rnd, rg, cg][None], (8, 8, 128)), nth_pivot + (16 * q + half))
            rows = lanes(dst[rnd, rg], in_grp[None] + 16 * q)
            left = lanes(jnp.broadcast_to(dst[rnd, :, cg][None], (8, 2, 8, 128)),
                         (nth_pivot + (grp_base + half)[None])[:, None])
            for p in range(8):
                rows = jnp.minimum(rows, ucol[0][None] + rows[:, p:p + 1, :])
                if p < 7:
                    ucol = jnp.minimum(ucol[1:], ucol[0][None] + ucol[1:, p:p + 1, :])
            block = dst[rnd]
            for p in range(8):
                block = jnp.minimum(block, left[p][:, None] + rows[:, p:p + 1, :][None])
            dst[rnd] = block
            return carry

        def groups(i, carry):
            return lax.fori_loop(0, 4, lambda u, c: group(i * 4 + u, c), carry, unroll=True)
        lax.fori_loop(0, 4, groups, 0)

    def make_brep(src, out):
        def one(i, carry):
            out[i] = lanes(src[lax.div(i, 8)], in_grp + 16 * lax.rem(i, 8))
            return carry
        lax.fori_loop(0, 16, one, 0, unroll=True)

    def product(acc, left, right, step):
        def chunk(i, acc):
            def pivot(u, acc):
                b = right[i * (step // 8) + lax.div(u, 8), :, pl.ds(lax.rem(u, 8), 1), :]
                return jnp.minimum(acc, left(i * (step // 16) + lax.div(u, 16), i * step + u, lax.rem(u, 16))[:, None] + b[None])
            return lax.fori_loop(0, step, pivot, acc, unroll=True)
        return lax.fori_loop(0, BLK // step, chunk, acc, unroll=step == BLK)

    def close_and_send(rnd, a, x):
        close(rnd, a, x)
        send_dia(rnd)

    slot_r = jnp.where(my_row == 0, 0, ROUNDS)
    slot_c = jnp.where(col == 0, 0, ROUNDS)
    def unpack(a, x):
        for r in range(2):
            tiles = swap_chunks(in_ref[a, 64 * r:64 * r + 64, BLK * x:BLK * x + BLK].reshape(8, 8, 128))
            mat[a, x, r] = tiles
            if a == 0:
                rowp[slot_r, x, r] = tiles
            if x == 0:
                colp[slot_c, a, r] = tiles

    unpack(0, 0)

    @pl.when((my_row == 0) & (col == 0))
    def _():
        close(0, 0, 0)
        pl.semaphore_wait(barrier, 7)
        send_dia(0)
    for a in range(2):
        for x in range(4):
            if a + x:
                unpack(a, x)

    @pl.when((my_row != 0) | (col != 0))
    def _():
        pl.semaphore_wait(barrier, 7)

    @pl.when(my_row == 0)
    def _():
        for x in (1, 2, 3):
            send_row(0, x)

        @pl.when(col != 0)
        def _():
            send_row(0, 0)

    @pl.when(col == 0)
    def _():
        @pl.when(my_row != 0)
        def _():
            col_copy(0, 0).start()
        col_copy(0, 1).start()

    def one_round(k, carry):
        n = k + 1
        more = n < ROUNDS
        own_row = (my_row == n % 4) & more
        own_col = (col == n % 2) & more
        a1 = jnp.minimum(n // 4, 1)
        x1 = ((n + jnp.where(col == n % 2, 0, 1)) // 2) % 4
        xk = k // 2
        is_row, is_col = my_row == k % 4, col == k % 2

        def first_rows():
            @pl.when(~is_row)
            def _():
                row_copy(k, x1, 0).wait_recv()
            make_brep(rowp.at[k, x1], brep.at[x1])

        @pl.when(~is_col)
        def _():
            first_rows()

        @pl.when(~is_row | ~is_col)
        def _():
            dia_copy(k, 0).wait_recv()

        @pl.when(passes(k))
        def _():
            dia_pass(k).start()

        def wait_row(x):
            @pl.when(~is_row)
            def _():
                row_copy(k, x, 0).wait_recv()

        make_brep(dst.at[k], brepd)

        def head(h, carry):
            a = jnp.where(h == 0, a1, 1 - a1)

            on_diag = is_row & (a == k // 4)
            send_it = own_row & (h == 0)

            @pl.when(~is_col & ~on_diag)
            def _():
                col_copy(k, a).wait_recv()

            @pl.when(on_diag)
            def _():
                cpr[...] = dst[k]

            @pl.when(~on_diag)
            def _():
                pan = colp.at[k, a]
                cpr[...] = product(pan[...], lambda c, p, l: lanes(pan[:, c], grp_base + l), brepd, HEAD_STEP)

            @pl.when(is_col)
            def _():
                mat[a, xk] = cpr[...]

                @pl.when(h == 0)
                def _():
                    first_rows()

            @pl.when(is_col & send_it)
            def _():
                rowp[n, xk] = cpr[...]
                send_row(n, xk)

            tab = cb.at[a]

            def fly(c, p, l):
                avs = lanes(cpr[:, c], grp_base + l)
                tab[p] = avs
                return avs
            acc = product(mat[a, x1], fly, brep.at[x1], HEAD_STEP)
            mat[a, x1] = acc
            rowp[jnp.where(send_it, n, ROUNDS), x1] = acc
            colp[jnp.where(own_col, n, ROUNDS), a] = acc

            @pl.when(send_it & ~own_col)
            def _():
                send_row(n, x1)

            @pl.when(own_col & ~send_it)
            def _():
                col_copy(n, a).start()

            @pl.when(send_it & own_col)
            def _():
                close_and_send(n, a, x1)
            return carry

        def tail(phase, t, carry):
            h = t // 3
            a = jnp.where(h == 0, a1, 1 - a1)
            x = (x1 + 1 + t % 3) % 4

            @pl.when(((col != k % 2) | (t % 3 != 2)) & ((own_row & (h == phase)) | (~own_row & (phase == 1))))
            def _():
                @pl.when(h == 0)
                def _():
                    wait_row(x)
                    make_brep(rowp.at[k, x], brep.at[x])

                tab = cb.at[a]
                acc = product(mat[a, x], lambda c, p, l: tab[p], brep.at[x], TAIL_STEP)
                mat[a, x] = acc
                send_it = own_row & (h == 0)
                rowp[jnp.where(send_it, n, ROUNDS), x] = acc

                @pl.when(send_it)
                def _():
                    send_row(n, x)
            return carry
        def in_order(phase, carry):
            head(phase, carry)
            return lax.fori_loop(0, 6, functools.partial(tail, phase), carry)
        lax.fori_loop(0, 2, in_order, 0)
        return carry
    lax.fori_loop(0, ROUNDS, one_round, 0)

    for a in range(2):
        for x in range(4):
            for r in range(2):
                tiles = swap_chunks(mat[a, x, r])
                out_ref[a, 64 * r:64 * r + 64, BLK * x:BLK * x + BLK] = tiles.reshape(64, 128)

    def drain(k, carry):
        is_row, is_col = my_row == k % 4, col == k % 2
        for x in range(4):
            @pl.when(is_row & (~is_col | (x != k // 2)))
            def _():
                for i in range(3):
                    row_copy(k, x, i).wait_send()
        for a in range(2):
            @pl.when(is_col & (~is_row | (a != k // 4)))
            def _():
                col_copy(k, a).wait_send()

        @pl.when(is_row & is_col)
        def _():
            for i in range(4):
                dia_copy(k, i).wait_send()

        @pl.when(passes(k))
        def _():
            dia_pass(k).wait_send()
        return carry
    lax.fori_loop(0, ROUNDS, drain, 0)


def solution(mesh):
    spec = P(('parts', 'row', 'sub'), None, 'col')
    tile = (8, 128)
    dma = pltpu.SemaphoreType.DMA

    def local_run(local_dist):
        return pl.pallas_call(
            kernel,
            out_shape=jax.ShapeDtypeStruct(local_dist.shape, local_dist.dtype),
            in_specs=[pl.BlockSpec(memory_space=pltpu.VMEM)],
            out_specs=pl.BlockSpec(memory_space=pltpu.VMEM),
            scratch_shapes=[
                pltpu.VMEM((2, 4, 2, 8) + tile, jnp.float32),
                pltpu.VMEM((ROUNDS + 1, 4, 2, 8) + tile, jnp.float32),
                pltpu.VMEM((ROUNDS + 1, 2, 2, 8) + tile, jnp.float32),
                pltpu.VMEM((ROUNDS, 2, 8) + tile, jnp.float32),
                pltpu.VMEM((2, BLK, 2) + tile, jnp.float32),
                pltpu.VMEM((4, 16, 8) + tile, jnp.float32),
                pltpu.VMEM((16, 8) + tile, jnp.float32),
                pltpu.VMEM((2, 8) + tile, jnp.float32),
                dma((ROUNDS, 4, 3)), dma((ROUNDS, 4)),
                dma((ROUNDS, 2)), dma((ROUNDS, 2)),
                dma((ROUNDS, 4)), dma((ROUNDS,)), dma((ROUNDS,)),
            ],
            compiler_params=pltpu.CompilerParams(collective_id=0, has_side_effects=True, vmem_limit_bytes=16 * 2 ** 20),
            name='apsp',
        )(local_dist)

    return jax.shard_map(local_run, mesh=mesh, in_specs=(spec,), out_specs=spec, check_vma=False)
```

```python
import functools

import jax
import jax.numpy as jnp
from jax import lax
from jax.experimental import pallas as pl
from jax.experimental.pallas import tpu as pltpu
from jax.sharding import PartitionSpec as P

MESH = pl.DeviceIdType.MESH
BLK = 128
ROUNDS = 8
HEAD_STEP, TAIL_STEP = 128, 64
ROW_PEERS = ((0, 1), (1, 1), (1, 0))
ALL_PEERS = ((1, 0, 1), (1, 1, 1), (0, 0, 1), (0, 1, 1), (1, 0, 0), (0, 1, 0), (1, 1, 0))


def lanes(tiles, idx):
    flat = tiles.reshape(-1, 128)
    idx = jnp.broadcast_to(idx, tiles.shape).reshape(-1, 128)
    return jnp.take_along_axis(flat, idx, axis=1, mode='promise_in_bounds').reshape(tiles.shape)


def kernel(src_ref, out_ref, in_ref, in_sem, mat, rowp, colp, dst, cb, brep, brepd, cpr,

           row_send, row_recv, col_send, col_recv, dia_send, dia_fwd, dia_recv):
    row, sub, col = lax.axis_index('row'), lax.axis_index('sub'), lax.axis_index('col')
    my_row = row * 2 + sub
    lane = lax.broadcasted_iota(jnp.int32, (8, 128), 1)
    in_grp = lane & 15
    grp_base = lane - in_grp
    nth_pivot = lax.broadcasted_iota(jnp.int32, (8, 8, 128), 0)

    def peer(d_col, d_row, d_sub):
        return {'col': (col + d_col) % 2, 'row': (row + d_row) % 2, 'sub': (sub + d_sub) % 2}

    barrier = pltpu.get_barrier_semaphore()
    for offs in ALL_PEERS:
        pl.semaphore_signal(barrier, inc=1, device_id=peer(*offs), device_id_type=MESH)
    fetch = pltpu.make_async_copy(src_ref, in_ref, in_sem)
    fetch.start()

    def swap_chunks(tiles):
        for bit in (1, 2, 4):
            mask = (lane & (16 * bit)) == 0
            pairs = tiles.reshape(8 // (2 * bit), 2, bit, 8, 128)
            lo, hi = pairs[:, 0].reshape(-1, 128), pairs[:, 1].reshape(-1, 128)
            lo_up = pltpu.roll(lo, 128 - 16 * bit, 1)
            hi_up = pltpu.roll(hi, 16 * bit, 1)
            lo, hi, lo_up, hi_up = (v.reshape(8 // (2 * bit), bit, 8, 128) for v in (lo, hi, lo_up, hi_up))
            tiles = jnp.stack([jnp.where(mask, lo, hi_up), jnp.where(mask, lo_up, hi)], axis=1).reshape(8, 8, 128)
        return tiles

    def row_copy(rnd, x, i):
        d_row, d_sub = ROW_PEERS[i]
        return pltpu.make_async_remote_copy(
            src_ref=rowp.at[rnd, x], dst_ref=rowp.at[rnd, x],
            send_sem=row_send.at[rnd, x, i], recv_sem=row_recv.at[rnd, x],
            device_id=peer(0, d_row, d_sub), device_id_type=MESH)

    def col_copy(rnd, a):
        return pltpu.make_async_remote_copy(
            src_ref=colp.at[rnd, a], dst_ref=colp.at[rnd, a],
            send_sem=col_send.at[rnd, a], recv_sem=col_recv.at[rnd, a],
            device_id=peer(1, 0, 0), device_id_type=MESH)

    def dia_copy(rnd, i):
        turn = rnd % 2
        offs = ((1, turn, 1), (1, 1 - turn, 1), (0, 1, 1), (0, 0, 1))[i]
        return pltpu.make_async_remote_copy(
            src_ref=dst.at[rnd], dst_ref=dst.at[rnd],
            send_sem=dia_send.at[rnd, i], recv_sem=dia_recv.at[rnd],
            device_id=peer(*offs), device_id_type=MESH)

    def dia_pass(rnd):
        return pltpu.make_async_remote_copy(
            src_ref=dst.at[rnd], dst_ref=dst.at[rnd],
            send_sem=dia_fwd.at[rnd], recv_sem=dia_recv.at[rnd],
            device_id=peer(0, 0, 1), device_id_type=MESH)

    def passes(rnd):
        return (sub != rnd % 2) & ((col != rnd % 2) | (row != (rnd % 4) // 2))

    def send_row(rnd, x):
        for i in range(3):
            row_copy(rnd, x, i).start()

    def send_dia(rnd):
        for i in range(4):
            dia_copy(rnd, i).start()

    def close(rnd, a, x):
        dst[rnd] = mat[a, x]

        def group(g, carry):
            rg, cg = lax.div(g, 8), lax.div(g, 2)
            q, half = lax.rem(g, 8), lax.rem(g, 2) * 8
            ucol = lanes(jnp.broadcast_to(dst[rnd, rg, cg][None], (8, 8, 128)), nth_pivot + (16 * q + half))
            rows = lanes(dst[rnd, rg], in_grp[None] + 16 * q)
            left = lanes(jnp.broadcast_to(dst[rnd, :, cg][None], (8, 2, 8, 128)),
                         (nth_pivot + (grp_base + half)[None])[:, None])
            for p in range(8):
                rows = jnp.minimum(rows, ucol[0][None] + rows[:, p:p + 1, :])
                if p < 7:
                    ucol = jnp.minimum(ucol[1:], ucol[0][None] + ucol[1:, p:p + 1, :])
            block = dst[rnd]
            for p in range(8):
                block = jnp.minimum(block, left[p][:, None] + rows[:, p:p + 1, :][None])
            dst[rnd] = block
            return carry

        def groups(i, carry):
            return lax.fori_loop(0, 4, lambda u, c: group(i * 4 + u, c), carry, unroll=True)
        lax.fori_loop(0, 4, groups, 0)

    def make_brep(src, out):
        def one(i, carry):
            out[i] = lanes(src[lax.div(i, 8)], in_grp + 16 * lax.rem(i, 8))
            return carry
        lax.fori_loop(0, 16, one, 0, unroll=True)

    def product(acc, left, right, step):
        def chunk(i, acc):
            def pivot(u, acc):
                b = right[i * (step // 8) + lax.div(u, 8), :, pl.ds(lax.rem(u, 8), 1), :]
                return jnp.minimum(acc, left(i * (step // 16) + lax.div(u, 16), i * step + u, lax.rem(u, 16))[:, None] + b[None])
            return lax.fori_loop(0, step, pivot, acc, unroll=True)
        return lax.fori_loop(0, BLK // step, chunk, acc, unroll=step == BLK)

    def close_and_send(rnd, a, x):
        close(rnd, a, x)
        send_dia(rnd)

    slot_r = jnp.where(my_row == 0, 0, ROUNDS)
    slot_c = jnp.where(col == 0, 0, ROUNDS)
    def unpack(a, x):
        for r in range(2):
            tiles = swap_chunks(in_ref[a, 64 * r:64 * r + 64, BLK * x:BLK * x + BLK].reshape(8, 8, 128))
            mat[a, x, r] = tiles
            if a == 0:
                rowp[slot_r, x, r] = tiles
            if x == 0:
                colp[slot_c, a, r] = tiles

    fetch.wait()
    unpack(0, 0)

    @pl.when((my_row == 0) & (col == 0))
    def _():
        close(0, 0, 0)
        pl.semaphore_wait(barrier, 7)
        send_dia(0)
    for a in range(2):
        for x in range(4):
            if a + x:
                unpack(a, x)

    @pl.when((my_row != 0) | (col != 0))
    def _():
        pl.semaphore_wait(barrier, 7)

    @pl.when(my_row == 0)
    def _():
        for x in (1, 2, 3):
            send_row(0, x)

        @pl.when(col != 0)
        def _():
            send_row(0, 0)

    @pl.when(col == 0)
    def _():
        @pl.when(my_row != 0)
        def _():
            col_copy(0, 0).start()
        col_copy(0, 1).start()

    def one_round(k, carry):
        n = k + 1
        more = n < ROUNDS
        own_row = (my_row == n % 4) & more
        own_col = (col == n % 2) & more
        a1 = jnp.minimum(n // 4, 1)
        x1 = ((n + jnp.where(col == n % 2, 0, 1)) // 2) % 4
        xk = k // 2
        is_row, is_col = my_row == k % 4, col == k % 2

        def first_rows():
            @pl.when(~is_row)
            def _():
                row_copy(k, x1, 0).wait_recv()
            make_brep(rowp.at[k, x1], brep.at[x1])

        @pl.when(~is_col)
        def _():
            first_rows()

        @pl.when(~is_row | ~is_col)
        def _():
            dia_copy(k, 0).wait_recv()

        @pl.when(passes(k))
        def _():
            dia_pass(k).start()

        def wait_row(x):
            @pl.when(~is_row)
            def _():
                row_copy(k, x, 0).wait_recv()

        make_brep(dst.at[k], brepd)

        def head(h, carry):
            a = jnp.where(h == 0, a1, 1 - a1)

            on_diag = is_row & (a == k // 4)
            send_it = own_row & (h == 0)

            @pl.when(~is_col & ~on_diag)
            def _():
                col_copy(k, a).wait_recv()

            @pl.when(on_diag)
            def _():
                cpr[...] = dst[k]

            @pl.when(~on_diag)
            def _():
                pan = colp.at[k, a]
                cpr[...] = product(pan[...], lambda c, p, l: lanes(pan[:, c], grp_base + l), brepd, HEAD_STEP)

            @pl.when(is_col)
            def _():
                mat[a, xk] = cpr[...]

                @pl.when(h == 0)
                def _():
                    first_rows()

            @pl.when(is_col & send_it)
            def _():
                rowp[n, xk] = cpr[...]
                send_row(n, xk)

            tab = cb.at[a]

            def fly(c, p, l):
                avs = lanes(cpr[:, c], grp_base + l)
                tab[p] = avs
                return avs
            acc = product(mat[a, x1], fly, brep.at[x1], HEAD_STEP)
            mat[a, x1] = acc
            rowp[jnp.where(send_it, n, ROUNDS), x1] = acc
            colp[jnp.where(own_col, n, ROUNDS), a] = acc

            @pl.when(send_it & ~own_col)
            def _():
                send_row(n, x1)

            @pl.when(own_col & ~send_it)
            def _():
                col_copy(n, a).start()

            @pl.when(send_it & own_col)
            def _():
                close_and_send(n, a, x1)
            return carry

        def tail(phase, t, carry):
            h = t // 3
            a = jnp.where(h == 0, a1, 1 - a1)
            x = (x1 + 1 + t % 3) % 4

            @pl.when(((col != k % 2) | (t % 3 != 2)) & ((own_row & (h == phase)) | (~own_row & (phase == 1))))
            def _():
                @pl.when(h == 0)
                def _():
                    wait_row(x)
                    make_brep(rowp.at[k, x], brep.at[x])

                tab = cb.at[a]
                acc = product(mat[a, x], lambda c, p, l: tab[p], brep.at[x], TAIL_STEP)
                mat[a, x] = acc
                send_it = own_row & (h == 0)
                rowp[jnp.where(send_it, n, ROUNDS), x] = acc

                @pl.when(send_it)
                def _():
                    send_row(n, x)
            return carry
        def in_order(phase, carry):
            head(phase, carry)
            return lax.fori_loop(0, 6, functools.partial(tail, phase), carry)
        lax.fori_loop(0, 2, in_order, 0)
        return carry
    lax.fori_loop(0, ROUNDS, one_round, 0)

    for a in range(2):
        for x in range(4):
            for r in range(2):
                tiles = swap_chunks(mat[a, x, r])
                out_ref[a, 64 * r:64 * r + 64, BLK * x:BLK * x + BLK] = tiles.reshape(64, 128)

    def drain(k, carry):
        is_row, is_col = my_row == k % 4, col == k % 2
        for x in range(4):
            @pl.when(is_row & (~is_col | (x != k // 2)))
            def _():
                for i in range(3):
                    row_copy(k, x, i).wait_send()
        for a in range(2):
            @pl.when(is_col & (~is_row | (a != k // 4)))
            def _():
                col_copy(k, a).wait_send()

        @pl.when(is_row & is_col)
        def _():
            for i in range(4):
                dia_copy(k, i).wait_send()

        @pl.when(passes(k))
        def _():
            dia_pass(k).wait_send()
        return carry
    lax.fori_loop(0, ROUNDS, drain, 0)


def solution(mesh):
    spec = P(('parts', 'row', 'sub'), None, 'col')
    tile = (8, 128)
    dma = pltpu.SemaphoreType.DMA

    def local_run(local_dist):
        return pl.pallas_call(
            kernel,
            out_shape=jax.ShapeDtypeStruct(local_dist.shape, local_dist.dtype),
            in_specs=[pl.BlockSpec(memory_space=pltpu.HBM)],
            out_specs=pl.BlockSpec(memory_space=pltpu.VMEM),
            scratch_shapes=[
                pltpu.VMEM(local_dist.shape, jnp.float32), dma(()),
                pltpu.VMEM((2, 4, 2, 8) + tile, jnp.float32),
                pltpu.VMEM((ROUNDS + 1, 4, 2, 8) + tile, jnp.float32),
                pltpu.VMEM((ROUNDS + 1, 2, 2, 8) + tile, jnp.float32),
                pltpu.VMEM((ROUNDS, 2, 8) + tile, jnp.float32),
                pltpu.VMEM((2, BLK, 2) + tile, jnp.float32),
                pltpu.VMEM((4, 16, 8) + tile, jnp.float32),
                pltpu.VMEM((16, 8) + tile, jnp.float32),
                pltpu.VMEM((2, 8) + tile, jnp.float32),
                dma((ROUNDS, 4, 3)), dma((ROUNDS, 4)),
                dma((ROUNDS, 2)), dma((ROUNDS, 2)),
                dma((ROUNDS, 4)), dma((ROUNDS,)), dma((ROUNDS,)),
            ],
            compiler_params=pltpu.CompilerParams(collective_id=0, has_side_effects=True, vmem_limit_bytes=55839744),
            name='apsp',
        )(local_dist)

    return jax.shard_map(local_run, mesh=mesh, in_specs=(spec,), out_specs=spec, check_vma=False)
```

```python
import functools

import jax
import jax.numpy as jnp
from jax import lax
from jax.experimental import pallas as pl
from jax.experimental.pallas import tpu as pltpu
from jax.sharding import PartitionSpec as P

MESH = pl.DeviceIdType.MESH
BLK = 128
ROUNDS = 8
HEAD_STEP, TAIL_STEP = 128, 64
ROW_PEERS = ((0, 1), (1, 1), (1, 0))
ALL_PEERS = ((1, 0, 1), (1, 1, 1), (0, 0, 1), (0, 1, 1), (1, 0, 0), (0, 1, 0), (1, 1, 0))


def lanes(tiles, idx):
    flat = tiles.reshape(-1, 128)
    idx = jnp.broadcast_to(idx, tiles.shape).reshape(-1, 128)
    return jnp.take_along_axis(flat, idx, axis=1, mode='promise_in_bounds').reshape(tiles.shape)


def kernel(src_ref, out_ref, in_ref, in_sem, mat, rowp, colp, dst, cb, brep, brepd, cpr,

           row_send, row_recv, col_send, col_recv, dia_send, dia_fwd, dia_recv):
    row, sub, col = lax.axis_index('row'), lax.axis_index('sub'), lax.axis_index('col')
    my_row = row * 2 + sub
    lane = lax.broadcasted_iota(jnp.int32, (8, 128), 1)
    in_grp = lane & 15
    grp_base = lane - in_grp
    nth_pivot = lax.broadcasted_iota(jnp.int32, (8, 8, 128), 0)

    def peer(d_col, d_row, d_sub):
        return {'col': (col + d_col) % 2, 'row': (row + d_row) % 2, 'sub': (sub + d_sub) % 2}

    barrier = pltpu.get_barrier_semaphore()
    for offs in ALL_PEERS:
        pl.semaphore_signal(barrier, inc=1, device_id=peer(*offs), device_id_type=MESH)
    fetch = pltpu.make_async_copy(src_ref, in_ref, in_sem)
    fetch.start()

    def swap_chunks(tiles):
        for bit in (1, 2, 4):
            mask = (lane & (16 * bit)) == 0
            pairs = tiles.reshape(8 // (2 * bit), 2, bit, 8, 128)
            lo, hi = pairs[:, 0].reshape(-1, 128), pairs[:, 1].reshape(-1, 128)
            lo_up = pltpu.roll(lo, 128 - 16 * bit, 1)
            hi_up = pltpu.roll(hi, 16 * bit, 1)
            lo, hi, lo_up, hi_up = (v.reshape(8 // (2 * bit), bit, 8, 128) for v in (lo, hi, lo_up, hi_up))
            tiles = jnp.stack([jnp.where(mask, lo, hi_up), jnp.where(mask, lo_up, hi)], axis=1).reshape(8, 8, 128)
        return tiles

    def row_copy(rnd, x, i):
        d_row, d_sub = ROW_PEERS[i]
        return pltpu.make_async_remote_copy(
            src_ref=rowp.at[rnd, x], dst_ref=rowp.at[rnd, x],
            send_sem=row_send.at[rnd, x, i], recv_sem=row_recv.at[rnd, x],
            device_id=peer(0, d_row, d_sub), device_id_type=MESH)

    def col_copy(rnd, a):
        return pltpu.make_async_remote_copy(
            src_ref=colp.at[rnd, a], dst_ref=colp.at[rnd, a],
            send_sem=col_send.at[rnd, a], recv_sem=col_recv.at[rnd, a],
            device_id=peer(1, 0, 0), device_id_type=MESH)

    def dia_copy(rnd, i):
        turn = rnd % 2
        offs = ((1, turn, 1), (1, 1 - turn, 1), (0, 1, 1), (0, 0, 1))[i]
        return pltpu.make_async_remote_copy(
            src_ref=dst.at[rnd], dst_ref=dst.at[rnd],
            send_sem=dia_send.at[rnd, i], recv_sem=dia_recv.at[rnd],
            device_id=peer(*offs), device_id_type=MESH)

    def dia_pass(rnd):
        return pltpu.make_async_remote_copy(
            src_ref=dst.at[rnd], dst_ref=dst.at[rnd],
            send_sem=dia_fwd.at[rnd], recv_sem=dia_recv.at[rnd],
            device_id=peer(0, 0, 1), device_id_type=MESH)

    def passes(rnd):
        return (sub != rnd % 2) & ((col != rnd % 2) | (row != (rnd % 4) // 2))

    def send_row(rnd, x):
        for i in range(3):
            row_copy(rnd, x, i).start()

    def send_dia(rnd):
        for i in range(4):
            dia_copy(rnd, i).start()

    def close(rnd, a, x):
        dst[rnd] = mat[a, x]

        def group(g, carry):
            rg, cg = lax.div(g, 8), lax.div(g, 2)
            q, half = lax.rem(g, 8), lax.rem(g, 2) * 8
            ucol = lanes(jnp.broadcast_to(dst[rnd, rg, cg][None], (8, 8, 128)), nth_pivot + (16 * q + half))
            rows = lanes(dst[rnd, rg], in_grp[None] + 16 * q)
            left = lanes(jnp.broadcast_to(dst[rnd, :, cg][None], (8, 2, 8, 128)),
                         (nth_pivot + (grp_base + half)[None])[:, None])
            for p in range(8):
                rows = jnp.minimum(rows, ucol[0][None] + rows[:, p:p + 1, :])
                if p < 7:
                    ucol = jnp.minimum(ucol[1:], ucol[0][None] + ucol[1:, p:p + 1, :])
            block = dst[rnd]
            for p in range(8):
                block = jnp.minimum(block, left[p][:, None] + rows[:, p:p + 1, :][None])
            dst[rnd] = block
            return carry

        def groups(i, carry):
            return lax.fori_loop(0, 4, lambda u, c: group(i * 4 + u, c), carry, unroll=True)
        lax.fori_loop(0, 4, groups, 0)

    def make_brep(src, out):
        def one(i, carry):
            out[i] = lanes(src[lax.div(i, 8)], in_grp + 16 * lax.rem(i, 8))
            return carry
        lax.fori_loop(0, 16, one, 0, unroll=True)

    def product(acc, left, right, step):
        def chunk(i, acc):
            def pivot(u, acc):
                b = right[i * (step // 8) + lax.div(u, 8), :, pl.ds(lax.rem(u, 8), 1), :]
                return jnp.minimum(acc, left(i * (step // 16) + lax.div(u, 16), i * step + u, lax.rem(u, 16))[:, None] + b[None])
            return lax.fori_loop(0, step, pivot, acc, unroll=True)
        return lax.fori_loop(0, BLK // step, chunk, acc, unroll=step == BLK)

    def close_and_send(rnd, a, x):
        close(rnd, a, x)
        send_dia(rnd)

    slot_r = jnp.where(my_row == 0, 0, ROUNDS)
    slot_c = jnp.where(col == 0, 0, ROUNDS)
    def unpack(a, x):
        for r in range(2):
            tiles = swap_chunks(in_ref[a, 64 * r:64 * r + 64, BLK * x:BLK * x + BLK].reshape(8, 8, 128))
            mat[a, x, r] = tiles
            if a == 0:
                rowp[slot_r, x, r] = tiles
            if x == 0:
                colp[slot_c, a, r] = tiles

    fetch.wait()
    unpack(0, 0)

    @pl.when((my_row == 0) & (col == 0))
    def _():
        close(0, 0, 0)
        pl.semaphore_wait(barrier, 7)
        send_dia(0)
    for a in range(2):
        for x in range(4):
            if a + x:
                unpack(a, x)

    @pl.when((my_row != 0) | (col != 0))
    def _():
        pl.semaphore_wait(barrier, 7)

    @pl.when(my_row == 0)
    def _():
        for x in (1, 2, 3):
            send_row(0, x)

        @pl.when(col != 0)
        def _():
            send_row(0, 0)

    @pl.when(col == 0)
    def _():
        @pl.when(my_row != 0)
        def _():
            col_copy(0, 0).start()
        col_copy(0, 1).start()

    def drain(k):
        is_row, is_col = my_row == k % 4, col == k % 2
        for x in range(4):
            @pl.when(is_row & (~is_col | (x != k // 2)))
            def _():
                for i in range(3):
                    row_copy(k, x, i).wait_send()
        for a in range(2):
            @pl.when(is_col & (~is_row | (a != k // 4)))
            def _():
                col_copy(k, a).wait_send()

        @pl.when(is_row & is_col)
        def _():
            for i in range(4):
                dia_copy(k, i).wait_send()

        @pl.when(passes(k))
        def _():
            dia_pass(k).wait_send()

    def one_round(k, carry):
        n = k + 1
        more = n < ROUNDS
        own_row = (my_row == n % 4) & more
        own_col = (col == n % 2) & more
        a1 = jnp.minimum(n // 4, 1)
        x1 = ((n + jnp.where(col == n % 2, 0, 1)) // 2) % 4
        xk = k // 2
        is_row, is_col = my_row == k % 4, col == k % 2

        def first_rows():
            @pl.when(~is_row)
            def _():
                row_copy(k, x1, 0).wait_recv()
            make_brep(rowp.at[k, x1], brep.at[x1])

        @pl.when(~is_col)
        def _():
            first_rows()

        @pl.when(k > 0)
        def _():
            drain(k - 1)

        @pl.when(~is_row | ~is_col)
        def _():
            dia_copy(k, 0).wait_recv()

        @pl.when(passes(k))
        def _():
            dia_pass(k).start()

        def wait_row(x):
            @pl.when(~is_row)
            def _():
                row_copy(k, x, 0).wait_recv()

        make_brep(dst.at[k], brepd)

        def head(h, carry):
            a = jnp.where(h == 0, a1, 1 - a1)

            on_diag = is_row & (a == k // 4)
            send_it = own_row & (h == 0)

            @pl.when(~is_col & ~on_diag)
            def _():
                col_copy(k, a).wait_recv()

            @pl.when(on_diag)
            def _():
                cpr[...] = dst[k]

            @pl.when(~on_diag)
            def _():
                pan = colp.at[k, a]
                cpr[...] = product(pan[...], lambda c, p, l: lanes(pan[:, c], grp_base + l), brepd, HEAD_STEP)

            @pl.when(is_col)
            def _():
                mat[a, xk] = cpr[...]

                @pl.when(h == 0)
                def _():
                    first_rows()

            @pl.when(is_col & send_it)
            def _():
                rowp[n, xk] = cpr[...]
                send_row(n, xk)

            tab = cb.at[a]

            def fly(c, p, l):
                avs = lanes(cpr[:, c], grp_base + l)
                tab[p] = avs
                return avs
            acc = product(mat[a, x1], fly, brep.at[x1], HEAD_STEP)
            mat[a, x1] = acc
            rowp[jnp.where(send_it, n, ROUNDS), x1] = acc
            colp[jnp.where(own_col, n, ROUNDS), a] = acc

            @pl.when(send_it & ~own_col)
            def _():
                send_row(n, x1)

            @pl.when(own_col & ~send_it)
            def _():
                col_copy(n, a).start()

            @pl.when(send_it & own_col)
            def _():
                close_and_send(n, a, x1)
            return carry

        def tail(phase, t, carry):
            h = t // 3
            a = jnp.where(h == 0, a1, 1 - a1)
            x = (x1 + 1 + t % 3) % 4

            @pl.when(((col != k % 2) | (t % 3 != 2)) & ((own_row & (h == phase)) | (~own_row & (phase == 1))))
            def _():
                @pl.when(h == 0)
                def _():
                    wait_row(x)
                    make_brep(rowp.at[k, x], brep.at[x])

                tab = cb.at[a]
                acc = product(mat[a, x], lambda c, p, l: tab[p], brep.at[x], TAIL_STEP)
                mat[a, x] = acc
                send_it = own_row & (h == 0)
                rowp[jnp.where(send_it, n, ROUNDS), x] = acc

                @pl.when(send_it)
                def _():
                    send_row(n, x)
            return carry
        def in_order(phase, carry):
            head(phase, carry)
            return lax.fori_loop(0, 6, functools.partial(tail, phase), carry)
        lax.fori_loop(0, 2, in_order, 0)
        return carry
    lax.fori_loop(0, ROUNDS, one_round, 0)

    for a in range(2):
        for x in range(4):
            for r in range(2):
                tiles = swap_chunks(mat[a, x, r])
                out_ref[a, 64 * r:64 * r + 64, BLK * x:BLK * x + BLK] = tiles.reshape(64, 128)

    drain(ROUNDS - 1)


def solution(mesh):
    spec = P(('parts', 'row', 'sub'), None, 'col')
    tile = (8, 128)
    dma = pltpu.SemaphoreType.DMA

    def local_run(local_dist):
        return pl.pallas_call(
            kernel,
            out_shape=jax.ShapeDtypeStruct(local_dist.shape, local_dist.dtype),
            in_specs=[pl.BlockSpec(memory_space=pltpu.HBM)],
            out_specs=pl.BlockSpec(memory_space=pltpu.VMEM),
            scratch_shapes=[
                pltpu.VMEM(local_dist.shape, jnp.float32), dma(()),
                pltpu.VMEM((2, 4, 2, 8) + tile, jnp.float32),
                pltpu.VMEM((ROUNDS + 1, 4, 2, 8) + tile, jnp.float32),
                pltpu.VMEM((ROUNDS + 1, 2, 2, 8) + tile, jnp.float32),
                pltpu.VMEM((ROUNDS, 2, 8) + tile, jnp.float32),
                pltpu.VMEM((2, BLK, 2) + tile, jnp.float32),
                pltpu.VMEM((4, 16, 8) + tile, jnp.float32),
                pltpu.VMEM((16, 8) + tile, jnp.float32),
                pltpu.VMEM((2, 8) + tile, jnp.float32),
                dma((ROUNDS, 4, 3)), dma((ROUNDS, 4)),
                dma((ROUNDS, 2)), dma((ROUNDS, 2)),
                dma((ROUNDS, 4)), dma((ROUNDS,)), dma((ROUNDS,)),
            ],
            compiler_params=pltpu.CompilerParams(collective_id=0, has_side_effects=True, vmem_limit_bytes=55839744),
            name='apsp',
        )(local_dist)

    return jax.shard_map(local_run, mesh=mesh, in_specs=(spec,), out_specs=spec, check_vma=False)
```

```python
import functools

import jax
import jax.numpy as jnp
from jax import lax
from jax.experimental import pallas as pl
from jax.experimental.pallas import tpu as pltpu
from jax.sharding import PartitionSpec as P

MESH = pl.DeviceIdType.MESH
BLK = 128
ROUNDS = 8
HEAD_STEP, TAIL_STEP = 128, 64
ROW_PEERS = ((0, 1), (1, 1), (1, 0))
ALL_PEERS = ((1, 0, 1), (1, 1, 1), (0, 0, 1), (0, 1, 1), (1, 0, 0), (0, 1, 0), (1, 1, 0))


def lanes(tiles, idx):
    flat = tiles.reshape(-1, 128)
    idx = jnp.broadcast_to(idx, tiles.shape).reshape(-1, 128)
    return jnp.take_along_axis(flat, idx, axis=1, mode='promise_in_bounds').reshape(tiles.shape)


def kernel(src_ref, out_ref, in_ref, in_sem, mat, rowp, colp, dst, cb, brep, brepd, cpr,

           row_send, row_recv, col_send, col_recv, dia_send, dia_fwd, dia_recv):
    row, sub, col = lax.axis_index('row'), lax.axis_index('sub'), lax.axis_index('col')
    my_row = row * 2 + sub
    lane = lax.broadcasted_iota(jnp.int32, (8, 128), 1)
    in_grp = lane & 15
    grp_base = lane - in_grp
    nth_pivot = lax.broadcasted_iota(jnp.int32, (8, 8, 128), 0)

    def peer(d_col, d_row, d_sub):
        return {'col': (col + d_col) % 2, 'row': (row + d_row) % 2, 'sub': (sub + d_sub) % 2}

    barrier = pltpu.get_barrier_semaphore()
    for offs in ALL_PEERS:
        pl.semaphore_signal(barrier, inc=1, device_id=peer(*offs), device_id_type=MESH)
    fetch = pltpu.make_async_copy(src_ref, in_ref, in_sem)
    fetch.start()

    def swap_chunks(tiles):
        for bit in (1, 2, 4):
            mask = (lane & (16 * bit)) == 0
            pairs = tiles.reshape(8 // (2 * bit), 2, bit, 8, 128)
            lo, hi = pairs[:, 0].reshape(-1, 128), pairs[:, 1].reshape(-1, 128)
            lo_up = pltpu.roll(lo, 128 - 16 * bit, 1)
            hi_up = pltpu.roll(hi, 16 * bit, 1)
            lo, hi, lo_up, hi_up = (v.reshape(8 // (2 * bit), bit, 8, 128) for v in (lo, hi, lo_up, hi_up))
            tiles = jnp.stack([jnp.where(mask, lo, hi_up), jnp.where(mask, lo_up, hi)], axis=1).reshape(8, 8, 128)
        return tiles

    def row_copy(rnd, x, i):
        d_row, d_sub = ROW_PEERS[i]
        return pltpu.make_async_remote_copy(
            src_ref=rowp.at[rnd, x], dst_ref=rowp.at[rnd, x],
            send_sem=row_send.at[rnd, x, i], recv_sem=row_recv.at[rnd, x],
            device_id=peer(0, d_row, d_sub), device_id_type=MESH)

    def col_copy(rnd, a):
        return pltpu.make_async_remote_copy(
            src_ref=colp.at[rnd, a], dst_ref=colp.at[rnd, a],
            send_sem=col_send.at[rnd, a], recv_sem=col_recv.at[rnd, a],
            device_id=peer(1, 0, 0), device_id_type=MESH)

    def dia_copy(rnd, i):
        turn = rnd % 2
        offs = ((1, turn, 1), (1, 1 - turn, 1), (0, 1, 1), (0, 0, 1))[i]
        return pltpu.make_async_remote_copy(
            src_ref=dst.at[rnd], dst_ref=dst.at[rnd],
            send_sem=dia_send.at[rnd, i], recv_sem=dia_recv.at[rnd],
            device_id=peer(*offs), device_id_type=MESH)

    def dia_pass(rnd):
        return pltpu.make_async_remote_copy(
            src_ref=dst.at[rnd], dst_ref=dst.at[rnd],
            send_sem=dia_fwd.at[rnd], recv_sem=dia_recv.at[rnd],
            device_id=peer(0, 0, 1), device_id_type=MESH)

    def passes(rnd):
        return (sub != rnd % 2) & ((col != rnd % 2) | (row != (rnd % 4) // 2))

    def send_row(rnd, x):
        for i in range(3):
            row_copy(rnd, x, i).start()

    def send_dia(rnd):
        for i in range(4):
            dia_copy(rnd, i).start()

    def close(rnd, a, x):
        dst[rnd] = mat[a, x]

        def group(g, carry):
            rg, cg = lax.div(g, 8), lax.div(g, 2)
            q, half = lax.rem(g, 8), lax.rem(g, 2) * 8
            ucol = lanes(jnp.broadcast_to(dst[rnd, rg, cg][None], (8, 8, 128)), nth_pivot + (16 * q + half))
            rows = lanes(dst[rnd, rg], in_grp[None] + 16 * q)
            left = lanes(jnp.broadcast_to(dst[rnd, :, cg][None], (8, 2, 8, 128)),
                         (nth_pivot + (grp_base + half)[None])[:, None])
            for p in range(8):
                rows = jnp.minimum(rows, ucol[0][None] + rows[:, p:p + 1, :])
                if p < 7:
                    ucol = jnp.minimum(ucol[1:], ucol[0][None] + ucol[1:, p:p + 1, :])
            block = dst[rnd]
            for p in range(8):
                block = jnp.minimum(block, left[p][:, None] + rows[:, p:p + 1, :][None])
            dst[rnd] = block
            return carry

        def groups(i, carry):
            return lax.fori_loop(0, 4, lambda u, c: group(i * 4 + u, c), carry, unroll=True)
        lax.fori_loop(0, 4, groups, 0)

    def make_brep(src, out):
        def one(i, carry):
            out[i] = lanes(src[lax.div(i, 8)], in_grp + 16 * lax.rem(i, 8))
            return carry
        lax.fori_loop(0, 16, one, 0, unroll=True)

    def product(acc, left, right, step):
        def chunk(i, acc):
            def pivot(u, acc):
                b = right[i * (step // 8) + lax.div(u, 8), :, pl.ds(lax.rem(u, 8), 1), :]
                return jnp.minimum(acc, left(i * (step // 16) + lax.div(u, 16), i * step + u, lax.rem(u, 16))[:, None] + b[None])
            return lax.fori_loop(0, step, pivot, acc, unroll=True)
        return lax.fori_loop(0, BLK // step, chunk, acc, unroll=step == BLK)

    def product_spreading(acc, tab, src, out):
        def half(r, acc):
            def group(q, acc):
                g = 8 * r + q
                out[g] = lanes(src[r], in_grp + 16 * q)
                for s in range(8):
                    acc = jnp.minimum(acc, tab[8 * g + s][:, None] + out[g, :, s:s + 1, :][None])
                return acc
            return lax.fori_loop(0, 8, group, acc, unroll=True)
        return lax.fori_loop(0, 2, half, acc)

    def close_and_send(rnd, a, x):
        close(rnd, a, x)
        send_dia(rnd)

    slot_r = jnp.where(my_row == 0, 0, ROUNDS)
    slot_c = jnp.where(col == 0, 0, ROUNDS)
    def unpack(a, x):
        for r in range(2):
            tiles = swap_chunks(in_ref[a, 64 * r:64 * r + 64, BLK * x:BLK * x + BLK].reshape(8, 8, 128))
            mat[a, x, r] = tiles
            if a == 0:
                rowp[slot_r, x, r] = tiles
            if x == 0:
                colp[slot_c, a, r] = tiles

    fetch.wait()
    unpack(0, 0)

    @pl.when((my_row == 0) & (col == 0))
    def _():
        close(0, 0, 0)
        pl.semaphore_wait(barrier, 7)
        send_dia(0)
    for a in range(2):
        for x in range(4):
            if a + x:
                unpack(a, x)

    @pl.when((my_row != 0) | (col != 0))
    def _():
        pl.semaphore_wait(barrier, 7)

    @pl.when(my_row == 0)
    def _():
        for x in (1, 2, 3):
            send_row(0, x)

        @pl.when(col != 0)
        def _():
            send_row(0, 0)

    @pl.when(col == 0)
    def _():
        @pl.when(my_row != 0)
        def _():
            col_copy(0, 0).start()
        col_copy(0, 1).start()

    def drain(k):
        is_row, is_col = my_row == k % 4, col == k % 2
        for x in range(4):
            @pl.when(is_row & (~is_col | (x != k // 2)))
            def _():
                for i in range(3):
                    row_copy(k, x, i).wait_send()
        for a in range(2):
            @pl.when(is_col & (~is_row | (a != k // 4)))
            def _():
                col_copy(k, a).wait_send()

        @pl.when(is_row & is_col)
        def _():
            for i in range(4):
                dia_copy(k, i).wait_send()

        @pl.when(passes(k))
        def _():
            dia_pass(k).wait_send()

    def one_round(k, carry):
        n = k + 1
        more = n < ROUNDS
        own_row = (my_row == n % 4) & more
        own_col = (col == n % 2) & more
        a1 = jnp.minimum(n // 4, 1)
        x1 = ((n + jnp.where(col == n % 2, 0, 1)) // 2) % 4
        xk = k // 2
        is_row, is_col = my_row == k % 4, col == k % 2

        def first_rows():
            @pl.when(~is_row)
            def _():
                row_copy(k, x1, 0).wait_recv()
            make_brep(rowp.at[k, x1], brep.at[x1])

        @pl.when(~is_col)
        def _():
            first_rows()

        @pl.when(k > 0)
        def _():
            drain(k - 1)

        @pl.when(~is_row | ~is_col)
        def _():
            dia_copy(k, 0).wait_recv()

        @pl.when(passes(k))
        def _():
            dia_pass(k).start()

        def wait_row(x):
            @pl.when(~is_row)
            def _():
                row_copy(k, x, 0).wait_recv()

        make_brep(dst.at[k], brepd)

        def head(h, carry):
            a = jnp.where(h == 0, a1, 1 - a1)

            on_diag = is_row & (a == k // 4)
            send_it = own_row & (h == 0)

            @pl.when(~is_col & ~on_diag)
            def _():
                col_copy(k, a).wait_recv()

            @pl.when(on_diag)
            def _():
                cpr[...] = dst[k]

            @pl.when(~on_diag)
            def _():
                pan = colp.at[k, a]
                cpr[...] = product(pan[...], lambda c, p, l: lanes(pan[:, c], grp_base + l), brepd, HEAD_STEP)

            @pl.when(is_col)
            def _():
                mat[a, xk] = cpr[...]

                @pl.when(h == 0)
                def _():
                    first_rows()

            @pl.when(is_col & send_it)
            def _():
                rowp[n, xk] = cpr[...]
                send_row(n, xk)

            tab = cb.at[a]

            def fly(c, p, l):
                avs = lanes(cpr[:, c], grp_base + l)
                tab[p] = avs
                return avs
            acc = product(mat[a, x1], fly, brep.at[x1], HEAD_STEP)
            mat[a, x1] = acc
            rowp[jnp.where(send_it, n, ROUNDS), x1] = acc
            colp[jnp.where(own_col, n, ROUNDS), a] = acc

            @pl.when(send_it & ~own_col)
            def _():
                send_row(n, x1)

            @pl.when(own_col & ~send_it)
            def _():
                col_copy(n, a).start()

            @pl.when(send_it & own_col)
            def _():
                close_and_send(n, a, x1)
            return carry

        def tail(phase, t, carry):
            h = t // 3
            a = jnp.where(h == 0, a1, 1 - a1)
            x = (x1 + 1 + t % 3) % 4

            @pl.when(((col != k % 2) | (t % 3 != 2)) & ((own_row & (h == phase)) | (~own_row & (phase == 1))))
            def _():
                tab = cb.at[a]

                @pl.when(h == 0)
                def _():
                    wait_row(x)
                    mat[a, x] = product_spreading(mat[a, x], tab, rowp.at[k, x], brep.at[x])

                @pl.when(h == 1)
                def _():
                    mat[a, x] = product(mat[a, x], lambda c, p, l: tab[p], brep.at[x], TAIL_STEP)

                @pl.when(own_row & (h == 0))
                def _():
                    rowp[n, x] = mat[a, x]
                    send_row(n, x)
            return carry
        def in_order(phase, carry):
            head(phase, carry)
            return lax.fori_loop(0, 6, functools.partial(tail, phase), carry)
        lax.fori_loop(0, 2, in_order, 0)
        return carry
    lax.fori_loop(0, ROUNDS, one_round, 0)

    for a in range(2):
        for x in range(4):
            for r in range(2):
                tiles = swap_chunks(mat[a, x, r])
                out_ref[a, 64 * r:64 * r + 64, BLK * x:BLK * x + BLK] = tiles.reshape(64, 128)

    drain(ROUNDS - 1)


def solution(mesh):
    spec = P(('parts', 'row', 'sub'), None, 'col')
    tile = (8, 128)
    dma = pltpu.SemaphoreType.DMA

    def local_run(local_dist):
        return pl.pallas_call(
            kernel,
            out_shape=jax.ShapeDtypeStruct(local_dist.shape, local_dist.dtype),
            in_specs=[pl.BlockSpec(memory_space=pltpu.HBM)],
            out_specs=pl.BlockSpec(memory_space=pltpu.VMEM),
            scratch_shapes=[
                pltpu.VMEM(local_dist.shape, jnp.float32), dma(()),
                pltpu.VMEM((2, 4, 2, 8) + tile, jnp.float32),
                pltpu.VMEM((ROUNDS + 1, 4, 2, 8) + tile, jnp.float32),
                pltpu.VMEM((ROUNDS + 1, 2, 2, 8) + tile, jnp.float32),
                pltpu.VMEM((ROUNDS, 2, 8) + tile, jnp.float32),
                pltpu.VMEM((2, BLK, 2) + tile, jnp.float32),
                pltpu.VMEM((4, 16, 8) + tile, jnp.float32),
                pltpu.VMEM((16, 8) + tile, jnp.float32),
                pltpu.VMEM((2, 8) + tile, jnp.float32),
                dma((ROUNDS, 4, 3)), dma((ROUNDS, 4)),
                dma((ROUNDS, 2)), dma((ROUNDS, 2)),
                dma((ROUNDS, 4)), dma((ROUNDS,)), dma((ROUNDS,)),
            ],
            compiler_params=pltpu.CompilerParams(collective_id=0, has_side_effects=True, vmem_limit_bytes=55839744),
            name='apsp',
        )(local_dist)

    return jax.shard_map(local_run, mesh=mesh, in_specs=(spec,), out_specs=spec, check_vma=False)
```

```python
import functools

import jax
import jax.numpy as jnp
from jax import lax
from jax.experimental import pallas as pl
from jax.experimental.pallas import tpu as pltpu
from jax.sharding import PartitionSpec as P

MESH = pl.DeviceIdType.MESH
BLK = 128
ROUNDS = 8
HEAD_STEP, TAIL_STEP = 128, 64
ROW_PEERS = ((0, 1), (1, 1), (1, 0))
ALL_PEERS = ((1, 0, 1), (1, 1, 1), (0, 0, 1), (0, 1, 1), (1, 0, 0), (0, 1, 0), (1, 1, 0))


def lanes(tiles, idx):
    flat = tiles.reshape(-1, 128)
    idx = jnp.broadcast_to(idx, tiles.shape).reshape(-1, 128)
    return jnp.take_along_axis(flat, idx, axis=1, mode='promise_in_bounds').reshape(tiles.shape)


def kernel(src_ref, out_ref, in_ref, in_sem, mat, rowp, colp, dst, cb, brep, brepd, cpr,

           row_send, row_recv, col_send, col_recv, dia_send, dia_fwd, dia_recv):
    row, sub, col = lax.axis_index('row'), lax.axis_index('sub'), lax.axis_index('col')
    my_row = row * 2 + sub
    lane = lax.broadcasted_iota(jnp.int32, (8, 128), 1)
    in_grp = lane & 15
    grp_base = lane - in_grp
    nth_pivot = lax.broadcasted_iota(jnp.int32, (8, 8, 128), 0)

    def peer(d_col, d_row, d_sub):
        return {'col': (col + d_col) % 2, 'row': (row + d_row) % 2, 'sub': (sub + d_sub) % 2}

    barrier = pltpu.get_barrier_semaphore()
    for offs in ALL_PEERS:
        pl.semaphore_signal(barrier, inc=1, device_id=peer(*offs), device_id_type=MESH)
    fetch = pltpu.make_async_copy(src_ref, in_ref, in_sem)
    fetch.start()

    def swap_chunks(tiles):
        for bit in (1, 2, 4):
            mask = (lane & (16 * bit)) == 0
            pairs = tiles.reshape(8 // (2 * bit), 2, bit, 8, 128)
            lo, hi = pairs[:, 0].reshape(-1, 128), pairs[:, 1].reshape(-1, 128)
            lo_up = pltpu.roll(lo, 128 - 16 * bit, 1)
            hi_up = pltpu.roll(hi, 16 * bit, 1)
            lo, hi, lo_up, hi_up = (v.reshape(8 // (2 * bit), bit, 8, 128) for v in (lo, hi, lo_up, hi_up))
            tiles = jnp.stack([jnp.where(mask, lo, hi_up), jnp.where(mask, lo_up, hi)], axis=1).reshape(8, 8, 128)
        return tiles

    def row_copy(rnd, x, i):
        d_row, d_sub = ROW_PEERS[i]
        return pltpu.make_async_remote_copy(
            src_ref=rowp.at[rnd, x], dst_ref=rowp.at[rnd, x],
            send_sem=row_send.at[rnd, x, i], recv_sem=row_recv.at[rnd, x],
            device_id=peer(0, d_row, d_sub), device_id_type=MESH)

    def col_copy(rnd, a):
        return pltpu.make_async_remote_copy(
            src_ref=colp.at[rnd, a], dst_ref=colp.at[rnd, a],
            send_sem=col_send.at[rnd, a], recv_sem=col_recv.at[rnd, a],
            device_id=peer(1, 0, 0), device_id_type=MESH)

    def dia_copy(rnd, i):
        turn = rnd % 2
        offs = ((1, turn, 1), (1, 1 - turn, 1), (0, 1, 1), (0, 0, 1))[i]
        return pltpu.make_async_remote_copy(
            src_ref=dst.at[rnd], dst_ref=dst.at[rnd],
            send_sem=dia_send.at[rnd, i], recv_sem=dia_recv.at[rnd],
            device_id=peer(*offs), device_id_type=MESH)

    def dia_pass(rnd):
        return pltpu.make_async_remote_copy(
            src_ref=dst.at[rnd], dst_ref=dst.at[rnd],
            send_sem=dia_fwd.at[rnd], recv_sem=dia_recv.at[rnd],
            device_id=peer(0, 0, 1), device_id_type=MESH)

    def passes(rnd):
        return (sub != rnd % 2) & ((col != rnd % 2) | (row != (rnd % 4) // 2))

    def send_row(rnd, x):
        for i in range(3):
            row_copy(rnd, x, i).start()

    def send_dia(rnd):
        for i in range(4):
            dia_copy(rnd, i).start()

    def close(rnd, a, x):
        dst[rnd] = mat[a, x]

        def group(g, carry):
            rg, cg = lax.div(g, 8), lax.div(g, 2)
            q, half = lax.rem(g, 8), lax.rem(g, 2) * 8
            ucol = lanes(jnp.broadcast_to(dst[rnd, rg, cg][None], (8, 8, 128)), nth_pivot + (16 * q + half))
            rows = lanes(dst[rnd, rg], in_grp[None] + 16 * q)
            left = lanes(jnp.broadcast_to(dst[rnd, :, cg][None], (8, 2, 8, 128)),
                         (nth_pivot + (grp_base + half)[None])[:, None])
            for p in range(8):
                rows = jnp.minimum(rows, ucol[0][None] + rows[:, p:p + 1, :])
                if p < 7:
                    ucol = jnp.minimum(ucol[1:], ucol[0][None] + ucol[1:, p:p + 1, :])
            block = dst[rnd]
            for p in range(8):
                block = jnp.minimum(block, left[p][:, None] + rows[:, p:p + 1, :][None])
            dst[rnd] = block
            return carry

        def groups(i, carry):
            return lax.fori_loop(0, 4, lambda u, c: group(i * 4 + u, c), carry, unroll=True)
        lax.fori_loop(0, 4, groups, 0)

    def make_brep(src, out):
        def one(i, carry):
            out[i] = lanes(src[lax.div(i, 8)], in_grp + 16 * lax.rem(i, 8))
            return carry
        lax.fori_loop(0, 16, one, 0, unroll=True)

    def product(acc, left, right, step):
        def chunk(i, acc):
            def pivot(u, acc):
                b = right[i * (step // 8) + lax.div(u, 8), :, pl.ds(lax.rem(u, 8), 1), :]
                return jnp.minimum(acc, left(i * (step // 16) + lax.div(u, 16), i * step + u, lax.rem(u, 16))[:, None] + b[None])
            return lax.fori_loop(0, step, pivot, acc, unroll=True)
        return lax.fori_loop(0, BLK // step, chunk, acc, unroll=step == BLK)

    def product_spreading(acc, tab, src, out):
        def half(r, acc):
            def group(q, acc):
                g = 8 * r + q
                out[g] = lanes(src[r], in_grp + 16 * q)
                for s in range(8):
                    acc = jnp.minimum(acc, tab[8 * g + s][:, None] + out[g, :, s:s + 1, :][None])
                return acc
            return lax.fori_loop(0, 8, group, acc, unroll=True)
        return lax.fori_loop(0, 2, half, acc)

    def close_and_send(rnd, a, x):
        close(rnd, a, x)
        send_dia(rnd)

    slot_r = jnp.where(my_row == 0, 0, ROUNDS)
    slot_c = jnp.where(col == 0, 0, ROUNDS)
    def unpack(a, x):
        for r in range(2):
            tiles = swap_chunks(in_ref[a, 64 * r:64 * r + 64, BLK * x:BLK * x + BLK].reshape(8, 8, 128))
            mat[a, x, r] = tiles
            if a == 0:
                rowp[slot_r, x, r] = tiles
            if x == 0:
                colp[slot_c, a, r] = tiles

    fetch.wait()
    unpack(0, 0)

    @pl.when((my_row == 0) & (col == 0))
    def _():
        close(0, 0, 0)
        pl.semaphore_wait(barrier, 7)
        send_dia(0)
    for a in range(2):
        for x in range(4):
            if a + x:
                unpack(a, x)

    @pl.when((my_row != 0) | (col != 0))
    def _():
        pl.semaphore_wait(barrier, 7)

    @pl.when(my_row == 0)
    def _():
        @pl.when(col != 0)
        def _():
            send_row(0, 0)
        for x in (1, 2, 3):
            send_row(0, x)

    @pl.when(col == 0)
    def _():
        @pl.when(my_row != 0)
        def _():
            col_copy(0, 0).start()
        col_copy(0, 1).start()

    def drain(k):
        is_row, is_col = my_row == k % 4, col == k % 2
        for x in range(4):
            @pl.when(is_row & (~is_col | (x != k // 2)))
            def _():
                for i in range(3):
                    row_copy(k, x, i).wait_send()
        for a in range(2):
            @pl.when(is_col & (~is_row | (a != k // 4)))
            def _():
                col_copy(k, a).wait_send()

        @pl.when(is_row & is_col)
        def _():
            for i in range(4):
                dia_copy(k, i).wait_send()

        @pl.when(passes(k))
        def _():
            dia_pass(k).wait_send()

    def one_round(k, carry):
        n = k + 1
        more = n < ROUNDS
        own_row = (my_row == n % 4) & more
        own_col = (col == n % 2) & more
        a1 = jnp.minimum(n // 4, 1)
        x1 = ((n + jnp.where(col == n % 2, 0, 1)) // 2) % 4
        xk = k // 2
        is_row, is_col = my_row == k % 4, col == k % 2

        def first_rows():
            @pl.when(~is_row)
            def _():
                row_copy(k, x1, 0).wait_recv()
            make_brep(rowp.at[k, x1], brep.at[x1])

        @pl.when(~is_col)
        def _():
            first_rows()

        @pl.when(k > 0)
        def _():
            drain(k - 1)

        @pl.when(~is_row | ~is_col)
        def _():
            dia_copy(k, 0).wait_recv()

        @pl.when(passes(k))
        def _():
            dia_pass(k).start()

        def wait_row(x):
            @pl.when(~is_row)
            def _():
                row_copy(k, x, 0).wait_recv()

        make_brep(dst.at[k], brepd)

        def head(h, carry):
            a = jnp.where(h == 0, a1, 1 - a1)

            on_diag = is_row & (a == k // 4)
            send_it = own_row & (h == 0)

            @pl.when(~is_col & ~on_diag)
            def _():
                col_copy(k, a).wait_recv()

            @pl.when(on_diag)
            def _():
                cpr[...] = dst[k]

            @pl.when(~on_diag)
            def _():
                pan = colp.at[k, a]
                cpr[...] = product(pan[...], lambda c, p, l: lanes(pan[:, c], grp_base + l), brepd, HEAD_STEP)

            @pl.when(is_col)
            def _():
                mat[a, xk] = cpr[...]

                @pl.when(h == 0)
                def _():
                    first_rows()

            @pl.when(is_col & send_it)
            def _():
                rowp[n, xk] = cpr[...]
                send_row(n, xk)

            tab = cb.at[a]

            def fly(c, p, l):
                avs = lanes(cpr[:, c], grp_base + l)
                tab[p] = avs
                return avs
            acc = product(mat[a, x1], fly, brep.at[x1], HEAD_STEP)
            mat[a, x1] = acc
            rowp[jnp.where(send_it, n, ROUNDS), x1] = acc
            colp[jnp.where(own_col, n, ROUNDS), a] = acc

            @pl.when(send_it & ~own_col)
            def _():
                send_row(n, x1)

            @pl.when(own_col & ~send_it)
            def _():
                col_copy(n, a).start()

            @pl.when(send_it & own_col)
            def _():
                close_and_send(n, a, x1)
            return carry

        def tail(phase, t, carry):
            h = t // 3
            a = jnp.where(h == 0, a1, 1 - a1)
            x = (x1 + 1 + t % 3) % 4

            @pl.when(((col != k % 2) | (t % 3 != 2)) & ((own_row & (h == phase)) | (~own_row & (phase == 1))))
            def _():
                tab = cb.at[a]

                @pl.when(h == 0)
                def _():
                    wait_row(x)
                    mat[a, x] = product_spreading(mat[a, x], tab, rowp.at[k, x], brep.at[x])

                @pl.when(h == 1)
                def _():
                    mat[a, x] = product(mat[a, x], lambda c, p, l: tab[p], brep.at[x], TAIL_STEP)

                @pl.when(own_row & (h == 0))
                def _():
                    rowp[n, x] = mat[a, x]
                    send_row(n, x)
            return carry
        def in_order(phase, carry):
            head(phase, carry)
            return lax.fori_loop(0, 6, functools.partial(tail, phase), carry)
        lax.fori_loop(0, 2, in_order, 0)
        return carry
    lax.fori_loop(0, ROUNDS, one_round, 0)

    for a in range(2):
        for x in range(4):
            for r in range(2):
                tiles = swap_chunks(mat[a, x, r])
                out_ref[a, 64 * r:64 * r + 64, BLK * x:BLK * x + BLK] = tiles.reshape(64, 128)

    drain(ROUNDS - 1)


def solution(mesh):
    spec = P(('parts', 'row', 'sub'), None, 'col')
    tile = (8, 128)
    dma = pltpu.SemaphoreType.DMA

    def local_run(local_dist):
        return pl.pallas_call(
            kernel,
            out_shape=jax.ShapeDtypeStruct(local_dist.shape, local_dist.dtype),
            in_specs=[pl.BlockSpec(memory_space=pltpu.HBM)],
            out_specs=pl.BlockSpec(memory_space=pltpu.VMEM),
            scratch_shapes=[
                pltpu.VMEM(local_dist.shape, jnp.float32), dma(()),
                pltpu.VMEM((2, 4, 2, 8) + tile, jnp.float32),
                pltpu.VMEM((ROUNDS + 1, 4, 2, 8) + tile, jnp.float32),
                pltpu.VMEM((ROUNDS + 1, 2, 2, 8) + tile, jnp.float32),
                pltpu.VMEM((ROUNDS, 2, 8) + tile, jnp.float32),
                pltpu.VMEM((2, BLK, 2) + tile, jnp.float32),
                pltpu.VMEM((4, 16, 8) + tile, jnp.float32),
                pltpu.VMEM((16, 8) + tile, jnp.float32),
                pltpu.VMEM((2, 8) + tile, jnp.float32),
                dma((ROUNDS, 4, 3)), dma((ROUNDS, 4)),
                dma((ROUNDS, 2)), dma((ROUNDS, 2)),
                dma((ROUNDS, 4)), dma((ROUNDS,)), dma((ROUNDS,)),
            ],
            compiler_params=pltpu.CompilerParams(collective_id=0, has_side_effects=True, vmem_limit_bytes=55839744),
            name='apsp',
        )(local_dist)

    return jax.shard_map(local_run, mesh=mesh, in_specs=(spec,), out_specs=spec, check_vma=False)
```

```python
import functools

import jax
import jax.numpy as jnp
from jax import lax
from jax.experimental import pallas as pl
from jax.experimental.pallas import tpu as pltpu
from jax.sharding import PartitionSpec as P

MESH = pl.DeviceIdType.MESH
BLK = 128
ROUNDS = 8
HEAD_STEP, TAIL_STEP = 128, 64
ROW_PEERS = ((0, 1), (1, 1), (1, 0))
ALL_PEERS = ((1, 0, 1), (1, 1, 1), (0, 0, 1), (0, 1, 1), (1, 0, 0), (0, 1, 0), (1, 1, 0))


def lanes(tiles, idx):
    flat = tiles.reshape(-1, 128)
    idx = jnp.broadcast_to(idx, tiles.shape).reshape(-1, 128)
    return jnp.take_along_axis(flat, idx, axis=1, mode='promise_in_bounds').reshape(tiles.shape)


def kernel(src_ref, out_ref, in_ref, in_sem, mat, rowp, colp, dst, cb, brep, brepd, cpr,

           row_send, row_recv, col_send, col_recv, dia_send, dia_fwd, dia_recv):
    row, sub, col = lax.axis_index('row'), lax.axis_index('sub'), lax.axis_index('col')
    my_row = row * 2 + sub
    lane = lax.broadcasted_iota(jnp.int32, (8, 128), 1)
    in_grp = lane & 15
    grp_base = lane - in_grp
    nth_pivot = lax.broadcasted_iota(jnp.int32, (8, 8, 128), 0)

    def peer(d_col, d_row, d_sub):
        return {'col': (col + d_col) % 2, 'row': (row + d_row) % 2, 'sub': (sub + d_sub) % 2}

    barrier = pltpu.get_barrier_semaphore()
    for offs in ALL_PEERS:
        pl.semaphore_signal(barrier, inc=1, device_id=peer(*offs), device_id_type=MESH)
    fetch = pltpu.make_async_copy(src_ref, in_ref, in_sem)
    fetch.start()

    def swap_chunks(tiles):
        for bit in (1, 2, 4):
            mask = (lane & (16 * bit)) == 0
            pairs = tiles.reshape(8 // (2 * bit), 2, bit, 8, 128)
            lo, hi = pairs[:, 0].reshape(-1, 128), pairs[:, 1].reshape(-1, 128)
            lo_up = pltpu.roll(lo, 128 - 16 * bit, 1)
            hi_up = pltpu.roll(hi, 16 * bit, 1)
            lo, hi, lo_up, hi_up = (v.reshape(8 // (2 * bit), bit, 8, 128) for v in (lo, hi, lo_up, hi_up))
            tiles = jnp.stack([jnp.where(mask, lo, hi_up), jnp.where(mask, lo_up, hi)], axis=1).reshape(8, 8, 128)
        return tiles

    def row_copy(rnd, x, i):
        d_row, d_sub = ROW_PEERS[i]
        return pltpu.make_async_remote_copy(
            src_ref=rowp.at[rnd, x], dst_ref=rowp.at[rnd, x],
            send_sem=row_send.at[rnd, x, i], recv_sem=row_recv.at[rnd, x],
            device_id=peer(0, d_row, d_sub), device_id_type=MESH)

    def col_copy(rnd, a):
        return pltpu.make_async_remote_copy(
            src_ref=colp.at[rnd, a], dst_ref=colp.at[rnd, a],
            send_sem=col_send.at[rnd, a], recv_sem=col_recv.at[rnd, a],
            device_id=peer(1, 0, 0), device_id_type=MESH)

    def dia_copy(rnd, i):
        turn = rnd % 2
        offs = ((1, turn, 1), (1, 1 - turn, 1), (0, 1, 1), (0, 0, 1))[i]
        return pltpu.make_async_remote_copy(
            src_ref=dst.at[rnd], dst_ref=dst.at[rnd],
            send_sem=dia_send.at[rnd, i], recv_sem=dia_recv.at[rnd],
            device_id=peer(*offs), device_id_type=MESH)

    def dia_pass(rnd):
        return pltpu.make_async_remote_copy(
            src_ref=dst.at[rnd], dst_ref=dst.at[rnd],
            send_sem=dia_fwd.at[rnd], recv_sem=dia_recv.at[rnd],
            device_id=peer(0, 0, 1), device_id_type=MESH)

    def passes(rnd):
        return (sub != rnd % 2) & ((col != rnd % 2) | (row != (rnd % 4) // 2))

    def send_row(rnd, x):
        for i in range(3):
            row_copy(rnd, x, i).start()

    def send_dia(rnd):
        for i in range(4):
            dia_copy(rnd, i).start()

    def close(rnd, a, x):
        dst[rnd] = mat[a, x]

        def group(g, carry):
            rg, cg = lax.div(g, 8), lax.div(g, 2)
            q, half = lax.rem(g, 8), lax.rem(g, 2) * 8
            ucol = lanes(jnp.broadcast_to(dst[rnd, rg, cg][None], (8, 8, 128)), nth_pivot + (16 * q + half))
            rows = lanes(dst[rnd, rg], in_grp[None] + 16 * q)
            left = lanes(jnp.broadcast_to(dst[rnd, :, cg][None], (8, 2, 8, 128)),
                         (nth_pivot + (grp_base + half)[None])[:, None])
            for p in range(8):
                rows = jnp.minimum(rows, ucol[0][None] + rows[:, p:p + 1, :])
                if p < 7:
                    ucol = jnp.minimum(ucol[1:], ucol[0][None] + ucol[1:, p:p + 1, :])
            block = dst[rnd]
            for p in range(8):
                block = jnp.minimum(block, left[p][:, None] + rows[:, p:p + 1, :][None])
            dst[rnd] = block
            return carry

        def groups(i, carry):
            return lax.fori_loop(0, 4, lambda u, c: group(i * 4 + u, c), carry, unroll=True)
        lax.fori_loop(0, 4, groups, 0)

    def make_brep(src, out):
        def one(i, carry):
            out[i] = lanes(src[lax.div(i, 8)], in_grp + 16 * lax.rem(i, 8))
            return carry
        lax.fori_loop(0, 16, one, 0, unroll=True)

    def product(acc, left, right, step):
        def chunk(i, acc):
            def pivot(u, acc):
                b = right[i * (step // 8) + lax.div(u, 8), :, pl.ds(lax.rem(u, 8), 1), :]
                return jnp.minimum(acc, left(i * (step // 16) + lax.div(u, 16), i * step + u, lax.rem(u, 16))[:, None] + b[None])
            return lax.fori_loop(0, step, pivot, acc, unroll=True)
        return lax.fori_loop(0, BLK // step, chunk, acc, unroll=step == BLK)

    def product_spreading(acc, tab, src, out):
        def half(r, acc):
            def group(q, acc):
                g = 8 * r + q
                out[g] = lanes(src[r], in_grp + 16 * q)
                for s in range(8):
                    acc = jnp.minimum(acc, tab[8 * g + s][:, None] + out[g, :, s:s + 1, :][None])
                return acc
            return lax.fori_loop(0, 8, group, acc, unroll=True)
        return lax.fori_loop(0, 2, half, acc)

    def close_and_send(rnd, a, x):
        close(rnd, a, x)
        send_dia(rnd)

    slot_r = jnp.where(my_row == 0, 0, ROUNDS)
    slot_c = jnp.where(col == 0, 0, ROUNDS)
    def unpack(a, x):
        for r in range(2):
            tiles = swap_chunks(in_ref[a, 64 * r:64 * r + 64, BLK * x:BLK * x + BLK].reshape(8, 8, 128))
            mat[a, x, r] = tiles
            if a == 0:
                rowp[slot_r, x, r] = tiles
            if x == 0:
                colp[slot_c, a, r] = tiles

    fetch.wait()
    unpack(0, 0)

    @pl.when((my_row == 0) & (col == 0))
    def _():
        close(0, 0, 0)
        pl.semaphore_wait(barrier, 7)
        send_dia(0)
    for a in range(2):
        for x in range(4):
            if a + x:
                unpack(a, x)

    @pl.when((my_row != 0) | (col != 0))
    def _():
        pl.semaphore_wait(barrier, 7)

    @pl.when(my_row == 0)
    def _():
        @pl.when(col != 0)
        def _():
            send_row(0, 0)
        for x in (1, 2, 3):
            send_row(0, x)

    @pl.when(col == 0)
    def _():
        @pl.when(my_row != 0)
        def _():
            col_copy(0, 0).start()
        col_copy(0, 1).start()

    def drain(k):
        is_row, is_col = my_row == k % 4, col == k % 2
        for x in range(4):
            @pl.when(is_row & (~is_col | (x != k // 2)))
            def _():
                for i in range(3):
                    row_copy(k, x, i).wait_send()
        for a in range(2):
            @pl.when(is_col & (~is_row | (a != k // 4)))
            def _():
                col_copy(k, a).wait_send()

        @pl.when(is_row & is_col)
        def _():
            for i in range(4):
                dia_copy(k, i).wait_send()

        @pl.when(passes(k))
        def _():
            dia_pass(k).wait_send()

    def one_round(k, carry):
        n = k + 1
        more = n < ROUNDS
        own_row = (my_row == n % 4) & more
        own_col = (col == n % 2) & more
        a1 = jnp.minimum(n // 4, 1)
        x1 = ((n + jnp.where(col == n % 2, 0, 1)) // 2) % 4
        xk = k // 2
        is_row, is_col = my_row == k % 4, col == k % 2

        def first_rows():
            @pl.when(~is_row)
            def _():
                row_copy(k, x1, 0).wait_recv()
            make_brep(rowp.at[k, x1], brep.at[x1])

        @pl.when(~is_col)
        def _():
            first_rows()

        @pl.when(k > 0)
        def _():
            drain(k - 1)

        @pl.when(~is_row | ~is_col)
        def _():
            dia_copy(k, 0).wait_recv()

        @pl.when(passes(k))
        def _():
            dia_pass(k).start()

        def wait_row(x):
            @pl.when(~is_row)
            def _():
                row_copy(k, x, 0).wait_recv()

        make_brep(dst.at[k], brepd)

        def head(h, carry):
            a = jnp.where(h == 0, a1, 1 - a1)

            on_diag = is_row & (a == k // 4)
            send_it = own_row & (h == 0)

            @pl.when(~is_col & ~on_diag)
            def _():
                col_copy(k, a).wait_recv()

            @pl.when(on_diag)
            def _():
                cpr[...] = dst[k]

            @pl.when(~on_diag)
            def _():
                pan = colp.at[k, a]
                cpr[...] = product(pan[...], lambda c, p, l: lanes(pan[:, c], grp_base + l), brepd, HEAD_STEP)

            @pl.when(is_col)
            def _():
                mat[a, xk] = cpr[...]

                @pl.when(h == 0)
                def _():
                    first_rows()

            @pl.when(is_col & send_it)
            def _():
                rowp[n, xk] = cpr[...]

            tab = cb.at[a]

            def fly(c, p, l):
                avs = lanes(cpr[:, c], grp_base + l)
                tab[p] = avs
                return avs
            acc = product(mat[a, x1], fly, brep.at[x1], HEAD_STEP)
            mat[a, x1] = acc
            rowp[jnp.where(send_it, n, ROUNDS), x1] = acc
            colp[jnp.where(own_col, n, ROUNDS), a] = acc

            @pl.when(send_it & ~own_col)
            def _():
                send_row(n, x1)

            @pl.when(own_col & ~send_it)
            def _():
                col_copy(n, a).start()

            @pl.when(send_it & own_col)
            def _():
                close_and_send(n, a, x1)
            return carry

        def tail(phase, t, carry):
            h = t // 3
            a = jnp.where(h == 0, a1, 1 - a1)
            x = (x1 + 1 + t % 3) % 4

            @pl.when(((col != k % 2) | (t % 3 != 2)) & ((own_row & (h == phase)) | (~own_row & (phase == 1))))
            def _():
                tab = cb.at[a]

                @pl.when(h == 0)
                def _():
                    wait_row(x)
                    mat[a, x] = product_spreading(mat[a, x], tab, rowp.at[k, x], brep.at[x])

                @pl.when(h == 1)
                def _():
                    mat[a, x] = product(mat[a, x], lambda c, p, l: tab[p], brep.at[x], TAIL_STEP)

                @pl.when(own_row & (h == 0))
                def _():
                    rowp[n, x] = mat[a, x]
                    send_row(n, x)
            return carry
        def in_order(phase, carry):
            head(phase, carry)
            lax.fori_loop(0, 6, functools.partial(tail, phase), 0)

            @pl.when(is_col & own_row & (phase == 0))
            def _():
                send_row(n, xk)
            return carry
        lax.fori_loop(0, 2, in_order, 0)
        return carry
    lax.fori_loop(0, ROUNDS, one_round, 0)

    for a in range(2):
        for x in range(4):
            for r in range(2):
                tiles = swap_chunks(mat[a, x, r])
                out_ref[a, 64 * r:64 * r + 64, BLK * x:BLK * x + BLK] = tiles.reshape(64, 128)

    drain(ROUNDS - 1)


def solution(mesh):
    spec = P(('parts', 'row', 'sub'), None, 'col')
    tile = (8, 128)
    dma = pltpu.SemaphoreType.DMA

    def local_run(local_dist):
        return pl.pallas_call(
            kernel,
            out_shape=jax.ShapeDtypeStruct(local_dist.shape, local_dist.dtype),
            in_specs=[pl.BlockSpec(memory_space=pltpu.HBM)],
            out_specs=pl.BlockSpec(memory_space=pltpu.VMEM),
            scratch_shapes=[
                pltpu.VMEM(local_dist.shape, jnp.float32), dma(()),
                pltpu.VMEM((2, 4, 2, 8) + tile, jnp.float32),
                pltpu.VMEM((ROUNDS + 1, 4, 2, 8) + tile, jnp.float32),
                pltpu.VMEM((ROUNDS + 1, 2, 2, 8) + tile, jnp.float32),
                pltpu.VMEM((ROUNDS, 2, 8) + tile, jnp.float32),
                pltpu.VMEM((2, BLK, 2) + tile, jnp.float32),
                pltpu.VMEM((4, 16, 8) + tile, jnp.float32),
                pltpu.VMEM((16, 8) + tile, jnp.float32),
                pltpu.VMEM((2, 8) + tile, jnp.float32),
                dma((ROUNDS, 4, 3)), dma((ROUNDS, 4)),
                dma((ROUNDS, 2)), dma((ROUNDS, 2)),
                dma((ROUNDS, 4)), dma((ROUNDS,)), dma((ROUNDS,)),
            ],
            compiler_params=pltpu.CompilerParams(collective_id=0, has_side_effects=True, vmem_limit_bytes=55839744),
            name='apsp',
        )(local_dist)

    return jax.shard_map(local_run, mesh=mesh, in_specs=(spec,), out_specs=spec, check_vma=False)
```
